32 devices in a mesh: lat: 4 (over y, x), lon: 8 (over z, core).
Axes of the slice: x: 2, y: 2, z: 4, core: 2. Of those that a mesh axis runs over, the one named last changes fastest.
Arguments:
- latent_field: bfloat16 [640, 32, 64], P(None, 'lat', 'lon'), may hold values from -6 to 6
- spectral_filter: float32 [640, 32], P('lon'), may hold values from -5 to 5
- conv_weight: float32 [9, 640], replicated, may hold values from -2 to 2
- norm_gain: float32 [640], replicated, may hold values from 0.1 to 1.9
- weight_in: bfloat16 [640, 1280], replicated, may hold values from -0.25 to 0.25
- weight_out: bfloat16 [1280, 640], replicated, may hold values from -0.15625 to 0.15625
Outputs:
- updated: bfloat16 [640, 32, 64], P(None, 'lat', 'lon')
The draws below stay inside these ranges and needn't reach their ends.
All inputs are finite; a program needn't handle non-finite values.
Results may differ from the reference program's by a relative error of at most 0.01.
Values may be sent and summed in bfloat16 or wider, within the bound.
A program may use at most 128 MiB of HBM per device.

```python
import math
import jax
import jax.numpy as jnp
from jax import lax

C = 640
HID = 1280
LAT_DEV = 8
NLAT = 32
NLON = 64
N_LAT = 4
N_LON = 8


def steps_of(key, dims, cuts, least, largest):
    gain, own = 1.0, jax.random.fold_in(key, 6)
    for axis_at, parts in cuts:
        steps = jnp.exp(jax.random.uniform(jax.random.fold_in(own, axis_at), (parts,), jnp.float32, least / len(cuts), largest / len(cuts)))
        gain = gain * jnp.repeat(steps, dims[axis_at] // parts).reshape([-1 if axis == axis_at else 1 for axis in range(len(dims))])
    return gain


def scatter_about(own_key, dims, scale, bound, pieces=(), kind=jnp.bfloat16):
    drawn = jax.random.normal(own_key, dims, jnp.float32) * scale
    if len(pieces) > 0:
        drawn = steps_of(own_key, dims, pieces, -0.22, 0.18) * drawn
    return jnp.clip(drawn, min=-bound, max=bound).astype(kind)


def setup_inputs(seed: int = 0) -> dict:
    keys = jax.random.split(jax.random.key(seed), 7)
    return {
        "latent_field": scatter_about(keys[0], (C, NLAT, NLON), 1.0, 6.0, ((1, 4), (2, 8))),
        "spectral_filter": scatter_about(keys[1], (C, NLAT), 1.0, 5.0, ((0, 8),), jnp.float32),
        "conv_weight": scatter_about(keys[2], (9, C), 9 ** -0.5, 2.0, (), jnp.float32),
        "norm_gain": jnp.clip(1.0 + 0.18 * jax.random.normal(keys[3], (C,), jnp.float32), 0.1, 1.9),
        "weight_in": scatter_about(keys[4], (C, HID), C ** -0.5, 0.25),
        "weight_out": scatter_about(keys[5], (HID, C), HID ** -0.5, 0.15625),
    }


highest = lax.Precision.HIGHEST
epsilon_norm = 1e-06

def quadrature(lat_count):
    colatitude = (jnp.arange(lat_count, dtype=jnp.float32) + 0.5) * (math.pi / lat_count)
    return jnp.sin(colatitude) * (math.pi / lat_count)

def fourier_tables(lon_count, mode_count):
    wave_index = jnp.arange(mode_count, dtype=jnp.int32)[:, None] * jnp.arange(lon_count, dtype=jnp.int32)[None, :]
    phase_angle = (wave_index % lon_count).astype(jnp.float32) * (2.0 * math.pi / lon_count)
    cosine = jnp.cos(phase_angle)
    sine_table = jnp.sin(phase_angle)
    angle_step = 2.0 * math.pi / lon_count
    forward = jnp.concatenate([angle_step * cosine, -angle_step * sine_table], axis=0)
    weight = jnp.where(jnp.arange(mode_count, dtype=jnp.int32) == 0, 1.0, 2.0).astype(jnp.float32)[:, None]
    inverse = jnp.concatenate([weight * cosine, -weight * sine_table], axis=0)
    return (forward, inverse)

def legendre_rows(order_ids, lat_count):
    colatitude = (jnp.arange(lat_count, dtype=jnp.float32) + 0.5) * (math.pi / lat_count)
    cosine = jnp.cos(colatitude)
    sine_col = jnp.sin(colatitude)
    order_f = order_ids.astype(jnp.float32)
    factor_index = jnp.arange(1, lat_count, dtype=jnp.float32)
    ratio_log = jnp.log((2.0 * factor_index - 1.0) / (2.0 * factor_index))
    included = (factor_index[None, :] <= order_f[:, None]).astype(jnp.float32)
    log_factor = lax.optimization_barrier(jnp.sum(included * ratio_log[None, :], axis=1))
    start_log = 0.5 * jnp.log((2.0 * order_f + 1.0) / (4.0 * math.pi)) + 0.5 * log_factor
    start_log = start_log[:, None] + order_f[:, None] * jnp.log(sine_col)[None, :]
    blank_rows = jnp.zeros((order_ids.shape[0], lat_count), jnp.float32)
    order_col = order_f[:, None]

    def advance(state_carry, degree):
        before, current, scale_log = state_carry
        degree_f = degree.astype(jnp.float32)
        alpha_term = jnp.sqrt((4.0 * degree_f * degree_f - 1.0) / jnp.maximum(degree_f * degree_f - order_col * order_col, 1.0))
        beta_term = jnp.sqrt(jnp.maximum((degree_f - 1.0) ** 2 - order_col * order_col, 0.0) / jnp.maximum(4.0 * (degree_f - 1.0) ** 2 - 1.0, 1.0))
        stepped = alpha_term * (cosine[None, :] * current - beta_term * before)
        at_start = order_ids[:, None] == degree
        past_start = order_ids[:, None] < degree
        fresh_value = jnp.where(at_start, 1.0, jnp.where(past_start, stepped, 0.0))
        fresh_log = jnp.where(at_start, start_log, scale_log)
        entry_value = fresh_value * jnp.exp(fresh_log)
        rescale = jnp.where(past_start | at_start, jnp.maximum(jnp.abs(fresh_value), jnp.abs(current)), 1.0)
        return ((current / rescale, fresh_value / rescale, fresh_log + jnp.log(rescale)), entry_value)
    degrees = jnp.arange(lat_count, dtype=jnp.int32)
    unused, legendre = lax.scan(advance, (blank_rows, blank_rows, blank_rows), degrees, unroll=16)
    return legendre

def filter_modes(banded, legendre, filter_block, quad_weights):
    coefficients = jnp.einsum('lmj,pmcj->pmcl', legendre, banded * quad_weights[None, None, None, :], precision=highest)
    coefficients = coefficients * filter_block[None, None, :, :]
    return jnp.einsum('lmj,pmcl->pmcj', legendre, coefficients, precision=highest)

def wrap_columns(extended):
    return jnp.concatenate([extended[:, :, -1:], extended, extended[:, :, :1]], axis=2)

def depthwise_core(extended, kernel, lat_rows, lon_cols):
    accumulated = jnp.zeros((extended.shape[0], lat_rows, lon_cols), jnp.float32)
    for row_shift in range(3):
        for col_shift in range(3):
            piece = extended[:, row_shift:row_shift + lat_rows, col_shift:col_shift + lon_cols].astype(jnp.float32)
            accumulated = accumulated + kernel[3 * row_shift + col_shift][:, None, None] * piece
    return accumulated.astype(jnp.bfloat16)

def channel_mlp(summed_low, norm_gain, weight_in, weight_out):
    summed = summed_low.astype(jnp.float32)
    scale_inv = lax.rsqrt(lax.optimization_barrier(jnp.mean(summed * summed, axis=0, keepdims=True)) + epsilon_norm)
    normed = (summed * scale_inv * norm_gain[:, None]).astype(jnp.bfloat16)
    hidden = lax.dot_general(weight_in, normed, (((0,), (0,)), ((), ())), preferred_element_type=jnp.float32)
    hidden = jax.nn.gelu(hidden, approximate=False).astype(jnp.bfloat16)
    result = summed + lax.dot_general(weight_out, hidden, (((0,), (0,)), ((), ())), preferred_element_type=jnp.float32)
    return result.astype(jnp.bfloat16)

def row_blocks(array):
    return jnp.transpose(array.reshape(C, N_LAT, LAT_DEV * NLON), (1, 0, 2))

def reference(latent_field, spectral_filter, conv_weight, norm_gain, weight_in, weight_out):
    chan_block = C // N_LON
    forward, inverse = fourier_tables(NLON, NLAT)
    legendre = legendre_rows(jnp.arange(NLAT, dtype=jnp.int32), NLAT)
    quad_weights = quadrature(NLAT)
    field_blocks = latent_field.reshape(N_LON, chan_block, NLAT, NLON)
    filter_blocks = spectral_filter.reshape(N_LON, chan_block, NLAT)
    kernel_blocks = jnp.transpose(conv_weight.reshape(9, N_LON, chan_block), (1, 0, 2))

    def branch_pair(inputs):
        field_block, filter_block, kernel_block = inputs
        flattened = field_block.astype(jnp.float32).reshape(chan_block * NLAT, NLON)
        spectrum = lax.dot_general(forward, flattened, (((1,), (1,)), ((), ())), precision=highest)
        spectrum = spectrum.reshape(2, NLAT, chan_block, NLAT)
        synthesized = filter_modes(spectrum, legendre, filter_block, quad_weights)
        regridded = lax.dot_general(synthesized.reshape(2 * NLAT, chan_block * NLAT), inverse, (((0,), (0,)), ((), ())), precision=highest)
        spectral = regridded.reshape(chan_block, NLAT, NLON).astype(jnp.bfloat16)
        extended = jnp.pad(field_block, ((0, 0), (1, 1), (0, 0)))
        local_mix = depthwise_core(wrap_columns(extended), kernel_block, NLAT, NLON)
        return (spectral, local_mix)
    spectral, local_mix = lax.map(branch_pair, (field_blocks, filter_blocks, kernel_blocks))
    spectral = spectral.reshape(C, NLAT, NLON)
    local_mix = local_mix.reshape(C, NLAT, NLON)

    def mix_band(inputs):
        field_band, spectral_band, conv_band = inputs
        summed = field_band.astype(jnp.float32) + spectral_band.astype(jnp.float32) + conv_band.astype(jnp.float32)
        return channel_mlp(summed.astype(jnp.bfloat16), norm_gain, weight_in, weight_out)
    bands = lax.map(mix_band, (row_blocks(latent_field), row_blocks(spectral), row_blocks(local_mix)))
    return jnp.transpose(bands, (1, 0, 2)).reshape(C, NLAT, NLON)
```

```python
import functools
import math

import jax
import jax.numpy as jnp
import numpy as np
from jax import lax
from jax.experimental import pallas as pl
from jax.experimental.pallas import tpu as pltpu
from jax.sharding import PartitionSpec as P

highest = lax.Precision.HIGHEST
epsilon_norm = 1e-06


def with_halo(cells, sides, width):
    for axis, dim in sides:
        count = lax.axis_size(axis)
        ends = count - 1
        head = lax.slice_in_dim(cells, 0, width, axis=dim)
        tail = lax.slice_in_dim(cells, cells.shape[dim] - width, cells.shape[dim], axis=dim)
        cells = jnp.concatenate(
            [
                lax.ppermute(tail, axis, [(i, (i + 1) % count) for i in range(ends)]),
                cells,
                lax.ppermute(head, axis, [((i + 1) % count, i) for i in range(ends)]),
            ],
            axis=dim,
        )
    return cells


def quadrature(lat_count):
    colatitude = (jnp.arange(lat_count, dtype=jnp.float32) + 0.5) * (math.pi / lat_count)
    return jnp.sin(colatitude) * (math.pi / lat_count)


def fourier_tables(lon_count, mode_count):
    wave_index = (
        jnp.arange(mode_count, dtype=jnp.int32)[:, None]
        * jnp.arange(lon_count, dtype=jnp.int32)[None, :]
    )
    phase_angle = (wave_index % lon_count).astype(jnp.float32) * (2.0 * math.pi / lon_count)
    cosine = jnp.cos(phase_angle)
    sine_table = jnp.sin(phase_angle)
    angle_step = 2.0 * math.pi / lon_count
    forward = jnp.concatenate([angle_step * cosine, -angle_step * sine_table], axis=0)
    weight = jnp.where(jnp.arange(mode_count, dtype=jnp.int32) == 0, 1.0, 2.0).astype(jnp.float32)[
        :, None
    ]
    inverse = jnp.concatenate([weight * cosine, -weight * sine_table], axis=0)
    return (forward, inverse)


def legendre_rows(order_ids, lat_count):
    colatitude = (jnp.arange(lat_count, dtype=jnp.float32) + 0.5) * (math.pi / lat_count)
    cosine = jnp.cos(colatitude)
    sine_col = jnp.sin(colatitude)
    order_f = order_ids.astype(jnp.float32)
    factor_index = jnp.arange(1, lat_count, dtype=jnp.float32)
    ratio_log = jnp.log((2.0 * factor_index - 1.0) / (2.0 * factor_index))
    included = (factor_index[None, :] <= order_f[:, None]).astype(jnp.float32)
    log_factor = jnp.sum(included * ratio_log[None, :], axis=1)
    start_log = 0.5 * jnp.log((2.0 * order_f + 1.0) / (4.0 * math.pi)) + 0.5 * log_factor
    start_log = start_log[:, None] + order_f[:, None] * jnp.log(sine_col)[None, :]
    blank_rows = jnp.zeros((order_ids.shape[0], lat_count), jnp.float32)
    order_col = order_f[:, None]

    def advance(state_carry, degree):
        before, current, scale_log = state_carry
        degree_f = degree.astype(jnp.float32)
        alpha_term = jnp.sqrt(
            (4.0 * degree_f * degree_f - 1.0)
            / jnp.maximum(degree_f * degree_f - order_col * order_col, 1.0)
        )
        beta_term = jnp.sqrt(
            jnp.maximum((degree_f - 1.0) ** 2 - order_col * order_col, 0.0)
            / jnp.maximum(4.0 * (degree_f - 1.0) ** 2 - 1.0, 1.0)
        )
        stepped = alpha_term * (cosine[None, :] * current - beta_term * before)
        at_start = order_ids[:, None] == degree
        past_start = order_ids[:, None] < degree
        fresh_value = jnp.where(at_start, 1.0, jnp.where(past_start, stepped, 0.0))
        fresh_log = jnp.where(at_start, start_log, scale_log)
        entry_value = fresh_value * jnp.exp(fresh_log)
        rescale = jnp.where(
            past_start | at_start, jnp.maximum(jnp.abs(fresh_value), jnp.abs(current)), 1.0
        )
        return (
            (current / rescale, fresh_value / rescale, fresh_log + jnp.log(rescale)),
            entry_value,
        )

    degrees = jnp.arange(lat_count, dtype=jnp.int32)
    unused, legendre = lax.scan(advance, (blank_rows, blank_rows, blank_rows), degrees)
    return legendre


def filter_modes(banded, legendre, filter_block, quad_weights):
    coefficients = jnp.einsum(
        "lmj,pmcj->pmcl", legendre, banded * quad_weights[None, None, None, :], precision=highest
    )
    coefficients = coefficients * filter_block[None, None, :, :]
    return jnp.einsum("lmj,pmcl->pmcj", legendre, coefficients, precision=highest)


def wrap_columns(extended):
    return jnp.concatenate([extended[:, :, -1:], extended, extended[:, :, :1]], axis=2)


def depthwise_core(extended, kernel, lat_rows, lon_cols):
    accumulated = jnp.zeros((extended.shape[0], lat_rows, lon_cols), jnp.float32)
    for row_shift in range(3):
        for col_shift in range(3):
            piece = extended[
                :, row_shift : row_shift + lat_rows, col_shift : col_shift + lon_cols
            ].astype(jnp.float32)
            accumulated = accumulated + kernel[3 * row_shift + col_shift][:, None, None] * piece
    return accumulated.astype(jnp.bfloat16)


def channel_mlp(summed_low, norm_gain, weight_in, weight_out):
    summed = summed_low.astype(jnp.float32)
    scale_inv = lax.rsqrt(jnp.mean(summed * summed, axis=0, keepdims=True) + epsilon_norm)
    normed = (summed * scale_inv * norm_gain[:, None]).astype(jnp.bfloat16)
    hidden = lax.dot_general(
        weight_in, normed, (((0,), (0,)), ((), ())), preferred_element_type=jnp.float32
    )
    hidden = jax.nn.gelu(hidden, approximate=False).astype(jnp.bfloat16)
    result = summed + lax.dot_general(
        weight_out, hidden, (((0,), (0,)), ((), ())), preferred_element_type=jnp.float32
    )
    return result.astype(jnp.bfloat16)


def add_three(first, second, third):
    total = first.astype(jnp.float32) + second.astype(jnp.float32) + third.astype(jnp.float32)
    return total.astype(jnp.bfloat16)


def on_device(latent_field, spectral_filter, conv_weight, norm_gain, weight_in, weight_out):
    channels, lat_rows, lon_cols = latent_field.shape
    sector_count = lax.axis_size("lon")
    lat_count = lat_rows * lax.axis_size("lat")
    lon_count = lon_cols * sector_count
    chan_block = channels // sector_count
    spread = lax.all_to_all(latent_field, "lon", split_axis=0, concat_axis=2, tiled=True)
    forward, inverse = fourier_tables(lon_count, lat_count)
    flattened = spread.astype(jnp.float32).reshape(chan_block * lat_rows, lon_count)
    spectrum = lax.dot_general(forward, flattened, (((1,), (1,)), ((), ())), precision=highest)
    spectrum = spectrum.reshape(2, lat_count, chan_block, lat_rows)
    banded = lax.all_to_all(spectrum, "lat", split_axis=1, concat_axis=3, tiled=True)
    order_ids = lax.axis_index("lat") * lat_rows + jnp.arange(lat_rows, dtype=jnp.int32)
    legendre = legendre_rows(order_ids, lat_count)
    synthesized = filter_modes(banded, legendre, spectral_filter, quadrature(lat_count))
    regathered = lax.all_to_all(synthesized, "lat", split_axis=3, concat_axis=1, tiled=True)
    regridded = lax.dot_general(
        regathered.reshape(2 * lat_count, chan_block * lat_rows),
        inverse,
        (((0,), (0,)), ((), ())),
        precision=highest,
    )
    spectral = regridded.reshape(chan_block, lat_rows, lon_count).astype(jnp.bfloat16)
    own_kernel = lax.dynamic_slice_in_dim(
        conv_weight, lax.axis_index("lon") * chan_block, chan_block, 1
    )
    rimmed = with_halo(spread, (("lat", 1),), 1)
    sector_mix = depthwise_core(wrap_columns(rimmed), own_kernel, lat_rows, lon_count)
    sector_sum = add_three(spread, spectral, sector_mix)
    summed = lax.all_to_all(sector_sum, "lon", split_axis=2, concat_axis=0, tiled=True)
    summed = summed.reshape(channels, lat_rows * lon_cols)
    result = channel_mlp(summed, norm_gain, weight_in, weight_out)
    return result.reshape(channels, lat_rows, lon_cols)


CLASSES = ((0, 0), (1, 0), (0, 1), (1, 1))


def folded_tables(lat_devices, lon_devices, lat_rows, lon_cols):
    lat_count, lon_count = lat_devices * lat_rows, lon_devices * lon_cols
    theta = (np.arange(lat_count // 2) + 0.5) * (math.pi / lat_count)
    x, s = np.cos(theta), np.sin(theta)
    phi = 2.0 * math.pi * (np.arange(lon_count // 2) + 0.5) / lon_count
    row, column = [], []
    for b in reversed(range(lon_devices // 2)):
        for a in range(lat_devices // 2):
            row.append(np.repeat(a * lat_rows + np.arange(lat_rows), lon_cols))
            column.append(np.tile(b * lon_cols + np.arange(lon_cols), lat_rows))
    row, column = np.concatenate(row), np.concatenate(column)
    columns = {key: [] for key in CLASSES}
    degrees = {key: [] for key in CLASSES}
    weights = {key: [] for key in CLASSES}
    for m in range(lat_count):
        k = np.arange(1, m + 1)
        log_start = 0.5 * (
            np.log((2 * m + 1) / (4 * math.pi)) + np.sum(np.log((2 * k - 1) / (2 * k)))
        )
        before, current = np.zeros(lat_count // 2), np.exp(log_start + m * np.log(s))
        for l in range(m, lat_count):
            if l > m:
                a = math.sqrt((4.0 * l * l - 1) / (l * l - m * m))
                b = math.sqrt(((l - 1.0) ** 2 - m * m) / (4.0 * (l - 1) ** 2 - 1))
                before, current = current, a * (x * current - b * before)
            for phase, wave in enumerate([np.cos(m * phi), -np.sin(m * phi)][: 1 if m == 0 else 2]):
                key = ((l + m) % 2, phase)
                columns[key].append(current[row] * wave[column])
                degrees[key].append(l)
                weights[key].append((1.0 if m == 0 else 2.0) * 2.0 * math.pi / lon_count)
    tables, selects, starts = [], [], [0]
    for key in CLASSES:
        width = -(-len(columns[key]) // 128) * 128
        fill = width - len(columns[key])
        tables.append(np.pad(np.stack(columns[key], 1), ((0, 0), (0, fill))))
        select = np.arange(lat_count)[:, None] == np.array(degrees[key])[None, :]
        selects.append(np.pad(select * np.array(weights[key])[None, :], ((0, 0), (0, fill))))
        starts.append(starts[-1] + width)
    quad = s * (math.pi / lat_count)
    quad = np.repeat(quad.reshape(lat_devices // 2, lat_rows), lon_cols, axis=1)
    return (
        np.concatenate(tables, 1),
        np.concatenate(selects, 1).astype(np.float32),
        np.tile(quad, (1, 2)).astype(np.float32),
        tuple(starts),
    )


MESH = pl.DeviceIdType.MESH
NT = (((1,), (1,)), ((), ()))


def upper_rows(own):
    return -(-(own // 2) // 8) * 8


def block_kernel(
    lat_devices, lon_devices, lat_rows, lon_cols, starts,
    x_hbm, filter_hbm, taps_hbm, norm_hbm, win_hbm, wout_hbm, table_hbm, select_hbm, quad_hbm,
    out_hbm,
    xb, filt, taps, norm, win, wout, table, select, quad,
    xf, src, mid, out, dst, filt_in, edge_out, corner_out, edge_in, corner_in, total, res,
    local_sem, send1, recv1, send2, recv2, halo_send, halo_recv, filt_send, filt_recv,
):
    A, B = lat_devices, lon_devices
    A2, B2, first = A // 2, B // 2, B // 4
    workers = A * B2
    devices = A * B
    points, channels = xb.shape
    own = channels // workers
    up = upper_rows(own)
    low = own - up
    half = points
    a, b = lax.axis_index("lat"), lax.axis_index("lon")
    me = b * A + a
    worker = jnp.logical_and(b >= first, b < first + B2)
    mine = jnp.where(worker, (b - first) * A + a, -1)
    f32, bf16 = jnp.float32, jnp.bfloat16

    fetch = [
        pltpu.make_async_copy(s, d, local_sem.at[i])
        for i, (s, d) in enumerate(
            [(x_hbm, xb), (filter_hbm, filt), (quad_hbm, quad), (table_hbm, table), (select_hbm, select),
             (taps_hbm, taps), (norm_hbm, norm), (win_hbm, win), (wout_hbm, wout)]
        )
    ]
    fetch[0].start()
    barrier = pltpu.get_barrier_semaphore()
    neighbours = [(da, db) for da in (-1, 0, 1) for db in (-1, 0, 1) if (da, db) != (0, 0)]

    def inside(da):
        return jnp.logical_and(a + da >= 0, a + da < A)

    def at(da, db):
        return (a + da, lax.rem(b + db + B, B))

    @pl.when(worker)
    def _():
        def greet(step, carry):
            peer = lax.rem(me + step, devices)
            pl.semaphore_signal(
                barrier, inc=1, device_id=(lax.rem(peer, A), lax.div(peer, A)), device_id_type=MESH
            )
            return carry

        lax.fori_loop(1, devices, greet, 0)

    @pl.when(jnp.logical_not(worker))
    def _():
        for da, db in neighbours:
            @pl.when(inside(da))
            def _():
                pl.semaphore_signal(barrier, inc=1, device_id=at(da, db), device_id_type=MESH)

    for copy in fetch[1:]:
        copy.start()

    turn_lat, turn_lon = a >= A2, b >= B2
    p_row = lax.broadcasted_iota(jnp.int32, (points, 2 * half), 0)
    p_col = lax.broadcasted_iota(jnp.int32, (points, 2 * half), 1)

    def turned(index):
        jl, kl = lax.div(index, lon_cols), lax.rem(index, lon_cols)
        jl = jnp.where(turn_lat, lat_rows - 1 - jl, jl)
        kl = jnp.where(turn_lon, lon_cols - 1 - kl, kl)
        return jl * lon_cols + kl

    place = jnp.where(p_row == turned(lax.rem(p_col, half)), 1.0, 0.0)
    place_both = place.astype(bf16)
    place_left = jnp.where(p_col < half, place, 0.0).astype(bf16)
    lane = lax.broadcasted_iota(jnp.int32, (up, 2 * half), 1)
    left = lane < half

    fetch[0].wait()
    xf[...] = xb[...].astype(f32)
    xt = jnp.transpose(xf[...], (1, 0)).astype(bf16)
    xt = jnp.dot(xt, place_both, preferred_element_type=f32)
    blank = jnp.zeros((up - low, 2 * half), f32)
    for g in range(workers):
        upper = xt[own * g : own * g + up]
        lower = jnp.concatenate([xt[own * g + up : own * (g + 1)], blank], 0)
        src[g] = jnp.where(left, upper, lower).astype(bf16)

    @pl.when(worker)
    def _():
        mid[me] = src[mine]

    west, east = [
        jnp.concatenate([xf[k + lon_cols * r : k + lon_cols * r + 1] for r in range(lat_rows)], 0)
        for k in (0, lon_cols - 1)
    ]
    edge_out[0] = west.astype(bf16)
    edge_out[1] = east.astype(bf16)
    chunks = channels // 128
    for i, (r, side) in enumerate([(0, west), (0, east), (lat_rows - 1, west), (lat_rows - 1, east)]):
        parts = [side[r : r + 1, 128 * c : 128 * (c + 1)] for c in range(chunks)]
        parts.append(jnp.zeros((8 - chunks, 128), f32))
        corner_out[i] = jnp.concatenate(parts, 0).astype(bf16)

    def outside(db):
        other = lax.rem(b + db + B, B)
        return jnp.where(jnp.logical_and(other >= first, other < first + B2), 0, 1)

    rims = jnp.where(a > 0, 1, 0) + jnp.where(a < A - 1, 1, 0)
    greetings = jnp.where(worker, workers - 1, workers)
    greetings = greetings + rims * outside(0) + (1 + rims) * (outside(-1) + outside(1))
    pl.semaphore_wait(barrier, greetings)

    def first_copy(g):
        return pltpu.make_async_remote_copy(
            src_ref=src.at[g], dst_ref=mid.at[me], send_sem=send1.at[g], recv_sem=recv1.at[me],
            device_id=(lax.rem(g, A), first + lax.div(g, A)), device_id_type=MESH,
        )

    def first_send(step, carry):
        g = lax.rem(me + step, workers)

        @pl.when(g != mine)
        def _():
            first_copy(g).start()

        return carry

    lax.fori_loop(0, workers, first_send, 0)

    fetch[1].wait()
    owner_row = lax.div(a, A2) == lax.rem(b, 2)
    filt_lon = first + lax.div(b, 2)
    keeps = jnp.logical_and(owner_row, filt_lon == b)
    gives = jnp.logical_and(owner_row, filt_lon != b)
    filt_copy = pltpu.make_async_remote_copy(
        src_ref=filt, dst_ref=filt_in, send_sem=filt_send, recv_sem=filt_recv,
        device_id=(a, filt_lon), device_id_type=MESH,
    )

    @pl.when(gives)
    def _():
        filt_copy.start()

    @pl.when(keeps)
    def _():
        filt_in[...] = filt[...]

    def halo_copy(da, db):
        if db == 0:
            row = 0 if da < 0 else points - lon_cols
            source, target = xb.at[pl.ds(row, lon_cols)], edge_in.at[1 if da < 0 else 0]
            slot = 1 if da < 0 else 0
        elif da == 0:
            slot = 3 if db < 0 else 2
            source, target = edge_out.at[0 if db < 0 else 1], edge_in.at[slot]
        else:
            index = (0 if da < 0 else 2) + (0 if db < 0 else 1)
            source, target = corner_out.at[index], corner_in.at[3 - index]
            slot = 4 + 3 - index
        return pltpu.make_async_remote_copy(
            src_ref=source, dst_ref=target, send_sem=halo_send.at[slot], recv_sem=halo_recv.at[slot],
            device_id=at(da, db), device_id_type=MESH,
        )

    for da, db in neighbours:
        @pl.when(inside(da))
        def _():
            halo_copy(da, db).start()

    def index_of(ai, bi):
        return bi * A + ai

    def first_wait(o, carry):
        @pl.when(o != me)
        def _():
            pltpu.make_async_remote_copy(
                src_ref=src.at[0], dst_ref=mid.at[o], send_sem=send1.at[0], recv_sem=recv1.at[o],
                device_id=(lax.rem(o, A), lax.div(o, A)), device_id_type=MESH,
            ).wait_recv()

        return carry

    def widths(c):
        return pl.ds(starts[c], starts[c + 1] - starts[c])

    def folded(bs):
        tiles = [[] for _ in CLASSES]
        for bi in bs:
            parts = []
            for ai in range(A2):
                f00, f10, f01, f11 = [
                    mid[index_of(i, j)].astype(f32)
                    for i, j in [(ai, bi), (A - 1 - ai, bi), (ai, B - 1 - bi), (A - 1 - ai, B - 1 - bi)]
                ]
                s0, d0, s1, d1 = f00 + f10, f00 - f10, f01 + f11, f01 - f11
                w = quad[ai : ai + 1, :]
                parts.append([(s0 + s1) * w, (d0 + d1) * w, (s0 - s1) * w, (d0 - d1) * w])
            for ai in range(0, A2, 2):
                for c in range(4):
                    u, v = parts[ai][c], parts[ai + 1][c]
                    upper = jnp.where(left, u, pltpu.roll(v, half, 1))
                    lower = jnp.where(left, pltpu.roll(u, half, 1), v)
                    tiles[c].append(jnp.concatenate([upper, lower[:low]], 0).astype(bf16))
        return [jnp.concatenate(t, 1) for t in tiles]

    inner = tuple(reversed(range(B2 // 2, B2)))
    outer = tuple(reversed(range(B2 // 2)))
    rows_of = lambda bs: pl.ds((B2 - 1 - bs[0]) * A2 * half, len(bs) * A2 * half)

    def second_copy(o):
        return pltpu.make_async_remote_copy(
            src_ref=out.at[o], dst_ref=dst.at[mine], send_sem=send2.at[o], recv_sem=recv2.at[mine],
            device_id=(lax.rem(o, A), lax.div(o, A)), device_id_type=MESH,
        )

    @pl.when(worker)
    def _():
        for i in (2, 3, 4):
            fetch[i].wait()

        @pl.when(jnp.logical_not(keeps))
        def _():
            pltpu.make_async_remote_copy(
                src_ref=filt, dst_ref=filt_in, send_sem=filt_send, recv_sem=filt_recv,
                device_id=(a, 2 * (b - first) + lax.div(a, A2)), device_id_type=MESH,
            ).wait_recv()

        held = filt_in.shape[1]
        r = lax.broadcasted_iota(jnp.int32, (own, held), 0)
        c = lax.broadcasted_iota(jnp.int32, (own, held), 1)
        pick = jnp.where(c == r + lax.rem(a, A2) * own, 1.0, 0.0)
        rows = lax.dot_general(pick, filt_in[...], NT, precision=highest, preferred_element_type=f32)
        gain = jnp.dot(rows, select[...], precision=highest, preferred_element_type=f32)

        lax.fori_loop(A * inner[-1], A * (B - inner[-1]), first_wait, 0)
        acc = [
            jnp.dot(t, table[rows_of(inner), widths(i)], preferred_element_type=f32)
            for i, t in enumerate(folded(inner))
        ]
        lax.fori_loop(0, A * inner[-1], first_wait, 0)
        lax.fori_loop(A * (B - inner[-1]), devices, first_wait, 0)
        for i, t in enumerate(folded(outer)):
            acc[i] = acc[i] + jnp.dot(t, table[rows_of(outer), widths(i)], preferred_element_type=f32)
        coef = [(acc[i] * gain[:, starts[i] : starts[i + 1]]).astype(bf16) for i in range(4)]

        for bs in (outer, inner):
            grid = [
                lax.dot_general(coef[i], table[rows_of(bs), widths(i)], NT, preferred_element_type=f32)
                for i in range(4)
            ]
            for n, bi in enumerate(bs):
                for ai in range(0, A2, 2):
                    at_lane = (n * A2 + ai) * half
                    pp, mp, pm, mm = [g[:, at_lane : at_lane + 2 * half] for g in grid]
                    e0, e1, o0, o1 = pp + mp, pp - mp, pm + mm, pm - mm
                    for i, j, value in [(0, 0, e0 + o0), (1, 0, e1 + o1), (0, 1, e0 - o0), (1, 1, e1 - o1)]:
                        upper = value[:up]
                        lower = jnp.concatenate([value[up:], blank], 0)
                        bj = B - 1 - bi if j else bi
                        a0, a1 = (A - 1 - ai, A - 2 - ai) if i else (ai, ai + 1)
                        out[index_of(a0, bj)] = jnp.where(left, upper, pltpu.roll(lower, half, 1)).astype(bf16)
                        out[index_of(a1, bj)] = jnp.where(left, pltpu.roll(upper, half, 1), lower).astype(bf16)

            count = 2 * len(bs) * A

            def second_send(step, carry):
                t = lax.rem(me + step, count)
                if bs == outer:
                    o = t + jnp.where(t >= count // 2, devices - count, 0)
                else:
                    o = t + A * bs[-1]

                @pl.when(o != me)
                def _():
                    second_copy(o).start()

                return carry

            lax.fori_loop(0, count, second_send, 0)
        dst[mine] = out[me]

    @pl.when(a == 0)
    def _():
        edge_in[0] = jnp.zeros(edge_in.shape[1:], bf16)
        corner_in[0] = jnp.zeros(corner_in.shape[1:], bf16)
        corner_in[1] = jnp.zeros(corner_in.shape[1:], bf16)

    @pl.when(a == A - 1)
    def _():
        edge_in[1] = jnp.zeros(edge_in.shape[1:], bf16)
        corner_in[2] = jnp.zeros(corner_in.shape[1:], bf16)
        corner_in[3] = jnp.zeros(corner_in.shape[1:], bf16)

    for da, db in neighbours:
        @pl.when(inside(-da))
        def _():
            halo_copy(da, db).wait_recv()

    fetch[5].wait()
    weight = taps[...]
    grid_rows = [edge_in[0].astype(f32)]
    grid_rows += [xf[pl.ds(lon_cols * r, lon_cols), :] for r in range(lat_rows)]
    grid_rows += [edge_in[1].astype(f32)]

    def corner(i):
        piece = corner_in[i].astype(f32)
        return jnp.concatenate([piece[c : c + 1] for c in range(chunks)], 1)

    west, east = edge_in[2].astype(f32), edge_in[3].astype(f32)
    west = [corner(0)] + [west[r : r + 1] for r in range(lat_rows)] + [corner(2)]
    east = [corner(1)] + [east[r : r + 1] for r in range(lat_rows)] + [corner(3)]
    sub = lax.broadcasted_iota(jnp.int32, (lon_cols, channels), 0)
    shifted = []
    for r in range(lat_rows + 2):
        here = grid_rows[r]
        before = jnp.where(sub == 0, west[r], pltpu.roll(here, 1, 0))
        after = jnp.where(sub == lon_cols - 1, east[r], pltpu.roll(here, lon_cols - 1, 0))
        shifted.append((before, here, after))
    for r in range(lat_rows):
        mix = sum(
            weight[3 * i + j : 3 * i + j + 1] * shifted[r + i][j] for i in range(3) for j in range(3)
        )
        mix = mix.astype(bf16).astype(f32)
        total[pl.ds(lon_cols * r, lon_cols), :] = grid_rows[r + 1] + mix

    for i in (6, 7, 8):
        fetch[i].wait()

    def second_wait(g, carry):
        @pl.when(g != mine)
        def _():
            pltpu.make_async_remote_copy(
                src_ref=out.at[0], dst_ref=dst.at[g], send_sem=send2.at[0], recv_sem=recv2.at[g],
                device_id=(lax.rem(g, A), first + lax.div(g, A)), device_id_type=MESH,
            ).wait_recv()

        return carry

    lax.fori_loop(0, workers, second_wait, 0)
    parts = []
    for g in range(workers):
        piece = dst[g].astype(f32)
        parts += [piece, pltpu.roll(piece, half, 1)[:low]]
    spectral = jnp.concatenate(parts, 0).astype(bf16)
    spectral = lax.dot_general(place_left, spectral, NT, preferred_element_type=f32)
    summed = (total[...] + spectral).astype(bf16).astype(f32)
    scale = lax.rsqrt(jnp.mean(summed * summed, axis=1, keepdims=True) + epsilon_norm)
    normed = (summed * scale * norm[...]).astype(bf16)
    hidden = jnp.dot(normed, win[...], preferred_element_type=f32)
    hidden = (0.5 * hidden * (1.0 + lax.erf(hidden * math.sqrt(0.5)))).astype(bf16)
    result = summed + jnp.dot(hidden, wout[...], preferred_element_type=f32)
    res[...] = result.astype(bf16)
    back = pltpu.make_async_copy(res, out_hbm, local_sem.at[0])
    back.start()

    def first_done(g, carry):
        @pl.when(g != mine)
        def _():
            first_copy(g).wait_send()

        return carry

    lax.fori_loop(0, workers, first_done, 0)

    @pl.when(gives)
    def _():
        filt_copy.wait_send()

    for da, db in neighbours:
        @pl.when(inside(da))
        def _():
            halo_copy(da, db).wait_send()

    @pl.when(worker)
    def _():
        def second_done(o, carry):
            @pl.when(o != me)
            def _():
                second_copy(o).wait_send()

            return carry

        lax.fori_loop(0, devices, second_done, 0)

    back.wait()

    @pl.when(jnp.logical_not(worker))
    def _():
        for i in (2, 3, 4):
            fetch[i].wait()


def sphere_block(lat_devices, lon_devices, latent_field, spectral_filter, conv_weight, norm_gain, weight_in, weight_out):
    channels, lat_rows, lon_cols = latent_field.shape
    points = lat_rows * lon_cols
    workers = lat_devices * lon_devices // 2
    own = channels // workers
    up = upper_rows(own)
    table, select, quad, starts = folded_tables(lat_devices, lon_devices, lat_rows, lon_cols)
    table = jnp.asarray(table.astype(jnp.bfloat16))
    args = [
        jnp.transpose(latent_field, (1, 2, 0)).reshape(points, channels),
        spectral_filter.T,
        conv_weight,
        norm_gain[None, :],
        weight_in,
        weight_out,
        table,
        jnp.asarray(select),
        jnp.asarray(quad),
    ]
    order = [0, 1, 2, 3, 4, 5, 6, 7, 8]
    copies = [pltpu.VMEM(args[i].shape, args[i].dtype) for i in order]
    devices = lat_devices * lon_devices
    bf16, f32, dma = jnp.bfloat16, jnp.float32, pltpu.SemaphoreType.DMA
    scratch = [
        pltpu.VMEM((points, channels), f32),
        pltpu.VMEM((workers, up, 128), bf16),
        pltpu.VMEM((devices, up, 128), bf16),
        pltpu.VMEM((devices, up, 128), bf16),
        pltpu.VMEM((workers, up, 128), bf16),
        pltpu.VMEM(args[1].shape, f32),
        pltpu.VMEM((2, lat_rows, channels), bf16),
        pltpu.VMEM((4, 8, 128), bf16),
        pltpu.VMEM((4, lat_rows, channels), bf16),
        pltpu.VMEM((4, 8, 128), bf16),
        pltpu.VMEM((points, channels), f32),
        pltpu.VMEM((points, channels), bf16),
        dma((9,)), dma((workers,)), dma((devices,)), dma((devices,)), dma((workers,)),
        dma((8,)), dma((8,)), dma, dma,
    ]
    result = pl.pallas_call(
        functools.partial(block_kernel, lat_devices, lon_devices, lat_rows, lon_cols, starts),
        out_shape=jax.ShapeDtypeStruct((points, channels), bf16),
        in_specs=[pl.BlockSpec(memory_space=pl.ANY)] * 9,
        out_specs=pl.BlockSpec(memory_space=pl.ANY),
        scratch_shapes=copies + scratch,
        compiler_params=pltpu.CompilerParams(collective_id=0, has_side_effects=True),
        name="sphere_block",
    )(*args)
    return jnp.transpose(result.reshape(lat_rows, lon_cols, channels), (2, 0, 1))


def fits_block(lat_devices, lon_devices, latent_field):
    channels, lat_rows, lon_cols = latent_field.shape
    workers = lat_devices * lon_devices // 2
    return (
        lat_devices % 4 == 0
        and lon_devices % 4 == 0
        and lat_rows == 8
        and lon_cols == 8
        and channels % (8 * workers) == 0
        and channels % 128 == 0
        and channels <= 1024
    )


def block_or_banded(lat_devices, lon_devices, *arguments):
    if fits_block(lat_devices, lon_devices, arguments[0]):
        return sphere_block(lat_devices, lon_devices, *arguments)
    return on_device(*arguments)


def solution(mesh):
    return jax.shard_map(
        functools.partial(block_or_banded, mesh.shape["lat"], mesh.shape["lon"]),
        mesh=mesh,
        in_specs=(P(None, "lat", "lon"), P("lon", None), P(), P(), P(), P()),
        out_specs=P(None, "lat", "lon"),
        check_vma=False,
    )
```

```python
import functools
import math

import jax
import jax.numpy as jnp
import numpy as np
from jax import lax
from jax.experimental import pallas as pl
from jax.experimental.pallas import tpu as pltpu
from jax.sharding import PartitionSpec as P

highest = lax.Precision.HIGHEST
epsilon_norm = 1e-06


def with_halo(cells, sides, width):
    for axis, dim in sides:
        count = lax.axis_size(axis)
        ends = count - 1
        head = lax.slice_in_dim(cells, 0, width, axis=dim)
        tail = lax.slice_in_dim(cells, cells.shape[dim] - width, cells.shape[dim], axis=dim)
        cells = jnp.concatenate(
            [
                lax.ppermute(tail, axis, [(i, (i + 1) % count) for i in range(ends)]),
                cells,
                lax.ppermute(head, axis, [((i + 1) % count, i) for i in range(ends)]),
            ],
            axis=dim,
        )
    return cells


def quadrature(lat_count):
    colatitude = (jnp.arange(lat_count, dtype=jnp.float32) + 0.5) * (math.pi / lat_count)
    return jnp.sin(colatitude) * (math.pi / lat_count)


def fourier_tables(lon_count, mode_count):
    wave_index = (
        jnp.arange(mode_count, dtype=jnp.int32)[:, None]
        * jnp.arange(lon_count, dtype=jnp.int32)[None, :]
    )
    phase_angle = (wave_index % lon_count).astype(jnp.float32) * (2.0 * math.pi / lon_count)
    cosine = jnp.cos(phase_angle)
    sine_table = jnp.sin(phase_angle)
    angle_step = 2.0 * math.pi / lon_count
    forward = jnp.concatenate([angle_step * cosine, -angle_step * sine_table], axis=0)
    weight = jnp.where(jnp.arange(mode_count, dtype=jnp.int32) == 0, 1.0, 2.0).astype(jnp.float32)[
        :, None
    ]
    inverse = jnp.concatenate([weight * cosine, -weight * sine_table], axis=0)
    return (forward, inverse)


def legendre_rows(order_ids, lat_count):
    colatitude = (jnp.arange(lat_count, dtype=jnp.float32) + 0.5) * (math.pi / lat_count)
    cosine = jnp.cos(colatitude)
    sine_col = jnp.sin(colatitude)
    order_f = order_ids.astype(jnp.float32)
    factor_index = jnp.arange(1, lat_count, dtype=jnp.float32)
    ratio_log = jnp.log((2.0 * factor_index - 1.0) / (2.0 * factor_index))
    included = (factor_index[None, :] <= order_f[:, None]).astype(jnp.float32)
    log_factor = jnp.sum(included * ratio_log[None, :], axis=1)
    start_log = 0.5 * jnp.log((2.0 * order_f + 1.0) / (4.0 * math.pi)) + 0.5 * log_factor
    start_log = start_log[:, None] + order_f[:, None] * jnp.log(sine_col)[None, :]
    blank_rows = jnp.zeros((order_ids.shape[0], lat_count), jnp.float32)
    order_col = order_f[:, None]

    def advance(state_carry, degree):
        before, current, scale_log = state_carry
        degree_f = degree.astype(jnp.float32)
        alpha_term = jnp.sqrt(
            (4.0 * degree_f * degree_f - 1.0)
            / jnp.maximum(degree_f * degree_f - order_col * order_col, 1.0)
        )
        beta_term = jnp.sqrt(
            jnp.maximum((degree_f - 1.0) ** 2 - order_col * order_col, 0.0)
            / jnp.maximum(4.0 * (degree_f - 1.0) ** 2 - 1.0, 1.0)
        )
        stepped = alpha_term * (cosine[None, :] * current - beta_term * before)
        at_start = order_ids[:, None] == degree
        past_start = order_ids[:, None] < degree
        fresh_value = jnp.where(at_start, 1.0, jnp.where(past_start, stepped, 0.0))
        fresh_log = jnp.where(at_start, start_log, scale_log)
        entry_value = fresh_value * jnp.exp(fresh_log)
        rescale = jnp.where(
            past_start | at_start, jnp.maximum(jnp.abs(fresh_value), jnp.abs(current)), 1.0
        )
        return (
            (current / rescale, fresh_value / rescale, fresh_log + jnp.log(rescale)),
            entry_value,
        )

    degrees = jnp.arange(lat_count, dtype=jnp.int32)
    unused, legendre = lax.scan(advance, (blank_rows, blank_rows, blank_rows), degrees)
    return legendre


def filter_modes(banded, legendre, filter_block, quad_weights):
    coefficients = jnp.einsum(
        "lmj,pmcj->pmcl", legendre, banded * quad_weights[None, None, None, :], precision=highest
    )
    coefficients = coefficients * filter_block[None, None, :, :]
    return jnp.einsum("lmj,pmcl->pmcj", legendre, coefficients, precision=highest)


def wrap_columns(extended):
    return jnp.concatenate([extended[:, :, -1:], extended, extended[:, :, :1]], axis=2)


def depthwise_core(extended, kernel, lat_rows, lon_cols):
    accumulated = jnp.zeros((extended.shape[0], lat_rows, lon_cols), jnp.float32)
    for row_shift in range(3):
        for col_shift in range(3):
            piece = extended[
                :, row_shift : row_shift + lat_rows, col_shift : col_shift + lon_cols
            ].astype(jnp.float32)
            accumulated = accumulated + kernel[3 * row_shift + col_shift][:, None, None] * piece
    return accumulated.astype(jnp.bfloat16)


def channel_mlp(summed_low, norm_gain, weight_in, weight_out):
    summed = summed_low.astype(jnp.float32)
    scale_inv = lax.rsqrt(jnp.mean(summed * summed, axis=0, keepdims=True) + epsilon_norm)
    normed = (summed * scale_inv * norm_gain[:, None]).astype(jnp.bfloat16)
    hidden = lax.dot_general(
        weight_in, normed, (((0,), (0,)), ((), ())), preferred_element_type=jnp.float32
    )
    hidden = jax.nn.gelu(hidden, approximate=False).astype(jnp.bfloat16)
    result = summed + lax.dot_general(
        weight_out, hidden, (((0,), (0,)), ((), ())), preferred_element_type=jnp.float32
    )
    return result.astype(jnp.bfloat16)


def add_three(first, second, third):
    total = first.astype(jnp.float32) + second.astype(jnp.float32) + third.astype(jnp.float32)
    return total.astype(jnp.bfloat16)


def on_device(latent_field, spectral_filter, conv_weight, norm_gain, weight_in, weight_out):
    channels, lat_rows, lon_cols = latent_field.shape
    sector_count = lax.axis_size("lon")
    lat_count = lat_rows * lax.axis_size("lat")
    lon_count = lon_cols * sector_count
    chan_block = channels // sector_count
    spread = lax.all_to_all(latent_field, "lon", split_axis=0, concat_axis=2, tiled=True)
    forward, inverse = fourier_tables(lon_count, lat_count)
    flattened = spread.astype(jnp.float32).reshape(chan_block * lat_rows, lon_count)
    spectrum = lax.dot_general(forward, flattened, (((1,), (1,)), ((), ())), precision=highest)
    spectrum = spectrum.reshape(2, lat_count, chan_block, lat_rows)
    banded = lax.all_to_all(spectrum, "lat", split_axis=1, concat_axis=3, tiled=True)
    order_ids = lax.axis_index("lat") * lat_rows + jnp.arange(lat_rows, dtype=jnp.int32)
    legendre = legendre_rows(order_ids, lat_count)
    synthesized = filter_modes(banded, legendre, spectral_filter, quadrature(lat_count))
    regathered = lax.all_to_all(synthesized, "lat", split_axis=3, concat_axis=1, tiled=True)
    regridded = lax.dot_general(
        regathered.reshape(2 * lat_count, chan_block * lat_rows),
        inverse,
        (((0,), (0,)), ((), ())),
        precision=highest,
    )
    spectral = regridded.reshape(chan_block, lat_rows, lon_count).astype(jnp.bfloat16)
    own_kernel = lax.dynamic_slice_in_dim(
        conv_weight, lax.axis_index("lon") * chan_block, chan_block, 1
    )
    rimmed = with_halo(spread, (("lat", 1),), 1)
    sector_mix = depthwise_core(wrap_columns(rimmed), own_kernel, lat_rows, lon_count)
    sector_sum = add_three(spread, spectral, sector_mix)
    summed = lax.all_to_all(sector_sum, "lon", split_axis=2, concat_axis=0, tiled=True)
    summed = summed.reshape(channels, lat_rows * lon_cols)
    result = channel_mlp(summed, norm_gain, weight_in, weight_out)
    return result.reshape(channels, lat_rows, lon_cols)


CLASSES = ((0, 0), (1, 0), (0, 1), (1, 1))


def folded_tables(lat_devices, lon_devices, lat_rows, lon_cols):
    lat_count, lon_count = lat_devices * lat_rows, lon_devices * lon_cols
    theta = (np.arange(lat_count // 2) + 0.5) * (math.pi / lat_count)
    x, s = np.cos(theta), np.sin(theta)
    phi = 2.0 * math.pi * (np.arange(lon_count // 2) + 0.5) / lon_count
    row, column = [], []
    for b in reversed(range(lon_devices // 2)):
        for a in range(lat_devices // 2):
            row.append(np.repeat(a * lat_rows + np.arange(lat_rows), lon_cols))
            column.append(np.tile(b * lon_cols + np.arange(lon_cols), lat_rows))
    row, column = np.concatenate(row), np.concatenate(column)
    columns = {key: [] for key in CLASSES}
    degrees = {key: [] for key in CLASSES}
    weights = {key: [] for key in CLASSES}
    for m in range(lat_count):
        k = np.arange(1, m + 1)
        log_start = 0.5 * (
            np.log((2 * m + 1) / (4 * math.pi)) + np.sum(np.log((2 * k - 1) / (2 * k)))
        )
        before, current = np.zeros(lat_count // 2), np.exp(log_start + m * np.log(s))
        for l in range(m, lat_count):
            if l > m:
                a = math.sqrt((4.0 * l * l - 1) / (l * l - m * m))
                b = math.sqrt(((l - 1.0) ** 2 - m * m) / (4.0 * (l - 1) ** 2 - 1))
                before, current = current, a * (x * current - b * before)
            for phase, wave in enumerate([np.cos(m * phi), -np.sin(m * phi)][: 1 if m == 0 else 2]):
                key = ((l + m) % 2, phase)
                columns[key].append(current[row] * wave[column])
                degrees[key].append(l)
                weights[key].append((1.0 if m == 0 else 2.0) * 2.0 * math.pi / lon_count)
    tables, selects, starts = [], [], [0]
    for key in CLASSES:
        width = -(-len(columns[key]) // 128) * 128
        fill = width - len(columns[key])
        tables.append(np.pad(np.stack(columns[key], 1), ((0, 0), (0, fill))))
        select = np.arange(lat_count)[:, None] == np.array(degrees[key])[None, :]
        selects.append(np.pad(select * np.array(weights[key])[None, :], ((0, 0), (0, fill))))
        starts.append(starts[-1] + width)
    quad = s * (math.pi / lat_count)
    quad = np.repeat(quad.reshape(lat_devices // 2, lat_rows), lon_cols, axis=1)
    return (
        np.concatenate(tables, 1),
        np.concatenate(selects, 1).astype(np.float32),
        np.tile(quad, (1, 2)).astype(np.float32),
        tuple(starts),
    )


MESH = pl.DeviceIdType.MESH
NT = (((1,), (1,)), ((), ()))


def block_kernel(
    lat_devices, lon_devices, lat_rows, lon_cols, starts,
    x_hbm, filter_hbm, taps_hbm, norm_hbm, win_hbm, table_hbm, select_hbm, quad_hbm,
    out_hbm, hid_hbm,
    xb, filt, taps, norm, win, table, select, quad,
    xf, src, mid, out, dst, filt_in, edge_out, corner_out, edge_in, corner_in, total, res, hid,
    local_sem, send1, recv1, send2, recv2, halo_send, halo_recv, filt_send, filt_recv,
):
    A, B = lat_devices, lon_devices
    A2, B2, first = A // 2, B // 2, B // 4
    workers = A * B2
    devices = A * B
    points, channels = xb.shape
    own = channels // workers
    rows = own // 2
    whole = rows // 8 * 8
    half = points
    a, b = lax.axis_index("lat"), lax.axis_index("lon")
    me = b * A + a
    worker = jnp.logical_and(b >= first, b < first + B2)
    mine = jnp.where(worker, (b - first) * A + a, -1)
    f32, bf16 = jnp.float32, jnp.bfloat16

    fetch = [
        pltpu.make_async_copy(s, d, local_sem.at[i])
        for i, (s, d) in enumerate(
            [(x_hbm, xb), (filter_hbm, filt), (quad_hbm, quad), (table_hbm, table), (select_hbm, select),
             (taps_hbm, taps), (norm_hbm, norm), (win_hbm, win)]
        )
    ]
    fetch[0].start()
    barrier = pltpu.get_barrier_semaphore()
    neighbours = [(da, db) for da in (-1, 0, 1) for db in (-1, 0, 1) if (da, db) != (0, 0)]

    def inside(da):
        return jnp.logical_and(a + da >= 0, a + da < A)

    def at(da, db):
        return (a + da, lax.rem(b + db + B, B))

    @pl.when(worker)
    def _():
        def greet(peer, carry):
            @pl.when(peer != me)
            def _():
                pl.semaphore_signal(
                    barrier, inc=1, device_id=(lax.rem(peer, A), lax.div(peer, A)), device_id_type=MESH
                )

            return carry

        lax.fori_loop(0, devices, greet, 0)

    @pl.when(jnp.logical_not(worker))
    def _():
        for da, db in neighbours:
            @pl.when(inside(da))
            def _():
                pl.semaphore_signal(barrier, inc=1, device_id=at(da, db), device_id_type=MESH)

    for copy in fetch[1:]:
        copy.start()

    turn_lat, turn_lon = a >= A2, b >= B2
    p_row = lax.broadcasted_iota(jnp.int32, (points, 2 * half), 0)
    p_col = lax.broadcasted_iota(jnp.int32, (points, 2 * half), 1)

    def turned(index):
        jl, kl = lax.div(index, lon_cols), lax.rem(index, lon_cols)
        jl = jnp.where(turn_lat, lat_rows - 1 - jl, jl)
        kl = jnp.where(turn_lon, lon_cols - 1 - kl, kl)
        return jl * lon_cols + kl

    place = jnp.where(p_row == turned(lax.rem(p_col, half)), 1.0, 0.0)
    place_both = place.astype(bf16)
    place_left = jnp.where(p_col < half, place, 0.0).astype(bf16)
    left = lax.broadcasted_iota(jnp.int32, (rows, 2 * half), 1) < half

    def halves(value):
        if rows == whole:
            return value[:rows], value[rows:]
        rest = value[2 * whole :]
        return (
            jnp.concatenate([value[:whole], rest[: rows - whole]], 0),
            jnp.concatenate([value[whole : 2 * whole], rest[rows - whole :]], 0),
        )

    def joined(upper, lower):
        pieces = [upper[:whole], lower[:whole]]
        if rows > whole:
            pieces += [upper[whole:], lower[whole:]]
        return pieces

    fetch[0].wait()
    xf[...] = xb[...].astype(f32)
    xt = jnp.transpose(xf[...], (1, 0)).astype(bf16)
    xt = jnp.dot(xt, place_both, preferred_element_type=f32)
    for g in range(workers):
        upper, lower = halves(xt[own * g : own * (g + 1)])
        src[g] = jnp.where(left, upper, lower).astype(bf16)

    west, east = [
        jnp.concatenate([xf[k + lon_cols * r : k + lon_cols * r + 1] for r in range(lat_rows)], 0)
        for k in (0, lon_cols - 1)
    ]
    edge_out[0] = west.astype(bf16)
    edge_out[1] = east.astype(bf16)
    chunks = channels // 128
    for i, (r, side) in enumerate([(0, west), (0, east), (lat_rows - 1, west), (lat_rows - 1, east)]):
        parts = [side[r : r + 1, 128 * c : 128 * (c + 1)] for c in range(chunks)]
        parts.append(jnp.zeros((8 - chunks, 128), f32))
        corner_out[i] = jnp.concatenate(parts, 0).astype(bf16)

    def outside(db):
        other = lax.rem(b + db + B, B)
        return jnp.where(jnp.logical_and(other >= first, other < first + B2), 0, 1)

    rims = jnp.where(a > 0, 1, 0) + jnp.where(a < A - 1, 1, 0)
    greetings = jnp.where(worker, workers - 1, workers)
    greetings = greetings + rims * outside(0) + (1 + rims) * (outside(-1) + outside(1))
    pl.semaphore_wait(barrier, greetings)

    zone = jnp.where(b < first, 0, jnp.where(worker, 1, 2))

    def first_copy(g):
        return pltpu.make_async_remote_copy(
            src_ref=src.at[g], dst_ref=mid.at[me], send_sem=send1, recv_sem=recv1.at[zone],
            device_id=(lax.rem(g, A), first + lax.div(g, A)), device_id_type=MESH,
        )

    @pl.when(worker)
    def _():
        pltpu.make_async_copy(src.at[mine], mid.at[me], recv1.at[1]).start()

    def first_send(step, carry):
        g = workers - 1 - step

        @pl.when(g != mine)
        def _():
            first_copy(g).start()

        return carry

    lax.fori_loop(0, workers, first_send, 0)

    fetch[1].wait()
    owner_row = lax.div(a, A2) == lax.rem(b, 2)
    filt_lon = first + lax.div(b, 2)
    keeps = jnp.logical_and(owner_row, filt_lon == b)
    gives = jnp.logical_and(owner_row, filt_lon != b)
    filt_copy = pltpu.make_async_remote_copy(
        src_ref=filt, dst_ref=filt_in, send_sem=filt_send, recv_sem=filt_recv,
        device_id=(a, filt_lon), device_id_type=MESH,
    )

    @pl.when(gives)
    def _():
        filt_copy.start()

    @pl.when(keeps)
    def _():
        filt_in[...] = filt[...]

    def halo_copy(da, db):
        if db == 0:
            row = 0 if da < 0 else points - lon_cols
            source, target = xb.at[pl.ds(row, lon_cols)], edge_in.at[1 if da < 0 else 0]
            kind = 0
        elif da == 0:
            slot = 3 if db < 0 else 2
            source, target = edge_out.at[0 if db < 0 else 1], edge_in.at[slot]
            kind = 0
        else:
            index = (0 if da < 0 else 2) + (0 if db < 0 else 1)
            source, target = corner_out.at[index], corner_in.at[3 - index]
            kind = 1
        return pltpu.make_async_remote_copy(
            src_ref=source, dst_ref=target, send_sem=halo_send.at[kind], recv_sem=halo_recv.at[kind],
            device_id=at(da, db), device_id_type=MESH,
        )

    for da, db in neighbours:
        @pl.when(inside(da))
        def _():
            halo_copy(da, db).start()

    def index_of(ai, bi):
        return bi * A + ai

    def arrived(zone, start, count):
        blocks = mid.at[pl.ds(start, count)]
        pltpu.make_async_copy(blocks, blocks, recv1.at[zone]).wait()

    def widths(c):
        return pl.ds(starts[c], starts[c + 1] - starts[c])

    def folded(bs):
        tiles = [[] for _ in CLASSES]
        for bi in bs:
            parts = []
            for ai in range(A2):
                f00, f10, f01, f11 = [
                    mid[index_of(i, j)].astype(f32)
                    for i, j in [(ai, bi), (A - 1 - ai, bi), (ai, B - 1 - bi), (A - 1 - ai, B - 1 - bi)]
                ]
                s0, d0, s1, d1 = f00 + f10, f00 - f10, f01 + f11, f01 - f11
                w = quad[ai : ai + 1, :]
                parts.append([(s0 + s1) * w, (d0 + d1) * w, (s0 - s1) * w, (d0 - d1) * w])
            for ai in range(0, A2, 2):
                for c in range(4):
                    u, v = parts[ai][c], parts[ai + 1][c]
                    upper = jnp.where(left, u, pltpu.roll(v, half, 1))
                    lower = jnp.where(left, pltpu.roll(u, half, 1), v)
                    tiles[c].append(jnp.concatenate(joined(upper, lower), 0).astype(bf16))
        return [jnp.concatenate(t, 1) for t in tiles]

    inner = tuple(reversed(range(B2 // 2, B2)))
    outer = tuple(reversed(range(B2 // 2)))
    rows_of = lambda bs: pl.ds((B2 - 1 - bs[0]) * A2 * half, len(bs) * A2 * half)

    def second_copy(o):
        return pltpu.make_async_remote_copy(
            src_ref=out.at[o], dst_ref=dst.at[mine], send_sem=send2, recv_sem=recv2,
            device_id=(lax.rem(o, A), lax.div(o, A)), device_id_type=MESH,
        )

    @pl.when(worker)
    def _():
        for i in (2, 3, 4):
            fetch[i].wait()

        @pl.when(jnp.logical_not(keeps))
        def _():
            pltpu.make_async_remote_copy(
                src_ref=filt, dst_ref=filt_in, send_sem=filt_send, recv_sem=filt_recv,
                device_id=(a, 2 * (b - first) + lax.div(a, A2)), device_id_type=MESH,
            ).wait_recv()

        held = filt_in.shape[1]
        r = lax.broadcasted_iota(jnp.int32, (own, held), 0)
        c = lax.broadcasted_iota(jnp.int32, (own, held), 1)
        pick = jnp.where(c == r + lax.rem(a, A2) * own, 1.0, 0.0)
        rows = lax.dot_general(pick, filt_in[...], NT, precision=highest, preferred_element_type=f32)
        gain = jnp.dot(rows, select[...], precision=highest, preferred_element_type=f32)

        arrived(1, A * first, A * B2)
        acc = [
            jnp.dot(t, table[rows_of(inner), widths(i)], preferred_element_type=f32)
            for i, t in enumerate(folded(inner))
        ]
        arrived(0, 0, A * first)
        arrived(2, A * (first + B2), A * (B - first - B2))
        for i, t in enumerate(folded(outer)):
            acc[i] = acc[i] + jnp.dot(t, table[rows_of(outer), widths(i)], preferred_element_type=f32)
        coef = [(acc[i] * gain[:, starts[i] : starts[i + 1]]).astype(bf16) for i in range(4)]

        for bs in (outer, inner):
            grid = [
                lax.dot_general(coef[i], table[rows_of(bs), widths(i)], NT, preferred_element_type=f32)
                for i in range(4)
            ]
            for n, bi in enumerate(bs):
                for ai in range(0, A2, 2):
                    at_lane = (n * A2 + ai) * half
                    pp, mp, pm, mm = [g[:, at_lane : at_lane + 2 * half] for g in grid]
                    e0, e1, o0, o1 = pp + mp, pp - mp, pm + mm, pm - mm
                    for i, j, value in [(0, 0, e0 + o0), (1, 0, e1 + o1), (0, 1, e0 - o0), (1, 1, e1 - o1)]:
                        upper, lower = halves(value)
                        bj = B - 1 - bi if j else bi
                        a0, a1 = (A - 1 - ai, A - 2 - ai) if i else (ai, ai + 1)
                        out[index_of(a0, bj)] = jnp.where(left, upper, pltpu.roll(lower, half, 1)).astype(bf16)
                        out[index_of(a1, bj)] = jnp.where(left, pltpu.roll(upper, half, 1), lower).astype(bf16)

            def second_send(o, carry):
                @pl.when(o != me)
                def _():
                    second_copy(o).start()

                return carry

            if bs == outer:
                lax.fori_loop(0, A * first, second_send, 0)
            else:
                lax.fori_loop(A * first, devices, second_send, 0)
        pltpu.make_async_copy(out.at[me], dst.at[mine], recv2).start()

    @pl.when(a == 0)
    def _():
        edge_in[0] = jnp.zeros(edge_in.shape[1:], bf16)
        corner_in[0] = jnp.zeros(corner_in.shape[1:], bf16)
        corner_in[1] = jnp.zeros(corner_in.shape[1:], bf16)

    @pl.when(a == A - 1)
    def _():
        edge_in[1] = jnp.zeros(edge_in.shape[1:], bf16)
        corner_in[2] = jnp.zeros(corner_in.shape[1:], bf16)
        corner_in[3] = jnp.zeros(corner_in.shape[1:], bf16)

    pole = rims == 1

    def halo_wait(sems):
        for edges, corners, case in [(3, 2, pole), (4, 4, jnp.logical_not(pole))]:
            @pl.when(case)
            def _():
                for kind, blocks in enumerate([edge_in.at[pl.ds(0, edges)], corner_in.at[pl.ds(0, corners)]]):
                    pltpu.make_async_copy(blocks, blocks, sems.at[kind]).wait()

    halo_wait(halo_recv)

    fetch[5].wait()
    weight = taps[...]
    grid_rows = [edge_in[0].astype(f32)]
    grid_rows += [xf[pl.ds(lon_cols * r, lon_cols), :] for r in range(lat_rows)]
    grid_rows += [edge_in[1].astype(f32)]

    def corner(i):
        piece = corner_in[i].astype(f32)
        return jnp.concatenate([piece[c : c + 1] for c in range(chunks)], 1)

    west, east = edge_in[2].astype(f32), edge_in[3].astype(f32)
    west = [corner(0)] + [west[r : r + 1] for r in range(lat_rows)] + [corner(2)]
    east = [corner(1)] + [east[r : r + 1] for r in range(lat_rows)] + [corner(3)]
    sub = lax.broadcasted_iota(jnp.int32, (lon_cols, channels), 0)
    shifted = []
    for r in range(lat_rows + 2):
        here = grid_rows[r]
        before = jnp.where(sub == 0, west[r], pltpu.roll(here, 1, 0))
        after = jnp.where(sub == lon_cols - 1, east[r], pltpu.roll(here, lon_cols - 1, 0))
        shifted.append((before, here, after))
    for r in range(lat_rows):
        mix = sum(
            weight[3 * i + j : 3 * i + j + 1] * shifted[r + i][j] for i in range(3) for j in range(3)
        )
        mix = mix.astype(bf16).astype(f32)
        total[pl.ds(lon_cols * r, lon_cols), :] = grid_rows[r + 1] + mix

    for i in (6, 7):
        fetch[i].wait()

    pltpu.make_async_copy(dst, dst, recv2).wait()
    parts = []
    for g in range(workers):
        piece = dst[g].astype(f32)
        parts += joined(piece, pltpu.roll(piece, half, 1))
    spectral = jnp.concatenate(parts, 0).astype(bf16)
    spectral = lax.dot_general(place_left, spectral, NT, preferred_element_type=f32)
    summed = (total[...] + spectral).astype(bf16).astype(f32)
    scale = lax.rsqrt(jnp.mean(summed * summed, axis=1, keepdims=True) + epsilon_norm)
    normed = (summed * scale * norm[...][None, :]).astype(bf16)
    hidden = jnp.dot(normed, win[...], preferred_element_type=f32)
    hidden = (0.5 * hidden * (1.0 + lax.erf(hidden * math.sqrt(0.5)))).astype(bf16)
    res[...] = summed.astype(bf16)
    hid[...] = hidden
    back = [
        pltpu.make_async_copy(res, out_hbm, local_sem.at[0]),
        pltpu.make_async_copy(hid, hid_hbm, local_sem.at[1]),
    ]
    for copy in back:
        copy.start()

    def left_already(blocks, sem):
        pltpu.make_async_copy(blocks, blocks, sem).wait()

    @pl.when(worker)
    def _():
        left_already(src.at[pl.ds(0, workers - 1)], send1)
        left_already(out.at[pl.ds(0, devices - 1)], send2)

    @pl.when(jnp.logical_not(worker))
    def _():
        left_already(src, send1)

    @pl.when(gives)
    def _():
        filt_copy.wait_send()

    halo_wait(halo_send)
    for copy in back:
        copy.wait()

    @pl.when(jnp.logical_not(worker))
    def _():
        for i in (2, 3, 4):
            fetch[i].wait()


def sphere_block(lat_devices, lon_devices, latent_field, spectral_filter, conv_weight, norm_gain, weight_in, weight_out):
    channels, lat_rows, lon_cols = latent_field.shape
    points = lat_rows * lon_cols
    workers = lat_devices * lon_devices // 2
    own = channels // workers
    table, select, quad, starts = folded_tables(lat_devices, lon_devices, lat_rows, lon_cols)
    table = jnp.asarray(table.astype(jnp.bfloat16))
    args = [
        jnp.transpose(latent_field, (1, 2, 0)).reshape(points, channels),
        spectral_filter.T,
        conv_weight,
        norm_gain,
        weight_in,
        table,
        jnp.asarray(select),
        jnp.asarray(quad),
    ]
    order = range(len(args))
    copies = [pltpu.VMEM(args[i].shape, args[i].dtype) for i in order]
    devices = lat_devices * lon_devices
    bf16, f32, dma = jnp.bfloat16, jnp.float32, pltpu.SemaphoreType.DMA
    scratch = [
        pltpu.VMEM((points, channels), f32),
        pltpu.VMEM((workers, own // 2, 128), bf16),
        pltpu.VMEM((devices, own // 2, 128), bf16),
        pltpu.VMEM((devices, own // 2, 128), bf16),
        pltpu.VMEM((workers, own // 2, 128), bf16),
        pltpu.VMEM(args[1].shape, f32),
        pltpu.VMEM((2, lat_rows, channels), bf16),
        pltpu.VMEM((4, 8, 128), bf16),
        pltpu.VMEM((4, lat_rows, channels), bf16),
        pltpu.VMEM((4, 8, 128), bf16),
        pltpu.VMEM((points, channels), f32),
        pltpu.VMEM((points, channels), bf16),
        pltpu.VMEM((points, weight_in.shape[1]), bf16),
        dma((len(args),)), dma, dma((3,)), dma, dma, dma((2,)), dma((2,)), dma, dma,
    ]
    summed, hidden = pl.pallas_call(
        functools.partial(block_kernel, lat_devices, lon_devices, lat_rows, lon_cols, starts),
        out_shape=[
            jax.ShapeDtypeStruct((points, channels), bf16),
            jax.ShapeDtypeStruct((points, weight_in.shape[1]), bf16),
        ],
        in_specs=[pl.BlockSpec(memory_space=pl.ANY)] * len(args),
        out_specs=[pl.BlockSpec(memory_space=pl.ANY)] * 2,
        scratch_shapes=copies + scratch,
        compiler_params=pltpu.CompilerParams(collective_id=0, has_side_effects=True),
        name="sphere_block",
    )(*args)
    result = jnp.dot(hidden, weight_out, preferred_element_type=f32)
    result = (summed.astype(f32) + result).astype(bf16)
    return jnp.transpose(result.reshape(lat_rows, lon_cols, channels), (2, 0, 1))


def fits_block(lat_devices, lon_devices, latent_field):
    channels, lat_rows, lon_cols = latent_field.shape
    workers = lat_devices * lon_devices // 2
    return (
        lat_devices % 4 == 0
        and lon_devices % 4 == 0
        and lat_rows == 8
        and lon_cols == 8
        and channels % (8 * workers) == 0
        and channels // workers % 2 == 0
        and channels % 128 == 0
        and channels <= 1024
    )


def block_or_banded(lat_devices, lon_devices, *arguments):
    if fits_block(lat_devices, lon_devices, arguments[0]):
        return sphere_block(lat_devices, lon_devices, *arguments)
    return on_device(*arguments)


def solution(mesh):
    return jax.shard_map(
        functools.partial(block_or_banded, mesh.shape["lat"], mesh.shape["lon"]),
        mesh=mesh,
        in_specs=(P(None, "lat", "lon"), P("lon", None), P(), P(), P(), P()),
        out_specs=P(None, "lat", "lon"),
        check_vma=False,
    )
```

```python
import functools
import math

import jax
import jax.numpy as jnp
import numpy as np
from jax import lax
from jax.experimental import pallas as pl
from jax.experimental.pallas import tpu as pltpu
from jax.sharding import PartitionSpec as P

highest = lax.Precision.HIGHEST
epsilon_norm = 1e-06


def with_halo(cells, sides, width):
    for axis, dim in sides:
        count = lax.axis_size(axis)
        ends = count - 1
        head = lax.slice_in_dim(cells, 0, width, axis=dim)
        tail = lax.slice_in_dim(cells, cells.shape[dim] - width, cells.shape[dim], axis=dim)
        cells = jnp.concatenate(
            [
                lax.ppermute(tail, axis, [(i, (i + 1) % count) for i in range(ends)]),
                cells,
                lax.ppermute(head, axis, [((i + 1) % count, i) for i in range(ends)]),
            ],
            axis=dim,
        )
    return cells


def quadrature(lat_count):
    colatitude = (jnp.arange(lat_count, dtype=jnp.float32) + 0.5) * (math.pi / lat_count)
    return jnp.sin(colatitude) * (math.pi / lat_count)


def fourier_tables(lon_count, mode_count):
    wave_index = (
        jnp.arange(mode_count, dtype=jnp.int32)[:, None]
        * jnp.arange(lon_count, dtype=jnp.int32)[None, :]
    )
    phase_angle = (wave_index % lon_count).astype(jnp.float32) * (2.0 * math.pi / lon_count)
    cosine = jnp.cos(phase_angle)
    sine_table = jnp.sin(phase_angle)
    angle_step = 2.0 * math.pi / lon_count
    forward = jnp.concatenate([angle_step * cosine, -angle_step * sine_table], axis=0)
    weight = jnp.where(jnp.arange(mode_count, dtype=jnp.int32) == 0, 1.0, 2.0).astype(jnp.float32)[
        :, None
    ]
    inverse = jnp.concatenate([weight * cosine, -weight * sine_table], axis=0)
    return (forward, inverse)


def legendre_rows(order_ids, lat_count):
    colatitude = (jnp.arange(lat_count, dtype=jnp.float32) + 0.5) * (math.pi / lat_count)
    cosine = jnp.cos(colatitude)
    sine_col = jnp.sin(colatitude)
    order_f = order_ids.astype(jnp.float32)
    factor_index = jnp.arange(1, lat_count, dtype=jnp.float32)
    ratio_log = jnp.log((2.0 * factor_index - 1.0) / (2.0 * factor_index))
    included = (factor_index[None, :] <= order_f[:, None]).astype(jnp.float32)
    log_factor = jnp.sum(included * ratio_log[None, :], axis=1)
    start_log = 0.5 * jnp.log((2.0 * order_f + 1.0) / (4.0 * math.pi)) + 0.5 * log_factor
    start_log = start_log[:, None] + order_f[:, None] * jnp.log(sine_col)[None, :]
    blank_rows = jnp.zeros((order_ids.shape[0], lat_count), jnp.float32)
    order_col = order_f[:, None]

    def advance(state_carry, degree):
        before, current, scale_log = state_carry
        degree_f = degree.astype(jnp.float32)
        alpha_term = jnp.sqrt(
            (4.0 * degree_f * degree_f - 1.0)
            / jnp.maximum(degree_f * degree_f - order_col * order_col, 1.0)
        )
        beta_term = jnp.sqrt(
            jnp.maximum((degree_f - 1.0) ** 2 - order_col * order_col, 0.0)
            / jnp.maximum(4.0 * (degree_f - 1.0) ** 2 - 1.0, 1.0)
        )
        stepped = alpha_term * (cosine[None, :] * current - beta_term * before)
        at_start = order_ids[:, None] == degree
        past_start = order_ids[:, None] < degree
        fresh_value = jnp.where(at_start, 1.0, jnp.where(past_start, stepped, 0.0))
        fresh_log = jnp.where(at_start, start_log, scale_log)
        entry_value = fresh_value * jnp.exp(fresh_log)
        rescale = jnp.where(
            past_start | at_start, jnp.maximum(jnp.abs(fresh_value), jnp.abs(current)), 1.0
        )
        return (
            (current / rescale, fresh_value / rescale, fresh_log + jnp.log(rescale)),
            entry_value,
        )

    degrees = jnp.arange(lat_count, dtype=jnp.int32)
    unused, legendre = lax.scan(advance, (blank_rows, blank_rows, blank_rows), degrees)
    return legendre


def filter_modes(banded, legendre, filter_block, quad_weights):
    coefficients = jnp.einsum(
        "lmj,pmcj->pmcl", legendre, banded * quad_weights[None, None, None, :], precision=highest
    )
    coefficients = coefficients * filter_block[None, None, :, :]
    return jnp.einsum("lmj,pmcl->pmcj", legendre, coefficients, precision=highest)


def wrap_columns(extended):
    return jnp.concatenate([extended[:, :, -1:], extended, extended[:, :, :1]], axis=2)


def depthwise_core(extended, kernel, lat_rows, lon_cols):
    accumulated = jnp.zeros((extended.shape[0], lat_rows, lon_cols), jnp.float32)
    for row_shift in range(3):
        for col_shift in range(3):
            piece = extended[
                :, row_shift : row_shift + lat_rows, col_shift : col_shift + lon_cols
            ].astype(jnp.float32)
            accumulated = accumulated + kernel[3 * row_shift + col_shift][:, None, None] * piece
    return accumulated.astype(jnp.bfloat16)


def channel_mlp(summed_low, norm_gain, weight_in, weight_out):
    summed = summed_low.astype(jnp.float32)
    scale_inv = lax.rsqrt(jnp.mean(summed * summed, axis=0, keepdims=True) + epsilon_norm)
    normed = (summed * scale_inv * norm_gain[:, None]).astype(jnp.bfloat16)
    hidden = lax.dot_general(
        weight_in, normed, (((0,), (0,)), ((), ())), preferred_element_type=jnp.float32
    )
    hidden = jax.nn.gelu(hidden, approximate=False).astype(jnp.bfloat16)
    result = summed + lax.dot_general(
        weight_out, hidden, (((0,), (0,)), ((), ())), preferred_element_type=jnp.float32
    )
    return result.astype(jnp.bfloat16)


def add_three(first, second, third):
    total = first.astype(jnp.float32) + second.astype(jnp.float32) + third.astype(jnp.float32)
    return total.astype(jnp.bfloat16)


def on_device(latent_field, spectral_filter, conv_weight, norm_gain, weight_in, weight_out):
    channels, lat_rows, lon_cols = latent_field.shape
    sector_count = lax.axis_size("lon")
    lat_count = lat_rows * lax.axis_size("lat")
    lon_count = lon_cols * sector_count
    chan_block = channels // sector_count
    spread = lax.all_to_all(latent_field, "lon", split_axis=0, concat_axis=2, tiled=True)
    forward, inverse = fourier_tables(lon_count, lat_count)
    flattened = spread.astype(jnp.float32).reshape(chan_block * lat_rows, lon_count)
    spectrum = lax.dot_general(forward, flattened, (((1,), (1,)), ((), ())), precision=highest)
    spectrum = spectrum.reshape(2, lat_count, chan_block, lat_rows)
    banded = lax.all_to_all(spectrum, "lat", split_axis=1, concat_axis=3, tiled=True)
    order_ids = lax.axis_index("lat") * lat_rows + jnp.arange(lat_rows, dtype=jnp.int32)
    legendre = legendre_rows(order_ids, lat_count)
    synthesized = filter_modes(banded, legendre, spectral_filter, quadrature(lat_count))
    regathered = lax.all_to_all(synthesized, "lat", split_axis=3, concat_axis=1, tiled=True)
    regridded = lax.dot_general(
        regathered.reshape(2 * lat_count, chan_block * lat_rows),
        inverse,
        (((0,), (0,)), ((), ())),
        precision=highest,
    )
    spectral = regridded.reshape(chan_block, lat_rows, lon_count).astype(jnp.bfloat16)
    own_kernel = lax.dynamic_slice_in_dim(
        conv_weight, lax.axis_index("lon") * chan_block, chan_block, 1
    )
    rimmed = with_halo(spread, (("lat", 1),), 1)
    sector_mix = depthwise_core(wrap_columns(rimmed), own_kernel, lat_rows, lon_count)
    sector_sum = add_three(spread, spectral, sector_mix)
    summed = lax.all_to_all(sector_sum, "lon", split_axis=2, concat_axis=0, tiled=True)
    summed = summed.reshape(channels, lat_rows * lon_cols)
    result = channel_mlp(summed, norm_gain, weight_in, weight_out)
    return result.reshape(channels, lat_rows, lon_cols)


CLASSES = ((0, 0), (1, 0), (0, 1), (1, 1))


def folded_tables(lat_devices, lon_devices, lat_rows, lon_cols):
    lat_count, lon_count = lat_devices * lat_rows, lon_devices * lon_cols
    theta = (np.arange(lat_count // 2) + 0.5) * (math.pi / lat_count)
    x, s = np.cos(theta), np.sin(theta)
    phi = 2.0 * math.pi * (np.arange(lon_count // 2) + 0.5) / lon_count
    row, column = [], []
    for b in reversed(range(lon_devices // 2)):
        for a in range(lat_devices // 2):
            row.append(np.repeat(a * lat_rows + np.arange(lat_rows), lon_cols))
            column.append(np.tile(b * lon_cols + np.arange(lon_cols), lat_rows))
    row, column = np.concatenate(row), np.concatenate(column)
    columns = {key: [] for key in CLASSES}
    degrees = {key: [] for key in CLASSES}
    weights = {key: [] for key in CLASSES}
    for m in range(lat_count):
        k = np.arange(1, m + 1)
        log_start = 0.5 * (
            np.log((2 * m + 1) / (4 * math.pi)) + np.sum(np.log((2 * k - 1) / (2 * k)))
        )
        before, current = np.zeros(lat_count // 2), np.exp(log_start + m * np.log(s))
        for l in range(m, lat_count):
            if l > m:
                a = math.sqrt((4.0 * l * l - 1) / (l * l - m * m))
                b = math.sqrt(((l - 1.0) ** 2 - m * m) / (4.0 * (l - 1) ** 2 - 1))
                before, current = current, a * (x * current - b * before)
            for phase, wave in enumerate([np.cos(m * phi), -np.sin(m * phi)][: 1 if m == 0 else 2]):
                key = ((l + m) % 2, phase)
                columns[key].append(current[row] * wave[column])
                degrees[key].append(l)
                weights[key].append((1.0 if m == 0 else 2.0) * 2.0 * math.pi / lon_count)
    tables, selects, starts = [], [], [0]
    for key in CLASSES:
        width = -(-len(columns[key]) // 128) * 128
        fill = width - len(columns[key])
        tables.append(np.pad(np.stack(columns[key], 1), ((0, 0), (0, fill))))
        select = np.arange(lat_count)[:, None] == np.array(degrees[key])[None, :]
        selects.append(np.pad(select * np.array(weights[key])[None, :], ((0, 0), (0, fill))))
        starts.append(starts[-1] + width)
    quad = s * (math.pi / lat_count)
    quad = np.repeat(quad.reshape(lat_devices // 2, lat_rows), lon_cols, axis=1)
    return (
        np.concatenate(tables, 1),
        np.concatenate(selects, 1).astype(np.float32),
        np.tile(quad, (1, 2)).astype(np.float32),
        tuple(starts),
    )


MESH = pl.DeviceIdType.MESH


def worker_columns(lon_devices):
    return lon_devices // 4, lon_devices // 2


NT = (((1,), (1,)), ((), ()))


def block_kernel(
    lat_devices, lon_devices, lat_rows, lon_cols, starts,
    x_hbm, filter_hbm, taps_hbm, norm_hbm, win_hbm, wout_hbm, table_hbm, select_hbm, quad_hbm,
    res,
    xb, filt, taps, norm, win, wout, table, select, quad,
    xf, src, mid, out, dst, filt_in, edge_out, corner_out, edge_in, corner_in, total,
    local_sem, send1, recv1, send2, recv2, halo_send, halo_recv, filt_send, filt_recv,
):
    A, B = lat_devices, lon_devices
    A2, B2 = A // 2, B // 2
    first, count = worker_columns(B)
    workers, devices = A * count, A * B
    groups = workers // B
    points, channels = xb.shape
    own = channels // workers
    rows = own // 2
    whole = rows // 8 * 8
    half = points
    a, b = lax.axis_index("lat"), lax.axis_index("lon")
    me = b * A + a
    worker = jnp.logical_and(b >= first, b < first + count)
    mine = jnp.where(worker, (b - first) * A + a, -1)
    f32, bf16 = jnp.float32, jnp.bfloat16

    fetch = [
        pltpu.make_async_copy(s, d, local_sem.at[i])
        for i, (s, d) in enumerate(
            [(x_hbm, xb), (filter_hbm, filt), (quad_hbm, quad), (table_hbm, table), (select_hbm, select),
             (taps_hbm, taps), (norm_hbm, norm), (win_hbm, win), (wout_hbm, wout)]
        )
    ]
    fetch[0].start()
    barrier = pltpu.get_barrier_semaphore()
    neighbours = [(da, db) for da in (-1, 0, 1) for db in (-1, 0, 1) if (da, db) != (0, 0)]

    def inside(da):
        return jnp.logical_and(a + da >= 0, a + da < A)

    def at(da, db):
        return (a + da, lax.rem(b + db + B, B))

    @pl.when(worker)
    def _():
        def greet(peer, carry):
            @pl.when(peer != me)
            def _():
                pl.semaphore_signal(
                    barrier, inc=1, device_id=(lax.rem(peer, A), lax.div(peer, A)), device_id_type=MESH
                )

            return carry

        lax.fori_loop(0, devices, greet, 0)

    @pl.when(jnp.logical_not(worker))
    def _():
        for da, db in neighbours:
            @pl.when(inside(da))
            def _():
                pl.semaphore_signal(barrier, inc=1, device_id=at(da, db), device_id_type=MESH)

    for copy in fetch[1:]:
        copy.start()

    turn_lat, turn_lon = a >= A2, b >= B2
    p_row = lax.broadcasted_iota(jnp.int32, (points, 2 * half), 0)
    p_col = lax.broadcasted_iota(jnp.int32, (points, 2 * half), 1)

    def turned(index):
        jl, kl = lax.div(index, lon_cols), lax.rem(index, lon_cols)
        jl = jnp.where(turn_lat, lat_rows - 1 - jl, jl)
        kl = jnp.where(turn_lon, lon_cols - 1 - kl, kl)
        return jl * lon_cols + kl

    place = jnp.where(p_row == turned(lax.rem(p_col, half)), 1.0, 0.0)
    place_both = place.astype(bf16)
    place_left = jnp.where(p_col < half, place, 0.0).astype(bf16)
    left = lax.broadcasted_iota(jnp.int32, (rows, 2 * half), 1) < half

    def halves(value):
        if rows == whole:
            return value[:rows], value[rows:]
        rest = value[2 * whole :]
        return (
            jnp.concatenate([value[:whole], rest[: rows - whole]], 0),
            jnp.concatenate([value[whole : 2 * whole], rest[rows - whole :]], 0),
        )

    def joined(upper, lower):
        pieces = [upper[:whole], lower[:whole]]
        if rows > whole:
            pieces += [upper[whole:], lower[whole:]]
        return pieces

    fetch[0].wait()
    xf[...] = xb[...].astype(f32)
    xt = jnp.transpose(xf[...], (1, 0)).astype(bf16)
    xt = jnp.dot(xt, place_both, preferred_element_type=f32)
    for g in range(workers):
        upper, lower = halves(xt[own * g : own * (g + 1)])
        src[g] = jnp.where(left, upper, lower).astype(bf16)

    west, east = [
        jnp.concatenate([xf[k + lon_cols * r : k + lon_cols * r + 1] for r in range(lat_rows)], 0)
        for k in (0, lon_cols - 1)
    ]
    edge_out[0] = west.astype(bf16)
    edge_out[1] = east.astype(bf16)
    chunks = channels // 128
    for i, (r, side) in enumerate([(0, west), (0, east), (lat_rows - 1, west), (lat_rows - 1, east)]):
        parts = [side[r : r + 1, 128 * c : 128 * (c + 1)] for c in range(chunks)]
        parts.append(jnp.zeros((8 - chunks, 128), f32))
        corner_out[i] = jnp.concatenate(parts, 0).astype(bf16)

    def outside(db):
        other = lax.rem(b + db + B, B)
        return jnp.where(jnp.logical_and(other >= first, other < first + count), 0, 1)

    rims = jnp.where(a > 0, 1, 0) + jnp.where(a < A - 1, 1, 0)
    greetings = jnp.where(worker, workers - 1, workers)
    greetings = greetings + rims * outside(0) + (1 + rims) * (outside(-1) + outside(1))
    pl.semaphore_wait(barrier, greetings)

    B4 = B2 // 2
    zone = jnp.where(b < B4, 0, jnp.where(b < B - B4, 1, 2))

    def first_copy(g):
        return pltpu.make_async_remote_copy(
            src_ref=src.at[g], dst_ref=mid.at[me], send_sem=send1, recv_sem=recv1.at[zone],
            device_id=(lax.rem(g, A), first + lax.div(g, A)), device_id_type=MESH,
        )

    @pl.when(worker)
    def _():
        pltpu.make_async_copy(src.at[mine], mid.at[me], recv1.at[zone]).start()

    def first_send(step, carry):
        g = workers - 1 - step

        @pl.when(g != mine)
        def _():
            first_copy(g).start()

        return carry

    lax.fori_loop(0, workers, first_send, 0)

    fetch[1].wait()
    share = lax.rem(a + A * B - b * groups, A)
    owner_row = share < groups
    filt_lon = first + lax.div(b * groups + share, A)
    keeps = jnp.logical_and(owner_row, filt_lon == b)
    gives = jnp.logical_and(owner_row, filt_lon != b)
    filt_copy = pltpu.make_async_remote_copy(
        src_ref=filt, dst_ref=filt_in, send_sem=filt_send, recv_sem=filt_recv,
        device_id=(a, filt_lon), device_id_type=MESH,
    )

    @pl.when(gives)
    def _():
        filt_copy.start()

    @pl.when(keeps)
    def _():
        filt_in[...] = filt[...]

    def halo_copy(da, db):
        if db == 0:
            row = 0 if da < 0 else points - lon_cols
            source, target = xb.at[pl.ds(row, lon_cols)], edge_in.at[1 if da < 0 else 0]
            kind = 0
        elif da == 0:
            slot = 3 if db < 0 else 2
            source, target = edge_out.at[0 if db < 0 else 1], edge_in.at[slot]
            kind = 0
        else:
            index = (0 if da < 0 else 2) + (0 if db < 0 else 1)
            source, target = corner_out.at[index], corner_in.at[3 - index]
            kind = 1
        return pltpu.make_async_remote_copy(
            src_ref=source, dst_ref=target, send_sem=halo_send.at[kind], recv_sem=halo_recv.at[kind],
            device_id=at(da, db), device_id_type=MESH,
        )

    for da, db in neighbours:
        @pl.when(inside(da))
        def _():
            halo_copy(da, db).start()

    def index_of(ai, bi):
        return bi * A + ai

    def arrived(zone, start, count):
        blocks = mid.at[pl.ds(start, count)]
        pltpu.make_async_copy(blocks, blocks, recv1.at[zone]).wait()

    def widths(c):
        return pl.ds(starts[c], starts[c + 1] - starts[c])

    def folded(bs):
        tiles = [[] for _ in CLASSES]
        for bi in bs:
            parts = []
            for ai in range(A2):
                f00, f10, f01, f11 = [
                    mid[index_of(i, j)].astype(f32)
                    for i, j in [(ai, bi), (A - 1 - ai, bi), (ai, B - 1 - bi), (A - 1 - ai, B - 1 - bi)]
                ]
                s0, d0, s1, d1 = f00 + f10, f00 - f10, f01 + f11, f01 - f11
                w = quad[ai : ai + 1, :]
                parts.append([(s0 + s1) * w, (d0 + d1) * w, (s0 - s1) * w, (d0 - d1) * w])
            for ai in range(0, A2, 2):
                for c in range(4):
                    u, v = parts[ai][c], parts[ai + 1][c]
                    upper = jnp.where(left, u, pltpu.roll(v, half, 1))
                    lower = jnp.where(left, pltpu.roll(u, half, 1), v)
                    tiles[c].append(jnp.concatenate(joined(upper, lower), 0).astype(bf16))
        return [jnp.concatenate(t, 1) for t in tiles]

    inner = tuple(reversed(range(B2 // 2, B2)))
    outer = tuple(reversed(range(B2 // 2)))
    rows_of = lambda bs: pl.ds((B2 - 1 - bs[0]) * A2 * half, len(bs) * A2 * half)

    def second_copy(o):
        return pltpu.make_async_remote_copy(
            src_ref=out.at[o], dst_ref=dst.at[mine], send_sem=send2, recv_sem=recv2,
            device_id=(lax.rem(o, A), lax.div(o, A)), device_id_type=MESH,
        )

    @pl.when(worker)
    def _():
        for i in (2, 3, 4):
            fetch[i].wait()

        @pl.when(jnp.logical_not(keeps))
        def _():
            pltpu.make_async_remote_copy(
                src_ref=filt, dst_ref=filt_in, send_sem=filt_send, recv_sem=filt_recv,
                device_id=(a, lax.div(mine, groups)), device_id_type=MESH,
            ).wait_recv()

        held = filt_in.shape[1]
        r = lax.broadcasted_iota(jnp.int32, (own, held), 0)
        c = lax.broadcasted_iota(jnp.int32, (own, held), 1)
        pick = jnp.where(c == r + lax.rem(mine, groups) * own, 1.0, 0.0)
        rows = lax.dot_general(pick, filt_in[...], NT, precision=highest, preferred_element_type=f32)
        gain = jnp.dot(rows, select[...], precision=highest, preferred_element_type=f32)

        arrived(1, A * B4, devices - 2 * A * B4)
        acc = [
            jnp.dot(t, table[rows_of(inner), widths(i)], preferred_element_type=f32)
            for i, t in enumerate(folded(inner))
        ]
        arrived(0, 0, A * B4)
        arrived(2, devices - A * B4, A * B4)
        for i, t in enumerate(folded(outer)):
            acc[i] = acc[i] + jnp.dot(t, table[rows_of(outer), widths(i)], preferred_element_type=f32)
        coef = [(acc[i] * gain[:, starts[i] : starts[i + 1]]).astype(bf16) for i in range(4)]

        for bs in (outer, inner):
            grid = [
                lax.dot_general(coef[i], table[rows_of(bs), widths(i)], NT, preferred_element_type=f32)
                for i in range(4)
            ]
            for n, bi in enumerate(bs):
                for ai in range(0, A2, 2):
                    at_lane = (n * A2 + ai) * half
                    pp, mp, pm, mm = [g[:, at_lane : at_lane + 2 * half] for g in grid]
                    e0, e1, o0, o1 = pp + mp, pp - mp, pm + mm, pm - mm
                    for i, j, value in [(0, 0, e0 + o0), (1, 0, e1 + o1), (0, 1, e0 - o0), (1, 1, e1 - o1)]:
                        upper, lower = halves(value)
                        bj = B - 1 - bi if j else bi
                        a0, a1 = (A - 1 - ai, A - 2 - ai) if i else (ai, ai + 1)
                        out[index_of(a0, bj)] = jnp.where(left, upper, pltpu.roll(lower, half, 1)).astype(bf16)
                        out[index_of(a1, bj)] = jnp.where(left, pltpu.roll(upper, half, 1), lower).astype(bf16)

            def second_send(o, carry):
                @pl.when(o != me)
                def _():
                    second_copy(o).start()

                return carry

            if bs == outer:
                lax.fori_loop(0, A * B4, second_send, 0)
            else:
                lax.fori_loop(A * B4, devices, second_send, 0)
        pltpu.make_async_copy(out.at[me], dst.at[mine], recv2).start()

    @pl.when(a == 0)
    def _():
        edge_in[0] = jnp.zeros(edge_in.shape[1:], bf16)
        corner_in[0] = jnp.zeros(corner_in.shape[1:], bf16)
        corner_in[1] = jnp.zeros(corner_in.shape[1:], bf16)

    @pl.when(a == A - 1)
    def _():
        edge_in[1] = jnp.zeros(edge_in.shape[1:], bf16)
        corner_in[2] = jnp.zeros(corner_in.shape[1:], bf16)
        corner_in[3] = jnp.zeros(corner_in.shape[1:], bf16)

    pole = rims == 1

    def halo_wait(sems):
        for edges, corners, case in [(3, 2, pole), (4, 4, jnp.logical_not(pole))]:
            @pl.when(case)
            def _():
                for kind, blocks in enumerate([edge_in.at[pl.ds(0, edges)], corner_in.at[pl.ds(0, corners)]]):
                    pltpu.make_async_copy(blocks, blocks, sems.at[kind]).wait()

    halo_wait(halo_recv)

    fetch[5].wait()
    weight = taps[...]
    grid_rows = [edge_in[0].astype(f32)]
    grid_rows += [xf[pl.ds(lon_cols * r, lon_cols), :] for r in range(lat_rows)]
    grid_rows += [edge_in[1].astype(f32)]

    def corner(i):
        piece = corner_in[i].astype(f32)
        return jnp.concatenate([piece[c : c + 1] for c in range(chunks)], 1)

    west, east = edge_in[2].astype(f32), edge_in[3].astype(f32)
    west = [corner(0)] + [west[r : r + 1] for r in range(lat_rows)] + [corner(2)]
    east = [corner(1)] + [east[r : r + 1] for r in range(lat_rows)] + [corner(3)]
    sub = lax.broadcasted_iota(jnp.int32, (lon_cols, channels), 0)
    shifted = []
    for r in range(lat_rows + 2):
        here = grid_rows[r]
        before = jnp.where(sub == 0, west[r], pltpu.roll(here, 1, 0))
        after = jnp.where(sub == lon_cols - 1, east[r], pltpu.roll(here, lon_cols - 1, 0))
        shifted.append((before, here, after))
    for r in range(lat_rows):
        mix = sum(
            weight[3 * i + j : 3 * i + j + 1] * shifted[r + i][j] for i in range(3) for j in range(3)
        )
        mix = mix.astype(bf16).astype(f32)
        total[pl.ds(lon_cols * r, lon_cols), :] = grid_rows[r + 1] + mix

    for i in (6, 7, 8):
        fetch[i].wait()

    pltpu.make_async_copy(dst, dst, recv2).wait()
    parts = []
    for g in range(workers):
        piece = dst[g].astype(f32)
        parts += joined(piece, pltpu.roll(piece, half, 1))
    spectral = jnp.concatenate(parts, 0).astype(bf16)
    spectral = lax.dot_general(place_left, spectral, NT, preferred_element_type=f32)
    summed = (total[...] + spectral).astype(bf16).astype(f32)
    scale = lax.rsqrt(jnp.mean(summed * summed, axis=1, keepdims=True) + epsilon_norm)
    normed = (summed * scale * norm[...][None, :]).astype(bf16)
    hidden = jnp.dot(normed, win[...], preferred_element_type=f32)
    hidden = (0.5 * hidden * (1.0 + lax.erf(hidden * math.sqrt(0.5)))).astype(bf16)
    result = summed + jnp.dot(hidden, wout[...], preferred_element_type=f32)
    res[...] = result.astype(bf16)

    def left_already(blocks, sem):
        pltpu.make_async_copy(blocks, blocks, sem).wait()

    @pl.when(worker)
    def _():
        left_already(src.at[pl.ds(0, workers - 1)], send1)
        left_already(out.at[pl.ds(0, devices - 1)], send2)

    @pl.when(jnp.logical_not(worker))
    def _():
        left_already(src, send1)

    @pl.when(gives)
    def _():
        filt_copy.wait_send()

    halo_wait(halo_send)

    @pl.when(jnp.logical_not(worker))
    def _():
        for i in (2, 3, 4):
            fetch[i].wait()


def sphere_block(lat_devices, lon_devices, latent_field, spectral_filter, conv_weight, norm_gain, weight_in, weight_out):
    channels, lat_rows, lon_cols = latent_field.shape
    points = lat_rows * lon_cols
    workers = lat_devices * worker_columns(lon_devices)[1]
    own = channels // workers
    table, select, quad, starts = folded_tables(lat_devices, lon_devices, lat_rows, lon_cols)
    table = jnp.asarray(table.astype(jnp.bfloat16))
    args = [
        jnp.transpose(latent_field, (1, 2, 0)).reshape(points, channels),
        spectral_filter.T,
        conv_weight,
        norm_gain,
        weight_in,
        weight_out,
        table,
        jnp.asarray(select),
        jnp.asarray(quad),
    ]
    order = range(len(args))
    copies = [pltpu.VMEM(args[i].shape, args[i].dtype) for i in order]
    devices = lat_devices * lon_devices
    bf16, f32, dma = jnp.bfloat16, jnp.float32, pltpu.SemaphoreType.DMA
    scratch = [
        pltpu.VMEM((points, channels), f32),
        pltpu.VMEM((workers, own // 2, 128), bf16),
        pltpu.VMEM((devices, own // 2, 128), bf16),
        pltpu.VMEM((devices, own // 2, 128), bf16),
        pltpu.VMEM((workers, own // 2, 128), bf16),
        pltpu.VMEM(args[1].shape, f32),
        pltpu.VMEM((2, lat_rows, channels), bf16),
        pltpu.VMEM((4, 8, 128), bf16),
        pltpu.VMEM((4, lat_rows, channels), bf16),
        pltpu.VMEM((4, 8, 128), bf16),
        pltpu.VMEM((points, channels), f32),
        dma((len(args),)), dma, dma((3,)), dma, dma, dma((2,)), dma((2,)), dma, dma,
    ]
    result = pl.pallas_call(
        functools.partial(block_kernel, lat_devices, lon_devices, lat_rows, lon_cols, starts),
        out_shape=pltpu.VMEM((points, channels), bf16),
        in_specs=[pl.BlockSpec(memory_space=pl.ANY)] * len(args),
        out_specs=pl.BlockSpec(memory_space=pltpu.VMEM),
        scratch_shapes=copies + scratch,
        compiler_params=pltpu.CompilerParams(collective_id=0, has_side_effects=True),
        name="sphere_block",
    )(*args)
    return jnp.transpose(result.reshape(lat_rows, lon_cols, channels), (2, 0, 1))


def fits_block(lat_devices, lon_devices, latent_field):
    channels, lat_rows, lon_cols = latent_field.shape
    workers = lat_devices * worker_columns(lon_devices)[1]
    return (
        lat_devices % 4 == 0
        and lon_devices % 4 == 0
        and lat_rows == 8
        and lon_cols == 8
        and channels % (8 * workers) == 0
        and channels // workers % 2 == 0
        and channels % 128 == 0
        and channels <= 1024
    )


def block_or_banded(lat_devices, lon_devices, *arguments):
    if fits_block(lat_devices, lon_devices, arguments[0]):
        return sphere_block(lat_devices, lon_devices, *arguments)
    return on_device(*arguments)


def solution(mesh):
    return jax.shard_map(
        functools.partial(block_or_banded, mesh.shape["lat"], mesh.shape["lon"]),
        mesh=mesh,
        in_specs=(P(None, "lat", "lon"), P("lon", None), P(), P(), P(), P()),
        out_specs=P(None, "lat", "lon"),
        check_vma=False,
    )
```

```python
import functools
import math

import jax
import jax.numpy as jnp
import numpy as np
from jax import lax
from jax.experimental import pallas as pl
from jax.experimental.pallas import tpu as pltpu
from jax.sharding import PartitionSpec as P

highest = lax.Precision.HIGHEST
epsilon_norm = 1e-06


def with_halo(cells, sides, width):
    for axis, dim in sides:
        count = lax.axis_size(axis)
        ends = count - 1
        head = lax.slice_in_dim(cells, 0, width, axis=dim)
        tail = lax.slice_in_dim(cells, cells.shape[dim] - width, cells.shape[dim], axis=dim)
        cells = jnp.concatenate(
            [
                lax.ppermute(tail, axis, [(i, (i + 1) % count) for i in range(ends)]),
                cells,
                lax.ppermute(head, axis, [((i + 1) % count, i) for i in range(ends)]),
            ],
            axis=dim,
        )
    return cells


def quadrature(lat_count):
    colatitude = (jnp.arange(lat_count, dtype=jnp.float32) + 0.5) * (math.pi / lat_count)
    return jnp.sin(colatitude) * (math.pi / lat_count)


def fourier_tables(lon_count, mode_count):
    wave_index = (
        jnp.arange(mode_count, dtype=jnp.int32)[:, None]
        * jnp.arange(lon_count, dtype=jnp.int32)[None, :]
    )
    phase_angle = (wave_index % lon_count).astype(jnp.float32) * (2.0 * math.pi / lon_count)
    cosine = jnp.cos(phase_angle)
    sine_table = jnp.sin(phase_angle)
    angle_step = 2.0 * math.pi / lon_count
    forward = jnp.concatenate([angle_step * cosine, -angle_step * sine_table], axis=0)
    weight = jnp.where(jnp.arange(mode_count, dtype=jnp.int32) == 0, 1.0, 2.0).astype(jnp.float32)[
        :, None
    ]
    inverse = jnp.concatenate([weight * cosine, -weight * sine_table], axis=0)
    return (forward, inverse)


def legendre_rows(order_ids, lat_count):
    colatitude = (jnp.arange(lat_count, dtype=jnp.float32) + 0.5) * (math.pi / lat_count)
    cosine = jnp.cos(colatitude)
    sine_col = jnp.sin(colatitude)
    order_f = order_ids.astype(jnp.float32)
    factor_index = jnp.arange(1, lat_count, dtype=jnp.float32)
    ratio_log = jnp.log((2.0 * factor_index - 1.0) / (2.0 * factor_index))
    included = (factor_index[None, :] <= order_f[:, None]).astype(jnp.float32)
    log_factor = jnp.sum(included * ratio_log[None, :], axis=1)
    start_log = 0.5 * jnp.log((2.0 * order_f + 1.0) / (4.0 * math.pi)) + 0.5 * log_factor
    start_log = start_log[:, None] + order_f[:, None] * jnp.log(sine_col)[None, :]
    blank_rows = jnp.zeros((order_ids.shape[0], lat_count), jnp.float32)
    order_col = order_f[:, None]

    def advance(state_carry, degree):
        before, current, scale_log = state_carry
        degree_f = degree.astype(jnp.float32)
        alpha_term = jnp.sqrt(
            (4.0 * degree_f * degree_f - 1.0)
            / jnp.maximum(degree_f * degree_f - order_col * order_col, 1.0)
        )
        beta_term = jnp.sqrt(
            jnp.maximum((degree_f - 1.0) ** 2 - order_col * order_col, 0.0)
            / jnp.maximum(4.0 * (degree_f - 1.0) ** 2 - 1.0, 1.0)
        )
        stepped = alpha_term * (cosine[None, :] * current - beta_term * before)
        at_start = order_ids[:, None] == degree
        past_start = order_ids[:, None] < degree
        fresh_value = jnp.where(at_start, 1.0, jnp.where(past_start, stepped, 0.0))
        fresh_log = jnp.where(at_start, start_log, scale_log)
        entry_value = fresh_value * jnp.exp(fresh_log)
        rescale = jnp.where(
            past_start | at_start, jnp.maximum(jnp.abs(fresh_value), jnp.abs(current)), 1.0
        )
        return (
            (current / rescale, fresh_value / rescale, fresh_log + jnp.log(rescale)),
            entry_value,
        )

    degrees = jnp.arange(lat_count, dtype=jnp.int32)
    unused, legendre = lax.scan(advance, (blank_rows, blank_rows, blank_rows), degrees)
    return legendre


def filter_modes(banded, legendre, filter_block, quad_weights):
    coefficients = jnp.einsum(
        "lmj,pmcj->pmcl", legendre, banded * quad_weights[None, None, None, :], precision=highest
    )
    coefficients = coefficients * filter_block[None, None, :, :]
    return jnp.einsum("lmj,pmcl->pmcj", legendre, coefficients, precision=highest)


def wrap_columns(extended):
    return jnp.concatenate([extended[:, :, -1:], extended, extended[:, :, :1]], axis=2)


def depthwise_core(extended, kernel, lat_rows, lon_cols):
    accumulated = jnp.zeros((extended.shape[0], lat_rows, lon_cols), jnp.float32)
    for row_shift in range(3):
        for col_shift in range(3):
            piece = extended[
                :, row_shift : row_shift + lat_rows, col_shift : col_shift + lon_cols
            ].astype(jnp.float32)
            accumulated = accumulated + kernel[3 * row_shift + col_shift][:, None, None] * piece
    return accumulated.astype(jnp.bfloat16)


def channel_mlp(summed_low, norm_gain, weight_in, weight_out):
    summed = summed_low.astype(jnp.float32)
    scale_inv = lax.rsqrt(jnp.mean(summed * summed, axis=0, keepdims=True) + epsilon_norm)
    normed = (summed * scale_inv * norm_gain[:, None]).astype(jnp.bfloat16)
    hidden = lax.dot_general(
        weight_in, normed, (((0,), (0,)), ((), ())), preferred_element_type=jnp.float32
    )
    hidden = jax.nn.gelu(hidden, approximate=False).astype(jnp.bfloat16)
    result = summed + lax.dot_general(
        weight_out, hidden, (((0,), (0,)), ((), ())), preferred_element_type=jnp.float32
    )
    return result.astype(jnp.bfloat16)


def add_three(first, second, third):
    total = first.astype(jnp.float32) + second.astype(jnp.float32) + third.astype(jnp.float32)
    return total.astype(jnp.bfloat16)


def on_device(latent_field, spectral_filter, conv_weight, norm_gain, weight_in, weight_out):
    channels, lat_rows, lon_cols = latent_field.shape
    sector_count = lax.axis_size("lon")
    lat_count = lat_rows * lax.axis_size("lat")
    lon_count = lon_cols * sector_count
    chan_block = channels // sector_count
    spread = lax.all_to_all(latent_field, "lon", split_axis=0, concat_axis=2, tiled=True)
    forward, inverse = fourier_tables(lon_count, lat_count)
    flattened = spread.astype(jnp.float32).reshape(chan_block * lat_rows, lon_count)
    spectrum = lax.dot_general(forward, flattened, (((1,), (1,)), ((), ())), precision=highest)
    spectrum = spectrum.reshape(2, lat_count, chan_block, lat_rows)
    banded = lax.all_to_all(spectrum, "lat", split_axis=1, concat_axis=3, tiled=True)
    order_ids = lax.axis_index("lat") * lat_rows + jnp.arange(lat_rows, dtype=jnp.int32)
    legendre = legendre_rows(order_ids, lat_count)
    synthesized = filter_modes(banded, legendre, spectral_filter, quadrature(lat_count))
    regathered = lax.all_to_all(synthesized, "lat", split_axis=3, concat_axis=1, tiled=True)
    regridded = lax.dot_general(
        regathered.reshape(2 * lat_count, chan_block * lat_rows),
        inverse,
        (((0,), (0,)), ((), ())),
        precision=highest,
    )
    spectral = regridded.reshape(chan_block, lat_rows, lon_count).astype(jnp.bfloat16)
    own_kernel = lax.dynamic_slice_in_dim(
        conv_weight, lax.axis_index("lon") * chan_block, chan_block, 1
    )
    rimmed = with_halo(spread, (("lat", 1),), 1)
    sector_mix = depthwise_core(wrap_columns(rimmed), own_kernel, lat_rows, lon_count)
    sector_sum = add_three(spread, spectral, sector_mix)
    summed = lax.all_to_all(sector_sum, "lon", split_axis=2, concat_axis=0, tiled=True)
    summed = summed.reshape(channels, lat_rows * lon_cols)
    result = channel_mlp(summed, norm_gain, weight_in, weight_out)
    return result.reshape(channels, lat_rows, lon_cols)


CLASSES = ((0, 0), (1, 0), (0, 1), (1, 1))


def folded_tables(lat_devices, lon_devices, lat_rows, lon_cols):
    lat_count, lon_count = lat_devices * lat_rows, lon_devices * lon_cols
    theta = (np.arange(lat_count // 2) + 0.5) * (math.pi / lat_count)
    x, s = np.cos(theta), np.sin(theta)
    phi = 2.0 * math.pi * (np.arange(lon_count // 2) + 0.5) / lon_count
    row, column = [], []
    for b in reversed(range(lon_devices // 2)):
        for a in range(lat_devices // 2):
            row.append(np.repeat(a * lat_rows + np.arange(lat_rows), lon_cols))
            column.append(np.tile(b * lon_cols + np.arange(lon_cols), lat_rows))
    row, column = np.concatenate(row), np.concatenate(column)
    columns = {key: [] for key in CLASSES}
    degrees = {key: [] for key in CLASSES}
    weights = {key: [] for key in CLASSES}
    for m in range(lat_count):
        k = np.arange(1, m + 1)
        log_start = 0.5 * (
            np.log((2 * m + 1) / (4 * math.pi)) + np.sum(np.log((2 * k - 1) / (2 * k)))
        )
        before, current = np.zeros(lat_count // 2), np.exp(log_start + m * np.log(s))
        for l in range(m, lat_count):
            if l > m:
                a = math.sqrt((4.0 * l * l - 1) / (l * l - m * m))
                b = math.sqrt(((l - 1.0) ** 2 - m * m) / (4.0 * (l - 1) ** 2 - 1))
                before, current = current, a * (x * current - b * before)
            for phase, wave in enumerate([np.cos(m * phi), -np.sin(m * phi)][: 1 if m == 0 else 2]):
                key = ((l + m) % 2, phase)
                columns[key].append(current[row] * wave[column])
                degrees[key].append(l)
                weights[key].append((1.0 if m == 0 else 2.0) * 2.0 * math.pi / lon_count)
    tables, selects, starts = [], [], [0]
    for key in CLASSES:
        width = -(-len(columns[key]) // 128) * 128
        fill = width - len(columns[key])
        tables.append(np.pad(np.stack(columns[key], 1), ((0, 0), (0, fill))))
        select = np.arange(lat_count)[:, None] == np.array(degrees[key])[None, :]
        selects.append(np.pad(select * np.array(weights[key])[None, :], ((0, 0), (0, fill))))
        starts.append(starts[-1] + width)
    quad = s * (math.pi / lat_count)
    quad = np.repeat(quad.reshape(lat_devices // 2, lat_rows), lon_cols, axis=1)
    return (
        np.concatenate(tables, 1),
        np.concatenate(selects, 1).astype(np.float32),
        np.tile(quad, (1, 2)).astype(np.float32),
        tuple(starts),
    )


MESH = pl.DeviceIdType.MESH


def worker_columns(lon_devices):
    return lon_devices // 4, lon_devices // 2


NT = (((1,), (1,)), ((), ()))


def block_kernel(
    lat_devices, lon_devices, lat_rows, lon_cols, starts,
    x_hbm, filter_hbm, taps_hbm, norm_hbm, win_hbm, wout_hbm, table_hbm, select_hbm, quad_hbm,
    res,
    xb, filt, taps, norm, win, wout, table, select, quad,
    xf, src, mid, out, dst, filt_in, edge_out, corner_out, edge_in, corner_in, total,
    local_sem, send1, recv1, send2, recv2, halo_send, halo_recv, filt_send, filt_recv,
):
    A, B = lat_devices, lon_devices
    A2, B2 = A // 2, B // 2
    first, count = worker_columns(B)
    workers, devices = A * count, A * B
    groups = workers // B
    points, channels = xb.shape
    own = channels // workers
    rows = own // 2
    whole = rows // 8 * 8
    half = points
    a, b = lax.axis_index("lat"), lax.axis_index("lon")
    me = b * A + a
    worker = jnp.logical_and(b >= first, b < first + count)
    mine = jnp.where(worker, (b - first) * A + a, -1)
    f32, bf16 = jnp.float32, jnp.bfloat16

    fetch = [
        pltpu.make_async_copy(s, d, local_sem.at[i])
        for i, (s, d) in enumerate(
            [(x_hbm, xb), (filter_hbm, filt), (quad_hbm, quad), (table_hbm, table), (select_hbm, select),
             (taps_hbm, taps), (norm_hbm, norm), (win_hbm, win), (wout_hbm, wout)]
        )
    ]
    fetch[0].start()
    barrier = pltpu.get_barrier_semaphore()
    neighbours = [(da, db) for da in (-1, 0, 1) for db in (-1, 0, 1) if (da, db) != (0, 0)]

    def inside(da):
        return jnp.logical_and(a + da >= 0, a + da < A)

    def at(da, db):
        return (a + da, lax.rem(b + db + B, B))

    @pl.when(worker)
    def _():
        def greet(peer, carry):
            @pl.when(peer != me)
            def _():
                pl.semaphore_signal(
                    barrier, inc=1, device_id=(lax.rem(peer, A), lax.div(peer, A)), device_id_type=MESH
                )

            return carry

        lax.fori_loop(0, devices, greet, 0)

    @pl.when(jnp.logical_not(worker))
    def _():
        for da, db in neighbours:
            @pl.when(inside(da))
            def _():
                pl.semaphore_signal(barrier, inc=1, device_id=at(da, db), device_id_type=MESH)

    for copy in fetch[1:]:
        copy.start()

    turn_lat, turn_lon = a >= A2, b >= B2
    p_row = lax.broadcasted_iota(jnp.int32, (points, 2 * half), 0)
    p_col = lax.broadcasted_iota(jnp.int32, (points, 2 * half), 1)

    def turned(index):
        jl, kl = lax.div(index, lon_cols), lax.rem(index, lon_cols)
        jl = jnp.where(turn_lat, lat_rows - 1 - jl, jl)
        kl = jnp.where(turn_lon, lon_cols - 1 - kl, kl)
        return jl * lon_cols + kl

    place = jnp.where(p_row == turned(lax.rem(p_col, half)), 1.0, 0.0)
    place_both = place.astype(bf16)
    place_left = jnp.where(p_col < half, place, 0.0).astype(bf16)
    left = lax.broadcasted_iota(jnp.int32, (rows, 2 * half), 1) < half

    def halves(value):
        if rows == whole:
            return value[:rows], value[rows:]
        rest = value[2 * whole :]
        return (
            jnp.concatenate([value[:whole], rest[: rows - whole]], 0),
            jnp.concatenate([value[whole : 2 * whole], rest[rows - whole :]], 0),
        )

    def joined(upper, lower):
        pieces = [upper[:whole], lower[:whole]]
        if rows > whole:
            pieces += [upper[whole:], lower[whole:]]
        return pieces

    fetch[0].wait()
    xf[...] = xb[...].astype(f32)
    xt = jnp.transpose(xf[...], (1, 0)).astype(bf16)
    xt = jnp.dot(xt, place_both, preferred_element_type=f32)
    for g in range(workers):
        upper, lower = halves(xt[own * g : own * (g + 1)])
        src[g] = jnp.where(left, upper, lower).astype(bf16)

    west, east = [
        jnp.concatenate([xf[k + lon_cols * r : k + lon_cols * r + 1] for r in range(lat_rows)], 0)
        for k in (0, lon_cols - 1)
    ]
    edge_out[0] = west.astype(bf16)
    edge_out[1] = east.astype(bf16)
    chunks = channels // 128
    for i, (r, side) in enumerate([(0, west), (0, east), (lat_rows - 1, west), (lat_rows - 1, east)]):
        parts = [side[r : r + 1, 128 * c : 128 * (c + 1)] for c in range(chunks)]
        parts.append(jnp.zeros((8 - chunks, 128), f32))
        corner_out[i] = jnp.concatenate(parts, 0).astype(bf16)

    def outside(db):
        other = lax.rem(b + db + B, B)
        return jnp.where(jnp.logical_and(other >= first, other < first + count), 0, 1)

    rims = jnp.where(a > 0, 1, 0) + jnp.where(a < A - 1, 1, 0)
    greetings = jnp.where(worker, workers - 1, workers)
    greetings = greetings + rims * outside(0) + (1 + rims) * (outside(-1) + outside(1))
    pl.semaphore_wait(barrier, greetings)

    B4 = B2 // 2
    zone = jnp.where(b < B4, 0, jnp.where(b < B - B4, 1, 2))

    def first_copy(g):
        return pltpu.make_async_remote_copy(
            src_ref=src.at[g], dst_ref=mid.at[me], send_sem=send1, recv_sem=recv1.at[zone],
            device_id=(lax.rem(g, A), first + lax.div(g, A)), device_id_type=MESH,
        )

    @pl.when(worker)
    def _():
        pltpu.make_async_copy(src.at[mine], mid.at[me], recv1.at[zone]).start()

    def first_send(step, carry):
        g = workers - 1 - step

        @pl.when(g != mine)
        def _():
            first_copy(g).start()

        return carry

    lax.fori_loop(0, workers, first_send, 0)

    fetch[1].wait()
    share = lax.rem(a + A * B - b * groups, A)
    owner_row = share < groups
    filt_lon = first + lax.div(b * groups + share, A)
    keeps = jnp.logical_and(owner_row, filt_lon == b)
    gives = jnp.logical_and(owner_row, filt_lon != b)
    filt_copy = pltpu.make_async_remote_copy(
        src_ref=filt, dst_ref=filt_in, send_sem=filt_send, recv_sem=filt_recv,
        device_id=(a, filt_lon), device_id_type=MESH,
    )

    @pl.when(gives)
    def _():
        filt_copy.start()

    @pl.when(keeps)
    def _():
        filt_in[...] = filt[...]

    def halo_copy(da, db):
        if db == 0:
            row = 0 if da < 0 else points - lon_cols
            source, target = xb.at[pl.ds(row, lon_cols)], edge_in.at[1 if da < 0 else 0]
            kind = 0
        elif da == 0:
            slot = 3 if db < 0 else 2
            source, target = edge_out.at[0 if db < 0 else 1], edge_in.at[slot]
            kind = 0
        else:
            index = (0 if da < 0 else 2) + (0 if db < 0 else 1)
            source, target = corner_out.at[index], corner_in.at[3 - index]
            kind = 1
        return pltpu.make_async_remote_copy(
            src_ref=source, dst_ref=target, send_sem=halo_send.at[kind], recv_sem=halo_recv.at[kind],
            device_id=at(da, db), device_id_type=MESH,
        )

    def left_already(blocks, sem):
        pltpu.make_async_copy(blocks, blocks, sem).wait()

    @pl.when(worker)
    def _():
        left_already(src.at[pl.ds(0, workers - 1)], send1)

    @pl.when(jnp.logical_not(worker))
    def _():
        left_already(src, send1)

    for da, db in neighbours:
        @pl.when(inside(da))
        def _():
            halo_copy(da, db).start()

    def index_of(ai, bi):
        return bi * A + ai

    def arrived(zone, start, count):
        blocks = mid.at[pl.ds(start, count)]
        pltpu.make_async_copy(blocks, blocks, recv1.at[zone]).wait()

    def widths(c):
        return pl.ds(starts[c], starts[c + 1] - starts[c])

    def folded(bs):
        tiles = [[] for _ in CLASSES]
        for bi in bs:
            parts = []
            for ai in range(A2):
                f00, f10, f01, f11 = [
                    mid[index_of(i, j)].astype(f32)
                    for i, j in [(ai, bi), (A - 1 - ai, bi), (ai, B - 1 - bi), (A - 1 - ai, B - 1 - bi)]
                ]
                s0, d0, s1, d1 = f00 + f10, f00 - f10, f01 + f11, f01 - f11
                w = quad[ai : ai + 1, :]
                parts.append([(s0 + s1) * w, (d0 + d1) * w, (s0 - s1) * w, (d0 - d1) * w])
            for ai in range(0, A2, 2):
                for c in range(4):
                    u, v = parts[ai][c], parts[ai + 1][c]
                    upper = jnp.where(left, u, pltpu.roll(v, half, 1))
                    lower = jnp.where(left, pltpu.roll(u, half, 1), v)
                    tiles[c].append(jnp.concatenate(joined(upper, lower), 0).astype(bf16))
        return [jnp.concatenate(t, 1) for t in tiles]

    inner = tuple(reversed(range(B2 // 2, B2)))
    outer = tuple(reversed(range(B2 // 2)))
    rows_of = lambda bs: pl.ds((B2 - 1 - bs[0]) * A2 * half, len(bs) * A2 * half)

    def second_copy(o):
        return pltpu.make_async_remote_copy(
            src_ref=out.at[o], dst_ref=dst.at[mine], send_sem=send2, recv_sem=recv2,
            device_id=(lax.rem(o, A), lax.div(o, A)), device_id_type=MESH,
        )

    @pl.when(worker)
    def _():
        for i in (2, 3, 4):
            fetch[i].wait()

        @pl.when(jnp.logical_not(keeps))
        def _():
            pltpu.make_async_remote_copy(
                src_ref=filt, dst_ref=filt_in, send_sem=filt_send, recv_sem=filt_recv,
                device_id=(a, lax.div(mine, groups)), device_id_type=MESH,
            ).wait_recv()

        held = filt_in.shape[1]
        r = lax.broadcasted_iota(jnp.int32, (own, held), 0)
        c = lax.broadcasted_iota(jnp.int32, (own, held), 1)
        pick = jnp.where(c == r + lax.rem(mine, groups) * own, 1.0, 0.0)
        rows = lax.dot_general(pick, filt_in[...], NT, precision=highest, preferred_element_type=f32)
        gain = jnp.dot(rows, select[...], precision=highest, preferred_element_type=f32)

        arrived(1, A * B4, devices - 2 * A * B4)
        acc = [
            jnp.dot(t, table[rows_of(inner), widths(i)], preferred_element_type=f32)
            for i, t in enumerate(folded(inner))
        ]
        arrived(0, 0, A * B4)
        arrived(2, devices - A * B4, A * B4)
        for i, t in enumerate(folded(outer)):
            acc[i] = acc[i] + jnp.dot(t, table[rows_of(outer), widths(i)], preferred_element_type=f32)
        coef = [(acc[i] * gain[:, starts[i] : starts[i + 1]]).astype(bf16) for i in range(4)]

        for bs in (outer, inner):
            grid = [
                lax.dot_general(coef[i], table[rows_of(bs), widths(i)], NT, preferred_element_type=f32)
                for i in range(4)
            ]
            for n, bi in enumerate(bs):
                for ai in range(0, A2, 2):
                    at_lane = (n * A2 + ai) * half
                    pp, mp, pm, mm = [g[:, at_lane : at_lane + 2 * half] for g in grid]
                    e0, e1, o0, o1 = pp + mp, pp - mp, pm + mm, pm - mm
                    for i, j, value in [(0, 0, e0 + o0), (1, 0, e1 + o1), (0, 1, e0 - o0), (1, 1, e1 - o1)]:
                        upper, lower = halves(value)
                        bj = B - 1 - bi if j else bi
                        a0, a1 = (A - 1 - ai, A - 2 - ai) if i else (ai, ai + 1)
                        out[index_of(a0, bj)] = jnp.where(left, upper, pltpu.roll(lower, half, 1)).astype(bf16)
                        out[index_of(a1, bj)] = jnp.where(left, pltpu.roll(upper, half, 1), lower).astype(bf16)

            def near_send(step, carry):
                second_copy(lax.rem(step, B4) * A + lax.div(step, B4)).start()
                return carry

            def second_send(o, carry):
                @pl.when(o != me)
                def _():
                    second_copy(o).start()

                return carry

            if bs == outer:
                lax.fori_loop(0, B4, near_send, 0)
            else:
                lax.fori_loop(B4, A * B4, near_send, 0)
                lax.fori_loop(A * B4, devices, second_send, 0)
        pltpu.make_async_copy(out.at[me], dst.at[mine], recv2).start()

    @pl.when(a == 0)
    def _():
        edge_in[0] = jnp.zeros(edge_in.shape[1:], bf16)
        corner_in[0] = jnp.zeros(corner_in.shape[1:], bf16)
        corner_in[1] = jnp.zeros(corner_in.shape[1:], bf16)

    @pl.when(a == A - 1)
    def _():
        edge_in[1] = jnp.zeros(edge_in.shape[1:], bf16)
        corner_in[2] = jnp.zeros(corner_in.shape[1:], bf16)
        corner_in[3] = jnp.zeros(corner_in.shape[1:], bf16)

    pole = rims == 1

    def halo_wait(sems):
        for edges, corners, case in [(3, 2, pole), (4, 4, jnp.logical_not(pole))]:
            @pl.when(case)
            def _():
                for kind, blocks in enumerate([edge_in.at[pl.ds(0, edges)], corner_in.at[pl.ds(0, corners)]]):
                    pltpu.make_async_copy(blocks, blocks, sems.at[kind]).wait()

    halo_wait(halo_recv)

    fetch[5].wait()
    weight = taps[...]
    grid_rows = [edge_in[0].astype(f32)]
    grid_rows += [xf[pl.ds(lon_cols * r, lon_cols), :] for r in range(lat_rows)]
    grid_rows += [edge_in[1].astype(f32)]

    def corner(i):
        piece = corner_in[i].astype(f32)
        return jnp.concatenate([piece[c : c + 1] for c in range(chunks)], 1)

    west, east = edge_in[2].astype(f32), edge_in[3].astype(f32)
    west = [corner(0)] + [west[r : r + 1] for r in range(lat_rows)] + [corner(2)]
    east = [corner(1)] + [east[r : r + 1] for r in range(lat_rows)] + [corner(3)]
    sub = lax.broadcasted_iota(jnp.int32, (lon_cols, channels), 0)
    shifted = []
    for r in range(lat_rows + 2):
        here = grid_rows[r]
        before = jnp.where(sub == 0, west[r], pltpu.roll(here, 1, 0))
        after = jnp.where(sub == lon_cols - 1, east[r], pltpu.roll(here, lon_cols - 1, 0))
        shifted.append((before, here, after))
    for r in range(lat_rows):
        mix = sum(
            weight[3 * i + j : 3 * i + j + 1] * shifted[r + i][j] for i in range(3) for j in range(3)
        )
        mix = mix.astype(bf16).astype(f32)
        total[pl.ds(lon_cols * r, lon_cols), :] = grid_rows[r + 1] + mix

    for i in (6, 7, 8):
        fetch[i].wait()

    pltpu.make_async_copy(dst, dst, recv2).wait()
    parts = []
    for g in range(workers):
        piece = dst[g].astype(f32)
        parts += joined(piece, pltpu.roll(piece, half, 1))
    spectral = jnp.concatenate(parts, 0).astype(bf16)
    spectral = lax.dot_general(place_left, spectral, NT, preferred_element_type=f32)
    summed = (total[...] + spectral).astype(bf16).astype(f32)
    scale = lax.rsqrt(jnp.mean(summed * summed, axis=1, keepdims=True) + epsilon_norm)
    normed = (summed * scale * norm[...][None, :]).astype(bf16)
    hidden = jnp.dot(normed, win[...], preferred_element_type=f32)
    hidden = (0.5 * hidden * (1.0 + lax.erf(hidden * math.sqrt(0.5)))).astype(bf16)
    result = summed + jnp.dot(hidden, wout[...], preferred_element_type=f32)
    res[...] = result.astype(bf16)

    @pl.when(worker)
    def _():
        left_already(out.at[pl.ds(0, devices - 1)], send2)

    @pl.when(gives)
    def _():
        filt_copy.wait_send()

    halo_wait(halo_send)

    @pl.when(jnp.logical_not(worker))
    def _():
        for i in (2, 3, 4):
            fetch[i].wait()


def sphere_block(lat_devices, lon_devices, latent_field, spectral_filter, conv_weight, norm_gain, weight_in, weight_out):
    channels, lat_rows, lon_cols = latent_field.shape
    points = lat_rows * lon_cols
    workers = lat_devices * worker_columns(lon_devices)[1]
    own = channels // workers
    table, select, quad, starts = folded_tables(lat_devices, lon_devices, lat_rows, lon_cols)
    table = jnp.asarray(table.astype(jnp.bfloat16))
    args = [
        jnp.transpose(latent_field, (1, 2, 0)).reshape(points, channels),
        spectral_filter.T,
        conv_weight,
        norm_gain,
        weight_in,
        weight_out,
        table,
        jnp.asarray(select),
        jnp.asarray(quad),
    ]
    order = range(len(args))
    copies = [pltpu.VMEM(args[i].shape, args[i].dtype) for i in order]
    devices = lat_devices * lon_devices
    bf16, f32, dma = jnp.bfloat16, jnp.float32, pltpu.SemaphoreType.DMA
    scratch = [
        pltpu.VMEM((points, channels), f32),
        pltpu.VMEM((workers, own // 2, 128), bf16),
        pltpu.VMEM((devices, own // 2, 128), bf16),
        pltpu.VMEM((devices, own // 2, 128), bf16),
        pltpu.VMEM((workers, own // 2, 128), bf16),
        pltpu.VMEM(args[1].shape, f32),
        pltpu.VMEM((2, lat_rows, channels), bf16),
        pltpu.VMEM((4, 8, 128), bf16),
        pltpu.VMEM((4, lat_rows, channels), bf16),
        pltpu.VMEM((4, 8, 128), bf16),
        pltpu.VMEM((points, channels), f32),
        dma((len(args),)), dma, dma((3,)), dma, dma, dma((2,)), dma((2,)), dma, dma,
    ]
    result = pl.pallas_call(
        functools.partial(block_kernel, lat_devices, lon_devices, lat_rows, lon_cols, starts),
        out_shape=pltpu.VMEM((points, channels), bf16),
        in_specs=[pl.BlockSpec(memory_space=pl.ANY)] * len(args),
        out_specs=pl.BlockSpec(memory_space=pltpu.VMEM),
        scratch_shapes=copies + scratch,
        compiler_params=pltpu.CompilerParams(collective_id=0, has_side_effects=True),
        name="sphere_block",
    )(*args)
    return jnp.transpose(result.reshape(lat_rows, lon_cols, channels), (2, 0, 1))


def fits_block(lat_devices, lon_devices, latent_field):
    channels, lat_rows, lon_cols = latent_field.shape
    workers = lat_devices * worker_columns(lon_devices)[1]
    return (
        lat_devices % 4 == 0
        and lon_devices % 4 == 0
        and lat_rows == 8
        and lon_cols == 8
        and channels % (8 * workers) == 0
        and channels // workers % 2 == 0
        and channels % 128 == 0
        and channels <= 1024
    )


def block_or_banded(lat_devices, lon_devices, *arguments):
    if fits_block(lat_devices, lon_devices, arguments[0]):
        return sphere_block(lat_devices, lon_devices, *arguments)
    return on_device(*arguments)


def solution(mesh):
    return jax.shard_map(
        functools.partial(block_or_banded, mesh.shape["lat"], mesh.shape["lon"]),
        mesh=mesh,
        in_specs=(P(None, "lat", "lon"), P("lon", None), P(), P(), P(), P()),
        out_specs=P(None, "lat", "lon"),
        check_vma=False,
    )
```

```python
import functools
import math

import jax
import jax.numpy as jnp
import numpy as np
from jax import lax
from jax.experimental import pallas as pl
from jax.experimental.pallas import tpu as pltpu
from jax.sharding import PartitionSpec as P

highest = lax.Precision.HIGHEST
epsilon_norm = 1e-06


def with_halo(cells, sides, width):
    for axis, dim in sides:
        count = lax.axis_size(axis)
        ends = count - 1
        head = lax.slice_in_dim(cells, 0, width, axis=dim)
        tail = lax.slice_in_dim(cells, cells.shape[dim] - width, cells.shape[dim], axis=dim)
        cells = jnp.concatenate(
            [
                lax.ppermute(tail, axis, [(i, (i + 1) % count) for i in range(ends)]),
                cells,
                lax.ppermute(head, axis, [((i + 1) % count, i) for i in range(ends)]),
            ],
            axis=dim,
        )
    return cells


def quadrature(lat_count):
    colatitude = (jnp.arange(lat_count, dtype=jnp.float32) + 0.5) * (math.pi / lat_count)
    return jnp.sin(colatitude) * (math.pi / lat_count)


def fourier_tables(lon_count, mode_count):
    wave_index = (
        jnp.arange(mode_count, dtype=jnp.int32)[:, None]
        * jnp.arange(lon_count, dtype=jnp.int32)[None, :]
    )
    phase_angle = (wave_index % lon_count).astype(jnp.float32) * (2.0 * math.pi / lon_count)
    cosine = jnp.cos(phase_angle)
    sine_table = jnp.sin(phase_angle)
    angle_step = 2.0 * math.pi / lon_count
    forward = jnp.concatenate([angle_step * cosine, -angle_step * sine_table], axis=0)
    weight = jnp.where(jnp.arange(mode_count, dtype=jnp.int32) == 0, 1.0, 2.0).astype(jnp.float32)[
        :, None
    ]
    inverse = jnp.concatenate([weight * cosine, -weight * sine_table], axis=0)
    return (forward, inverse)


def legendre_rows(order_ids, lat_count):
    colatitude = (jnp.arange(lat_count, dtype=jnp.float32) + 0.5) * (math.pi / lat_count)
    cosine = jnp.cos(colatitude)
    sine_col = jnp.sin(colatitude)
    order_f = order_ids.astype(jnp.float32)
    factor_index = jnp.arange(1, lat_count, dtype=jnp.float32)
    ratio_log = jnp.log((2.0 * factor_index - 1.0) / (2.0 * factor_index))
    included = (factor_index[None, :] <= order_f[:, None]).astype(jnp.float32)
    log_factor = jnp.sum(included * ratio_log[None, :], axis=1)
    start_log = 0.5 * jnp.log((2.0 * order_f + 1.0) / (4.0 * math.pi)) + 0.5 * log_factor
    start_log = start_log[:, None] + order_f[:, None] * jnp.log(sine_col)[None, :]
    blank_rows = jnp.zeros((order_ids.shape[0], lat_count), jnp.float32)
    order_col = order_f[:, None]

    def advance(state_carry, degree):
        before, current, scale_log = state_carry
        degree_f = degree.astype(jnp.float32)
        alpha_term = jnp.sqrt(
            (4.0 * degree_f * degree_f - 1.0)
            / jnp.maximum(degree_f * degree_f - order_col * order_col, 1.0)
        )
        beta_term = jnp.sqrt(
            jnp.maximum((degree_f - 1.0) ** 2 - order_col * order_col, 0.0)
            / jnp.maximum(4.0 * (degree_f - 1.0) ** 2 - 1.0, 1.0)
        )
        stepped = alpha_term * (cosine[None, :] * current - beta_term * before)
        at_start = order_ids[:, None] == degree
        past_start = order_ids[:, None] < degree
        fresh_value = jnp.where(at_start, 1.0, jnp.where(past_start, stepped, 0.0))
        fresh_log = jnp.where(at_start, start_log, scale_log)
        entry_value = fresh_value * jnp.exp(fresh_log)
        rescale = jnp.where(
            past_start | at_start, jnp.maximum(jnp.abs(fresh_value), jnp.abs(current)), 1.0
        )
        return (
            (current / rescale, fresh_value / rescale, fresh_log + jnp.log(rescale)),
            entry_value,
        )

    degrees = jnp.arange(lat_count, dtype=jnp.int32)
    unused, legendre = lax.scan(advance, (blank_rows, blank_rows, blank_rows), degrees)
    return legendre


def filter_modes(banded, legendre, filter_block, quad_weights):
    coefficients = jnp.einsum(
        "lmj,pmcj->pmcl", legendre, banded * quad_weights[None, None, None, :], precision=highest
    )
    coefficients = coefficients * filter_block[None, None, :, :]
    return jnp.einsum("lmj,pmcl->pmcj", legendre, coefficients, precision=highest)


def wrap_columns(extended):
    return jnp.concatenate([extended[:, :, -1:], extended, extended[:, :, :1]], axis=2)


def depthwise_core(extended, kernel, lat_rows, lon_cols):
    accumulated = jnp.zeros((extended.shape[0], lat_rows, lon_cols), jnp.float32)
    for row_shift in range(3):
        for col_shift in range(3):
            piece = extended[
                :, row_shift : row_shift + lat_rows, col_shift : col_shift + lon_cols
            ].astype(jnp.float32)
            accumulated = accumulated + kernel[3 * row_shift + col_shift][:, None, None] * piece
    return accumulated.astype(jnp.bfloat16)


def channel_mlp(summed_low, norm_gain, weight_in, weight_out):
    summed = summed_low.astype(jnp.float32)
    scale_inv = lax.rsqrt(jnp.mean(summed * summed, axis=0, keepdims=True) + epsilon_norm)
    normed = (summed * scale_inv * norm_gain[:, None]).astype(jnp.bfloat16)
    hidden = lax.dot_general(
        weight_in, normed, (((0,), (0,)), ((), ())), preferred_element_type=jnp.float32
    )
    hidden = jax.nn.gelu(hidden, approximate=False).astype(jnp.bfloat16)
    result = summed + lax.dot_general(
        weight_out, hidden, (((0,), (0,)), ((), ())), preferred_element_type=jnp.float32
    )
    return result.astype(jnp.bfloat16)


def add_three(first, second, third):
    total = first.astype(jnp.float32) + second.astype(jnp.float32) + third.astype(jnp.float32)
    return total.astype(jnp.bfloat16)


def on_device(latent_field, spectral_filter, conv_weight, norm_gain, weight_in, weight_out):
    channels, lat_rows, lon_cols = latent_field.shape
    sector_count = lax.axis_size("lon")
    lat_count = lat_rows * lax.axis_size("lat")
    lon_count = lon_cols * sector_count
    chan_block = channels // sector_count
    spread = lax.all_to_all(latent_field, "lon", split_axis=0, concat_axis=2, tiled=True)
    forward, inverse = fourier_tables(lon_count, lat_count)
    flattened = spread.astype(jnp.float32).reshape(chan_block * lat_rows, lon_count)
    spectrum = lax.dot_general(forward, flattened, (((1,), (1,)), ((), ())), precision=highest)
    spectrum = spectrum.reshape(2, lat_count, chan_block, lat_rows)
    banded = lax.all_to_all(spectrum, "lat", split_axis=1, concat_axis=3, tiled=True)
    order_ids = lax.axis_index("lat") * lat_rows + jnp.arange(lat_rows, dtype=jnp.int32)
    legendre = legendre_rows(order_ids, lat_count)
    synthesized = filter_modes(banded, legendre, spectral_filter, quadrature(lat_count))
    regathered = lax.all_to_all(synthesized, "lat", split_axis=3, concat_axis=1, tiled=True)
    regridded = lax.dot_general(
        regathered.reshape(2 * lat_count, chan_block * lat_rows),
        inverse,
        (((0,), (0,)), ((), ())),
        precision=highest,
    )
    spectral = regridded.reshape(chan_block, lat_rows, lon_count).astype(jnp.bfloat16)
    own_kernel = lax.dynamic_slice_in_dim(
        conv_weight, lax.axis_index("lon") * chan_block, chan_block, 1
    )
    rimmed = with_halo(spread, (("lat", 1),), 1)
    sector_mix = depthwise_core(wrap_columns(rimmed), own_kernel, lat_rows, lon_count)
    sector_sum = add_three(spread, spectral, sector_mix)
    summed = lax.all_to_all(sector_sum, "lon", split_axis=2, concat_axis=0, tiled=True)
    summed = summed.reshape(channels, lat_rows * lon_cols)
    result = channel_mlp(summed, norm_gain, weight_in, weight_out)
    return result.reshape(channels, lat_rows, lon_cols)


CLASSES = ((0, 0), (1, 0), (0, 1), (1, 1))


def folded_tables(lat_devices, lon_devices, lat_rows, lon_cols):
    lat_count, lon_count = lat_devices * lat_rows, lon_devices * lon_cols
    theta = (np.arange(lat_count // 2) + 0.5) * (math.pi / lat_count)
    x, s = np.cos(theta), np.sin(theta)
    phi = 2.0 * math.pi * (np.arange(lon_count // 2) + 0.5) / lon_count
    row, column = [], []
    for b in reversed(range(lon_devices // 2)):
        for a in range(lat_devices // 2):
            row.append(np.repeat(a * lat_rows + np.arange(lat_rows), lon_cols))
            column.append(np.tile(b * lon_cols + np.arange(lon_cols), lat_rows))
    row, column = np.concatenate(row), np.concatenate(column)
    columns = {key: [] for key in CLASSES}
    degrees = {key: [] for key in CLASSES}
    weights = {key: [] for key in CLASSES}
    for m in range(lat_count):
        k = np.arange(1, m + 1)
        log_start = 0.5 * (
            np.log((2 * m + 1) / (4 * math.pi)) + np.sum(np.log((2 * k - 1) / (2 * k)))
        )
        before, current = np.zeros(lat_count // 2), np.exp(log_start + m * np.log(s))
        for l in range(m, lat_count):
            if l > m:
                a = math.sqrt((4.0 * l * l - 1) / (l * l - m * m))
                b = math.sqrt(((l - 1.0) ** 2 - m * m) / (4.0 * (l - 1) ** 2 - 1))
                before, current = current, a * (x * current - b * before)
            for phase, wave in enumerate([np.cos(m * phi), -np.sin(m * phi)][: 1 if m == 0 else 2]):
                key = ((l + m) % 2, phase)
                columns[key].append(current[row] * wave[column])
                degrees[key].append(l)
                weights[key].append((1.0 if m == 0 else 2.0) * 2.0 * math.pi / lon_count)
    tables, selects, starts = [], [], [0]
    for key in CLASSES:
        width = -(-len(columns[key]) // 128) * 128
        fill = width - len(columns[key])
        tables.append(np.pad(np.stack(columns[key], 1), ((0, 0), (0, fill))))
        select = np.arange(lat_count)[:, None] == np.array(degrees[key])[None, :]
        selects.append(np.pad(select * np.array(weights[key])[None, :], ((0, 0), (0, fill))))
        starts.append(starts[-1] + width)
    quad = s * (math.pi / lat_count)
    quad = np.repeat(quad.reshape(lat_devices // 2, lat_rows), lon_cols, axis=1)
    return (
        np.concatenate(tables, 1),
        np.concatenate(selects, 1).astype(np.float32),
        np.tile(quad, (1, 2)).astype(np.float32),
        tuple(starts),
    )


MESH = pl.DeviceIdType.MESH


def worker_columns(lon_devices):
    return lon_devices // 4, lon_devices // 2


NT = (((1,), (1,)), ((), ()))


def block_kernel(
    lat_devices, lon_devices, lat_rows, lon_cols, starts,
    x_hbm, filter_hbm, taps_hbm, norm_hbm, win_hbm, wout_hbm, table_hbm, select_hbm, quad_hbm,
    res,
    xb, filt, taps, norm, win, wout, table, select, quad,
    xf, src, mid, out, dst, filt_in, edge_out, corner_out, edge_in, corner_in, total,
    local_sem, send1, recv1, send2, recv2, halo_send, halo_recv, filt_send, filt_recv,
):
    A, B = lat_devices, lon_devices
    A2, B2 = A // 2, B // 2
    first, count = worker_columns(B)
    workers, devices = A * count, A * B
    groups = workers // B
    points, channels = xb.shape
    own = channels // workers
    rows = own // 2
    whole = rows // 8 * 8
    half = points
    a, b = lax.axis_index("lat"), lax.axis_index("lon")
    me = b * A + a
    worker = jnp.logical_and(b >= first, b < first + count)
    mine = jnp.where(worker, (b - first) * A + a, -1)
    f32, bf16 = jnp.float32, jnp.bfloat16

    fetch = [
        pltpu.make_async_copy(s, d, local_sem.at[i])
        for i, (s, d) in enumerate(
            [(x_hbm, xb), (filter_hbm, filt), (quad_hbm, quad), (table_hbm, table), (select_hbm, select),
             (taps_hbm, taps), (norm_hbm, norm), (win_hbm, win), (wout_hbm, wout)]
        )
    ]
    fetch[0].start()
    barrier = pltpu.get_barrier_semaphore()
    neighbours = [(da, db) for da in (-1, 0, 1) for db in (-1, 0, 1) if (da, db) != (0, 0)]

    def inside(da):
        return jnp.logical_and(a + da >= 0, a + da < A)

    def at(da, db):
        return (a + da, lax.rem(b + db + B, B))

    @pl.when(worker)
    def _():
        def greet(peer, carry):
            @pl.when(peer != me)
            def _():
                pl.semaphore_signal(
                    barrier, inc=1, device_id=(lax.rem(peer, A), lax.div(peer, A)), device_id_type=MESH
                )

            return carry

        lax.fori_loop(0, devices, greet, 0)

    @pl.when(jnp.logical_not(worker))
    def _():
        for da, db in neighbours:
            @pl.when(inside(da))
            def _():
                pl.semaphore_signal(barrier, inc=1, device_id=at(da, db), device_id_type=MESH)

    for copy in fetch[1:]:
        copy.start()

    turn_lat, turn_lon = a >= A2, b >= B2
    p_row = lax.broadcasted_iota(jnp.int32, (points, 2 * half), 0)
    p_col = lax.broadcasted_iota(jnp.int32, (points, 2 * half), 1)

    def turned(index):
        jl, kl = lax.div(index, lon_cols), lax.rem(index, lon_cols)
        jl = jnp.where(turn_lat, lat_rows - 1 - jl, jl)
        kl = jnp.where(turn_lon, lon_cols - 1 - kl, kl)
        return jl * lon_cols + kl

    place = jnp.where(p_row == turned(lax.rem(p_col, half)), 1.0, 0.0)
    place_both = place.astype(bf16)
    place_left = jnp.where(p_col < half, place, 0.0).astype(bf16)
    left = lax.broadcasted_iota(jnp.int32, (rows, 2 * half), 1) < half

    def halves(value):
        if rows == whole:
            return value[:rows], value[rows:]
        rest = value[2 * whole :]
        return (
            jnp.concatenate([value[:whole], rest[: rows - whole]], 0),
            jnp.concatenate([value[whole : 2 * whole], rest[rows - whole :]], 0),
        )

    def joined(upper, lower):
        pieces = [upper[:whole], lower[:whole]]
        if rows > whole:
            pieces += [upper[whole:], lower[whole:]]
        return pieces

    fetch[0].wait()
    xf[...] = xb[...].astype(f32)
    xt = jnp.transpose(xf[...], (1, 0)).astype(bf16)
    xt = jnp.dot(xt, place_both, preferred_element_type=f32)
    for g in range(workers):
        upper, lower = halves(xt[own * g : own * (g + 1)])
        src[g] = jnp.where(left, upper, lower).astype(bf16)

    west, east = [
        jnp.concatenate([xf[k + lon_cols * r : k + lon_cols * r + 1] for r in range(lat_rows)], 0)
        for k in (0, lon_cols - 1)
    ]
    edge_out[0] = west.astype(bf16)
    edge_out[1] = east.astype(bf16)
    chunks = channels // 128
    for i, (r, side) in enumerate([(0, west), (0, east), (lat_rows - 1, west), (lat_rows - 1, east)]):
        parts = [side[r : r + 1, 128 * c : 128 * (c + 1)] for c in range(chunks)]
        parts.append(jnp.zeros((8 - chunks, 128), f32))
        corner_out[i] = jnp.concatenate(parts, 0).astype(bf16)

    def outside(db):
        other = lax.rem(b + db + B, B)
        return jnp.where(jnp.logical_and(other >= first, other < first + count), 0, 1)

    rims = jnp.where(a > 0, 1, 0) + jnp.where(a < A - 1, 1, 0)
    greetings = jnp.where(worker, workers - 1, workers)
    greetings = greetings + rims * outside(0) + (1 + rims) * (outside(-1) + outside(1))
    pl.semaphore_wait(barrier, greetings)

    B4 = B2 // 2
    zone = jnp.where(b < B4, 0, jnp.where(b < B - B4, 1, 2))

    def first_copy(g):
        return pltpu.make_async_remote_copy(
            src_ref=src.at[g], dst_ref=mid.at[me], send_sem=send1, recv_sem=recv1.at[zone],
            device_id=(lax.rem(g, A), first + lax.div(g, A)), device_id_type=MESH,
        )

    @pl.when(worker)
    def _():
        pltpu.make_async_copy(src.at[mine], mid.at[me], recv1.at[zone]).start()

    def first_send(step, carry):
        g = workers - 1 - step

        @pl.when(g != mine)
        def _():
            first_copy(g).start()

        return carry

    lax.fori_loop(0, workers, first_send, 0)

    fetch[1].wait()
    share = lax.rem(a + A * B - b * groups, A)
    owner_row = share < groups
    filt_lon = first + lax.div(b * groups + share, A)
    keeps = jnp.logical_and(owner_row, filt_lon == b)
    gives = jnp.logical_and(owner_row, filt_lon != b)
    filt_copy = pltpu.make_async_remote_copy(
        src_ref=filt, dst_ref=filt_in, send_sem=filt_send, recv_sem=filt_recv,
        device_id=(a, filt_lon), device_id_type=MESH,
    )

    @pl.when(gives)
    def _():
        filt_copy.start()

    @pl.when(keeps)
    def _():
        filt_in[...] = filt[...]

    def halo_copy(da, db):
        if db == 0:
            row = 0 if da < 0 else points - lon_cols
            source, target = xb.at[pl.ds(row, lon_cols)], edge_in.at[1 if da < 0 else 0]
            kind = 0
        elif da == 0:
            slot = 3 if db < 0 else 2
            source, target = edge_out.at[0 if db < 0 else 1], edge_in.at[slot]
            kind = 0
        else:
            index = (0 if da < 0 else 2) + (0 if db < 0 else 1)
            source, target = corner_out.at[index], corner_in.at[3 - index]
            kind = 1
        return pltpu.make_async_remote_copy(
            src_ref=source, dst_ref=target, send_sem=halo_send.at[kind], recv_sem=halo_recv.at[kind],
            device_id=at(da, db), device_id_type=MESH,
        )

    def left_already(blocks, sem):
        pltpu.make_async_copy(blocks, blocks, sem).wait()

    @pl.when(worker)
    def _():
        left_already(src.at[pl.ds(0, workers - 1)], send1)

    @pl.when(jnp.logical_not(worker))
    def _():
        left_already(src, send1)

    for da, db in neighbours:
        @pl.when(inside(da))
        def _():
            halo_copy(da, db).start()

    def index_of(ai, bi):
        return bi * A + ai

    def arrived(zone, start, count):
        blocks = mid.at[pl.ds(start, count)]
        pltpu.make_async_copy(blocks, blocks, recv1.at[zone]).wait()

    def widths(c):
        return pl.ds(starts[c], starts[c + 1] - starts[c])

    def folded(bs):
        tiles = [[] for _ in CLASSES]
        for bi in bs:
            parts = []
            for ai in range(A2):
                f00, f10, f01, f11 = [
                    mid[index_of(i, j)].astype(f32)
                    for i, j in [(ai, bi), (A - 1 - ai, bi), (ai, B - 1 - bi), (A - 1 - ai, B - 1 - bi)]
                ]
                s0, d0, s1, d1 = f00 + f10, f00 - f10, f01 + f11, f01 - f11
                w = quad[ai : ai + 1, :]
                parts.append([(s0 + s1) * w, (d0 + d1) * w, (s0 - s1) * w, (d0 - d1) * w])
            for ai in range(0, A2, 2):
                for c in range(4):
                    u, v = parts[ai][c], parts[ai + 1][c]
                    upper = jnp.where(left, u, pltpu.roll(v, half, 1))
                    lower = jnp.where(left, pltpu.roll(u, half, 1), v)
                    tiles[c].append(jnp.concatenate(joined(upper, lower), 0).astype(bf16))
        return [jnp.concatenate(t, 1) for t in tiles]

    inner = tuple(reversed(range(B2 // 2, B2)))
    outer = tuple(reversed(range(B2 // 2)))
    rows_of = lambda bs: pl.ds((B2 - 1 - bs[0]) * A2 * half, len(bs) * A2 * half)

    def second_copy(o):
        return pltpu.make_async_remote_copy(
            src_ref=out.at[o], dst_ref=dst.at[mine], send_sem=send2, recv_sem=recv2,
            device_id=(lax.rem(o, A), lax.div(o, A)), device_id_type=MESH,
        )

    @pl.when(worker)
    def _():
        for i in (2, 3, 4):
            fetch[i].wait()

        @pl.when(jnp.logical_not(keeps))
        def _():
            pltpu.make_async_remote_copy(
                src_ref=filt, dst_ref=filt_in, send_sem=filt_send, recv_sem=filt_recv,
                device_id=(a, lax.div(mine, groups)), device_id_type=MESH,
            ).wait_recv()

        held = filt_in.shape[1]
        r = lax.broadcasted_iota(jnp.int32, (own, held), 0)
        c = lax.broadcasted_iota(jnp.int32, (own, held), 1)
        pick = jnp.where(c == r + lax.rem(mine, groups) * own, 1.0, 0.0)
        rows = lax.dot_general(pick, filt_in[...], NT, precision=highest, preferred_element_type=f32)
        gain = jnp.dot(rows, select[...], precision=highest, preferred_element_type=f32)

        arrived(1, A * B4, devices - 2 * A * B4)
        acc = [
            jnp.dot(t, table[rows_of(inner), widths(i)], preferred_element_type=f32)
            for i, t in enumerate(folded(inner))
        ]
        arrived(0, 0, A * B4)
        arrived(2, devices - A * B4, A * B4)
        for i, t in enumerate(folded(outer)):
            acc[i] = acc[i] + jnp.dot(t, table[rows_of(outer), widths(i)], preferred_element_type=f32)
        coef = [(acc[i] * gain[:, starts[i] : starts[i + 1]]).astype(bf16) for i in range(4)]

        for bs in (outer, inner):
            grid = [
                lax.dot_general(coef[i], table[rows_of(bs), widths(i)], NT, preferred_element_type=f32)
                for i in range(4)
            ]
            for n, bi in enumerate(bs):
                for ai in range(0, A2, 2):
                    at_lane = (n * A2 + ai) * half
                    pp, mp, pm, mm = [g[:, at_lane : at_lane + 2 * half] for g in grid]
                    e0, e1, o0, o1 = pp + mp, pp - mp, pm + mm, pm - mm
                    for i, j, value in [(0, 0, e0 + o0), (1, 0, e1 + o1), (0, 1, e0 - o0), (1, 1, e1 - o1)]:
                        upper, lower = halves(value)
                        bj = B - 1 - bi if j else bi
                        a0, a1 = (A - 1 - ai, A - 2 - ai) if i else (ai, ai + 1)
                        out[index_of(a0, bj)] = jnp.where(left, upper, pltpu.roll(lower, half, 1)).astype(bf16)
                        out[index_of(a1, bj)] = jnp.where(left, pltpu.roll(upper, half, 1), lower).astype(bf16)

            def near_send(step, carry):
                second_copy(lax.rem(step, B4) * A + lax.div(step, B4)).start()
                return carry

            def second_send(o, carry):
                @pl.when(o != me)
                def _():
                    second_copy(o).start()

                return carry

            if bs == outer:
                lax.fori_loop(0, B4, near_send, 0)
            else:
                lax.fori_loop(B4, A * B4, near_send, 0)
                lax.fori_loop(A * B4, devices, second_send, 0)
        pltpu.make_async_copy(out.at[me], dst.at[mine], recv2).start()

    @pl.when(a == 0)
    def _():
        edge_in[0] = jnp.zeros(edge_in.shape[1:], bf16)
        corner_in[0] = jnp.zeros(corner_in.shape[1:], bf16)
        corner_in[1] = jnp.zeros(corner_in.shape[1:], bf16)

    @pl.when(a == A - 1)
    def _():
        edge_in[1] = jnp.zeros(edge_in.shape[1:], bf16)
        corner_in[2] = jnp.zeros(corner_in.shape[1:], bf16)
        corner_in[3] = jnp.zeros(corner_in.shape[1:], bf16)

    pole = rims == 1

    def halo_wait(sems):
        for edges, corners, case in [(3, 2, pole), (4, 4, jnp.logical_not(pole))]:
            @pl.when(case)
            def _():
                for kind, blocks in enumerate([edge_in.at[pl.ds(0, edges)], corner_in.at[pl.ds(0, corners)]]):
                    pltpu.make_async_copy(blocks, blocks, sems.at[kind]).wait()

    halo_wait(halo_recv)

    fetch[5].wait()
    weight = taps[...]
    grid_rows = [edge_in[0].astype(f32)]
    grid_rows += [xf[pl.ds(lon_cols * r, lon_cols), :] for r in range(lat_rows)]
    grid_rows += [edge_in[1].astype(f32)]

    def corner(i):
        piece = corner_in[i].astype(f32)
        return jnp.concatenate([piece[c : c + 1] for c in range(chunks)], 1)

    west, east = edge_in[2].astype(f32), edge_in[3].astype(f32)
    west = [corner(0)] + [west[r : r + 1] for r in range(lat_rows)] + [corner(2)]
    east = [corner(1)] + [east[r : r + 1] for r in range(lat_rows)] + [corner(3)]
    sub = lax.broadcasted_iota(jnp.int32, (lon_cols, channels), 0)
    shifted = []
    for r in range(lat_rows + 2):
        here = grid_rows[r]
        before = jnp.where(sub == 0, west[r], pltpu.roll(here, 1, 0))
        after = jnp.where(sub == lon_cols - 1, east[r], pltpu.roll(here, lon_cols - 1, 0))
        shifted.append((before, here, after))
    for r in range(lat_rows):
        mix = sum(
            weight[3 * i + j : 3 * i + j + 1] * shifted[r + i][j] for i in range(3) for j in range(3)
        )
        mix = mix.astype(bf16).astype(f32)
        total[pl.ds(lon_cols * r, lon_cols), :] = grid_rows[r + 1] + mix

    for i in (6, 7, 8):
        fetch[i].wait()

    pltpu.make_async_copy(dst, dst, recv2).wait()
    parts = []
    for g in range(workers):
        piece = dst[g].astype(f32)
        parts += joined(piece, pltpu.roll(piece, half, 1))
    spectral = jnp.concatenate(parts, 0).astype(bf16)
    spectral = lax.dot_general(place_left, spectral, NT, preferred_element_type=f32)
    summed = (total[...] + spectral).astype(bf16).astype(f32)
    scale = lax.rsqrt(jnp.mean(summed * summed, axis=1, keepdims=True) + epsilon_norm)
    scaled = (summed * norm[...][None, :]).astype(bf16)
    hidden = jnp.dot(scaled, win[...], preferred_element_type=f32) * scale
    hidden = (0.5 * hidden * (1.0 + lax.erf(hidden * math.sqrt(0.5)))).astype(bf16)
    result = summed + jnp.dot(hidden, wout[...], preferred_element_type=f32)
    res[...] = result.astype(bf16)

    @pl.when(worker)
    def _():
        left_already(out.at[pl.ds(0, devices - 1)], send2)

    @pl.when(gives)
    def _():
        filt_copy.wait_send()

    halo_wait(halo_send)

    @pl.when(jnp.logical_not(worker))
    def _():
        for i in (2, 3, 4):
            fetch[i].wait()


def sphere_block(lat_devices, lon_devices, latent_field, spectral_filter, conv_weight, norm_gain, weight_in, weight_out):
    channels, lat_rows, lon_cols = latent_field.shape
    points = lat_rows * lon_cols
    workers = lat_devices * worker_columns(lon_devices)[1]
    own = channels // workers
    table, select, quad, starts = folded_tables(lat_devices, lon_devices, lat_rows, lon_cols)
    table = jnp.asarray(table.astype(jnp.bfloat16))
    args = [
        jnp.transpose(latent_field, (1, 2, 0)).reshape(points, channels),
        spectral_filter.T,
        conv_weight,
        norm_gain,
        weight_in,
        weight_out,
        table,
        jnp.asarray(select),
        jnp.asarray(quad),
    ]
    order = range(len(args))
    copies = [pltpu.VMEM(args[i].shape, args[i].dtype) for i in order]
    devices = lat_devices * lon_devices
    bf16, f32, dma = jnp.bfloat16, jnp.float32, pltpu.SemaphoreType.DMA
    scratch = [
        pltpu.VMEM((points, channels), f32),
        pltpu.VMEM((workers, own // 2, 128), bf16),
        pltpu.VMEM((devices, own // 2, 128), bf16),
        pltpu.VMEM((devices, own // 2, 128), bf16),
        pltpu.VMEM((workers, own // 2, 128), bf16),
        pltpu.VMEM(args[1].shape, f32),
        pltpu.VMEM((2, lat_rows, channels), bf16),
        pltpu.VMEM((4, 8, 128), bf16),
        pltpu.VMEM((4, lat_rows, channels), bf16),
        pltpu.VMEM((4, 8, 128), bf16),
        pltpu.VMEM((points, channels), f32),
        dma((len(args),)), dma, dma((3,)), dma, dma, dma((2,)), dma((2,)), dma, dma,
    ]
    result = pl.pallas_call(
        functools.partial(block_kernel, lat_devices, lon_devices, lat_rows, lon_cols, starts),
        out_shape=pltpu.VMEM((points, channels), bf16),
        in_specs=[pl.BlockSpec(memory_space=pl.ANY)] * len(args),
        out_specs=pl.BlockSpec(memory_space=pltpu.VMEM),
        scratch_shapes=copies + scratch,
        compiler_params=pltpu.CompilerParams(collective_id=0, has_side_effects=True),
        name="sphere_block",
    )(*args)
    return jnp.transpose(result.reshape(lat_rows, lon_cols, channels), (2, 0, 1))


def fits_block(lat_devices, lon_devices, latent_field):
    channels, lat_rows, lon_cols = latent_field.shape
    workers = lat_devices * worker_columns(lon_devices)[1]
    return (
        lat_devices % 4 == 0
        and lon_devices % 4 == 0
        and lat_rows == 8
        and lon_cols == 8
        and channels % (8 * workers) == 0
        and channels // workers % 2 == 0
        and channels % 128 == 0
        and channels <= 1024
    )


def block_or_banded(lat_devices, lon_devices, *arguments):
    if fits_block(lat_devices, lon_devices, arguments[0]):
        return sphere_block(lat_devices, lon_devices, *arguments)
    return on_device(*arguments)


def solution(mesh):
    return jax.shard_map(
        functools.partial(block_or_banded, mesh.shape["lat"], mesh.shape["lon"]),
        mesh=mesh,
        in_specs=(P(None, "lat", "lon"), P("lon", None), P(), P(), P(), P()),
        out_specs=P(None, "lat", "lon"),
        check_vma=False,
    )
```

```python
import functools
import math

import jax
import jax.numpy as jnp
import numpy as np
from jax import lax
from jax.experimental import pallas as pl
from jax.experimental.pallas import tpu as pltpu
from jax.sharding import PartitionSpec as P

highest = lax.Precision.HIGHEST
epsilon_norm = 1e-06


def with_halo(cells, sides, width):
    for axis, dim in sides:
        count = lax.axis_size(axis)
        ends = count - 1
        head = lax.slice_in_dim(cells, 0, width, axis=dim)
        tail = lax.slice_in_dim(cells, cells.shape[dim] - width, cells.shape[dim], axis=dim)
        cells = jnp.concatenate(
            [
                lax.ppermute(tail, axis, [(i, (i + 1) % count) for i in range(ends)]),
                cells,
                lax.ppermute(head, axis, [((i + 1) % count, i) for i in range(ends)]),
            ],
            axis=dim,
        )
    return cells


def quadrature(lat_count):
    colatitude = (jnp.arange(lat_count, dtype=jnp.float32) + 0.5) * (math.pi / lat_count)
    return jnp.sin(colatitude) * (math.pi / lat_count)


def fourier_tables(lon_count, mode_count):
    wave_index = (
        jnp.arange(mode_count, dtype=jnp.int32)[:, None]
        * jnp.arange(lon_count, dtype=jnp.int32)[None, :]
    )
    phase_angle = (wave_index % lon_count).astype(jnp.float32) * (2.0 * math.pi / lon_count)
    cosine = jnp.cos(phase_angle)
    sine_table = jnp.sin(phase_angle)
    angle_step = 2.0 * math.pi / lon_count
    forward = jnp.concatenate([angle_step * cosine, -angle_step * sine_table], axis=0)
    weight = jnp.where(jnp.arange(mode_count, dtype=jnp.int32) == 0, 1.0, 2.0).astype(jnp.float32)[
        :, None
    ]
    inverse = jnp.concatenate([weight * cosine, -weight * sine_table], axis=0)
    return (forward, inverse)


def legendre_rows(order_ids, lat_count):
    colatitude = (jnp.arange(lat_count, dtype=jnp.float32) + 0.5) * (math.pi / lat_count)
    cosine = jnp.cos(colatitude)
    sine_col = jnp.sin(colatitude)
    order_f = order_ids.astype(jnp.float32)
    factor_index = jnp.arange(1, lat_count, dtype=jnp.float32)
    ratio_log = jnp.log((2.0 * factor_index - 1.0) / (2.0 * factor_index))
    included = (factor_index[None, :] <= order_f[:, None]).astype(jnp.float32)
    log_factor = jnp.sum(included * ratio_log[None, :], axis=1)
    start_log = 0.5 * jnp.log((2.0 * order_f + 1.0) / (4.0 * math.pi)) + 0.5 * log_factor
    start_log = start_log[:, None] + order_f[:, None] * jnp.log(sine_col)[None, :]
    blank_rows = jnp.zeros((order_ids.shape[0], lat_count), jnp.float32)
    order_col = order_f[:, None]

    def advance(state_carry, degree):
        before, current, scale_log = state_carry
        degree_f = degree.astype(jnp.float32)
        alpha_term = jnp.sqrt(
            (4.0 * degree_f * degree_f - 1.0)
            / jnp.maximum(degree_f * degree_f - order_col * order_col, 1.0)
        )
        beta_term = jnp.sqrt(
            jnp.maximum((degree_f - 1.0) ** 2 - order_col * order_col, 0.0)
            / jnp.maximum(4.0 * (degree_f - 1.0) ** 2 - 1.0, 1.0)
        )
        stepped = alpha_term * (cosine[None, :] * current - beta_term * before)
        at_start = order_ids[:, None] == degree
        past_start = order_ids[:, None] < degree
        fresh_value = jnp.where(at_start, 1.0, jnp.where(past_start, stepped, 0.0))
        fresh_log = jnp.where(at_start, start_log, scale_log)
        entry_value = fresh_value * jnp.exp(fresh_log)
        rescale = jnp.where(
            past_start | at_start, jnp.maximum(jnp.abs(fresh_value), jnp.abs(current)), 1.0
        )
        return (
            (current / rescale, fresh_value / rescale, fresh_log + jnp.log(rescale)),
            entry_value,
        )

    degrees = jnp.arange(lat_count, dtype=jnp.int32)
    unused, legendre = lax.scan(advance, (blank_rows, blank_rows, blank_rows), degrees)
    return legendre


def filter_modes(banded, legendre, filter_block, quad_weights):
    coefficients = jnp.einsum(
        "lmj,pmcj->pmcl", legendre, banded * quad_weights[None, None, None, :], precision=highest
    )
    coefficients = coefficients * filter_block[None, None, :, :]
    return jnp.einsum("lmj,pmcl->pmcj", legendre, coefficients, precision=highest)


def wrap_columns(extended):
    return jnp.concatenate([extended[:, :, -1:], extended, extended[:, :, :1]], axis=2)


def depthwise_core(extended, kernel, lat_rows, lon_cols):
    accumulated = jnp.zeros((extended.shape[0], lat_rows, lon_cols), jnp.float32)
    for row_shift in range(3):
        for col_shift in range(3):
            piece = extended[
                :, row_shift : row_shift + lat_rows, col_shift : col_shift + lon_cols
            ].astype(jnp.float32)
            accumulated = accumulated + kernel[3 * row_shift + col_shift][:, None, None] * piece
    return accumulated.astype(jnp.bfloat16)


def channel_mlp(summed_low, norm_gain, weight_in, weight_out):
    summed = summed_low.astype(jnp.float32)
    scale_inv = lax.rsqrt(jnp.mean(summed * summed, axis=0, keepdims=True) + epsilon_norm)
    normed = (summed * scale_inv * norm_gain[:, None]).astype(jnp.bfloat16)
    hidden = lax.dot_general(
        weight_in, normed, (((0,), (0,)), ((), ())), preferred_element_type=jnp.float32
    )
    hidden = jax.nn.gelu(hidden, approximate=False).astype(jnp.bfloat16)
    result = summed + lax.dot_general(
        weight_out, hidden, (((0,), (0,)), ((), ())), preferred_element_type=jnp.float32
    )
    return result.astype(jnp.bfloat16)


def add_three(first, second, third):
    total = first.astype(jnp.float32) + second.astype(jnp.float32) + third.astype(jnp.float32)
    return total.astype(jnp.bfloat16)


def on_device(latent_field, spectral_filter, conv_weight, norm_gain, weight_in, weight_out):
    channels, lat_rows, lon_cols = latent_field.shape
    sector_count = lax.axis_size("lon")
    lat_count = lat_rows * lax.axis_size("lat")
    lon_count = lon_cols * sector_count
    chan_block = channels // sector_count
    spread = lax.all_to_all(latent_field, "lon", split_axis=0, concat_axis=2, tiled=True)
    forward, inverse = fourier_tables(lon_count, lat_count)
    flattened = spread.astype(jnp.float32).reshape(chan_block * lat_rows, lon_count)
    spectrum = lax.dot_general(forward, flattened, (((1,), (1,)), ((), ())), precision=highest)
    spectrum = spectrum.reshape(2, lat_count, chan_block, lat_rows)
    banded = lax.all_to_all(spectrum, "lat", split_axis=1, concat_axis=3, tiled=True)
    order_ids = lax.axis_index("lat") * lat_rows + jnp.arange(lat_rows, dtype=jnp.int32)
    legendre = legendre_rows(order_ids, lat_count)
    synthesized = filter_modes(banded, legendre, spectral_filter, quadrature(lat_count))
    regathered = lax.all_to_all(synthesized, "lat", split_axis=3, concat_axis=1, tiled=True)
    regridded = lax.dot_general(
        regathered.reshape(2 * lat_count, chan_block * lat_rows),
        inverse,
        (((0,), (0,)), ((), ())),
        precision=highest,
    )
    spectral = regridded.reshape(chan_block, lat_rows, lon_count).astype(jnp.bfloat16)
    own_kernel = lax.dynamic_slice_in_dim(
        conv_weight, lax.axis_index("lon") * chan_block, chan_block, 1
    )
    rimmed = with_halo(spread, (("lat", 1),), 1)
    sector_mix = depthwise_core(wrap_columns(rimmed), own_kernel, lat_rows, lon_count)
    sector_sum = add_three(spread, spectral, sector_mix)
    summed = lax.all_to_all(sector_sum, "lon", split_axis=2, concat_axis=0, tiled=True)
    summed = summed.reshape(channels, lat_rows * lon_cols)
    result = channel_mlp(summed, norm_gain, weight_in, weight_out)
    return result.reshape(channels, lat_rows, lon_cols)


CLASSES = ((0, 0), (1, 0), (0, 1), (1, 1))


def folded_tables(lat_devices, lon_devices, lat_rows, lon_cols):
    lat_count, lon_count = lat_devices * lat_rows, lon_devices * lon_cols
    theta = (np.arange(lat_count // 2) + 0.5) * (math.pi / lat_count)
    x, s = np.cos(theta), np.sin(theta)
    phi = 2.0 * math.pi * (np.arange(lon_count // 2) + 0.5) / lon_count
    row, column = [], []
    for b in reversed(range(lon_devices // 2)):
        for a in range(lat_devices // 2):
            row.append(np.repeat(a * lat_rows + np.arange(lat_rows), lon_cols))
            column.append(np.tile(b * lon_cols + np.arange(lon_cols), lat_rows))
    row, column = np.concatenate(row), np.concatenate(column)
    columns = {key: [] for key in CLASSES}
    degrees = {key: [] for key in CLASSES}
    weights = {key: [] for key in CLASSES}
    for m in range(lat_count):
        k = np.arange(1, m + 1)
        log_start = 0.5 * (
            np.log((2 * m + 1) / (4 * math.pi)) + np.sum(np.log((2 * k - 1) / (2 * k)))
        )
        before, current = np.zeros(lat_count // 2), np.exp(log_start + m * np.log(s))
        for l in range(m, lat_count):
            if l > m:
                a = math.sqrt((4.0 * l * l - 1) / (l * l - m * m))
                b = math.sqrt(((l - 1.0) ** 2 - m * m) / (4.0 * (l - 1) ** 2 - 1))
                before, current = current, a * (x * current - b * before)
            for phase, wave in enumerate([np.cos(m * phi), -np.sin(m * phi)][: 1 if m == 0 else 2]):
                key = ((l + m) % 2, phase)
                columns[key].append(current[row] * wave[column])
                degrees[key].append(l)
                weights[key].append((1.0 if m == 0 else 2.0) * 2.0 * math.pi / lon_count)
    tables, selects, starts = [], [], [0]
    for key in CLASSES:
        width = -(-len(columns[key]) // 128) * 128
        fill = width - len(columns[key])
        tables.append(np.pad(np.stack(columns[key], 1), ((0, 0), (0, fill))))
        select = np.arange(lat_count)[:, None] == np.array(degrees[key])[None, :]
        selects.append(np.pad(select * np.array(weights[key])[None, :], ((0, 0), (0, fill))))
        starts.append(starts[-1] + width)
    quad = s * (math.pi / lat_count)
    quad = np.repeat(quad.reshape(lat_devices // 2, lat_rows), lon_cols, axis=1)
    return (
        np.concatenate(tables, 1),
        np.concatenate(selects, 1).astype(np.float32),
        np.tile(quad, (1, 2)).astype(np.float32),
        tuple(starts),
    )


MESH = pl.DeviceIdType.MESH


def worker_places(lat_devices, lon_devices):
    quarter = lon_devices // 4
    second = [(a, b) for b in range(quarter, 2 * quarter) for a in range(lat_devices)]
    third = [(a, b) for b in range(2 * quarter, 3 * quarter) for a in range(lat_devices - 1)]
    return [(0, b) for b in range(quarter)] + second + third


NT = (((1,), (1,)), ((), ()))


def block_kernel(
    lat_devices, lon_devices, lat_rows, lon_cols, starts,
    x_hbm, filter_hbm, taps_hbm, norm_hbm, win_hbm, wout_hbm, table_hbm, select_hbm, quad_hbm,
    res,
    xb, filt, taps, norm, win, wout, table, select, quad,
    xf, src, mid, out, dst, filt_in, edge_out, corner_out, edge_in, corner_in, total,
    local_sem, send1, recv1, send2, recv2, halo_send, halo_recv, filt_send, filt_recv, wrap,
):
    A, B = lat_devices, lon_devices
    A2, B2 = A // 2, B // 2
    places = worker_places(A, B)
    workers, devices = len(places), A * B
    groups = workers // B
    points, channels = xb.shape
    own = channels // workers
    rows = own // 2
    whole = rows // 8 * 8
    half = points
    a, b = lax.axis_index("lat"), lax.axis_index("lon")
    me = b * A + a
    quarter = B // 4

    def works(a, b):
        z = lax.div(b, quarter)
        return jnp.logical_or(
            z == 1, jnp.logical_or(jnp.logical_and(z == 2, a < A - 1), jnp.logical_and(z == 0, a == 0))
        )

    worker = works(a, b)
    mine = jnp.where(
        b < quarter,
        b,
        quarter
        + jnp.where(b < 2 * quarter, (b - quarter) * A + a, quarter * A + (b - 2 * quarter) * (A - 1) + a),
    )
    mine = jnp.where(worker, mine, -1)
    f32, bf16 = jnp.float32, jnp.bfloat16

    fetch = [
        pltpu.make_async_copy(s, d, local_sem.at[i])
        for i, (s, d) in enumerate(
            [(x_hbm, xb), (filter_hbm, filt), (quad_hbm, quad), (table_hbm, table), (select_hbm, select),
             (taps_hbm, taps), (norm_hbm, norm), (win_hbm, win), (wout_hbm, wout)]
        )
    ]
    fetch[0].start()
    barrier = pltpu.get_barrier_semaphore()
    neighbours = [(da, db) for da in (-1, 0, 1) for db in (-1, 0, 1) if (da, db) != (0, 0)]

    def inside(da):
        return jnp.logical_and(a + da >= 0, a + da < A)

    def at(da, db):
        return (a + da, lax.rem(b + db + B, B))

    @pl.when(worker)
    def _():
        def greet(peer, carry):
            @pl.when(peer != me)
            def _():
                pl.semaphore_signal(
                    barrier, inc=1, device_id=(lax.rem(peer, A), lax.div(peer, A)), device_id_type=MESH
                )

            return carry

        lax.fori_loop(0, devices, greet, 0)

    @pl.when(jnp.logical_not(worker))
    def _():
        for da, db in neighbours:
            @pl.when(jnp.logical_and(inside(da), b < B - 1) if db > 0 else inside(da))
            def _():
                pl.semaphore_signal(barrier, inc=1, device_id=at(da, db), device_id_type=MESH)

    for copy in fetch[1:]:
        copy.start()

    turn_lat, turn_lon = a >= A2, b >= B2
    p_row = lax.broadcasted_iota(jnp.int32, (points, 2 * half), 0)
    p_col = lax.broadcasted_iota(jnp.int32, (points, 2 * half), 1)

    def turned(index):
        jl, kl = lax.div(index, lon_cols), lax.rem(index, lon_cols)
        jl = jnp.where(turn_lat, lat_rows - 1 - jl, jl)
        kl = jnp.where(turn_lon, lon_cols - 1 - kl, kl)
        return jl * lon_cols + kl

    place = jnp.where(p_row == turned(lax.rem(p_col, half)), 1.0, 0.0)
    place_both = place.astype(bf16)
    place_left = jnp.where(p_col < half, place, 0.0).astype(bf16)
    left = lax.broadcasted_iota(jnp.int32, (rows, 2 * half), 1) < half

    def halves(value):
        if rows == whole:
            return value[:rows], value[rows:]
        rest = value[2 * whole :]
        return (
            jnp.concatenate([value[:whole], rest[: rows - whole]], 0),
            jnp.concatenate([value[whole : 2 * whole], rest[rows - whole :]], 0),
        )

    def joined(upper, lower):
        pieces = [upper[:whole], lower[:whole]]
        if rows > whole:
            pieces += [upper[whole:], lower[whole:]]
        return pieces

    fetch[0].wait()
    xf[...] = xb[...].astype(f32)
    xt = jnp.transpose(xf[...], (1, 0)).astype(bf16)
    xt = jnp.dot(xt, place_both, preferred_element_type=f32)
    for g in range(workers):
        upper, lower = halves(xt[own * g : own * (g + 1)])
        src[g] = jnp.where(left, upper, lower).astype(bf16)

    west, east = [
        jnp.concatenate([xf[k + lon_cols * r : k + lon_cols * r + 1] for r in range(lat_rows)], 0)
        for k in (0, lon_cols - 1)
    ]
    edge_out[0] = west.astype(bf16)
    edge_out[1] = east.astype(bf16)
    chunks = channels // 128
    for i, (r, side) in enumerate([(0, west), (0, east), (lat_rows - 1, west), (lat_rows - 1, east)]):
        parts = [side[r : r + 1, 128 * c : 128 * (c + 1)] for c in range(chunks)]
        parts.append(jnp.zeros((8 - chunks, 128), f32))
        corner_out[i] = jnp.concatenate(parts, 0).astype(bf16)

    rims = jnp.where(a > 0, 1, 0) + jnp.where(a < A - 1, 1, 0)
    greetings = jnp.where(worker, workers - 1, workers)
    for da, db in neighbours:
        other = at(da, db)
        known = jnp.logical_and(inside(da), jnp.logical_not(works(*other)))
        if db < 0:
            known = jnp.logical_and(known, b > 0)
        greetings = greetings + jnp.where(known, 1, 0)
    pl.semaphore_wait(barrier, greetings)

    @pl.when(b == B - 1)
    def _():
        for da in (-1, 0, 1):
            @pl.when(inside(da))
            def _():
                pl.semaphore_signal(wrap, inc=1, device_id=(a + da, 0), device_id_type=MESH)

    B4 = B2 // 2
    zone = jnp.where(b < B4, 0, jnp.where(b < B - B4, 1, 2))

    def first_copy(g):
        return pltpu.make_async_remote_copy(
            src_ref=src.at[g], dst_ref=mid.at[me], send_sem=send1, recv_sem=recv1.at[zone],
            device_id=places[g], device_id_type=MESH,
        )

    @pl.when(worker)
    def _():
        pltpu.make_async_copy(src.at[mine], mid.at[me], recv1.at[zone]).start()

    for order, case in [(reversed(range(workers)), b < B2), (range(workers), b >= B2)]:
        for g in order:
            @pl.when(jnp.logical_and(mine != g, case))
            def _():
                first_copy(g).start()

    fetch[1].wait()
    def filt_copy(g):
        return pltpu.make_async_remote_copy(
            src_ref=filt, dst_ref=filt_in, send_sem=filt_send.at[g % groups], recv_sem=filt_recv,
            device_id=places[g], device_id_type=MESH,
        )

    givers, keeps = [], False
    for g, (ag, bg) in enumerate(places):
        if bg == g // groups:
            keeps = jnp.logical_or(keeps, mine == g)
        else:
            givers.append((g, me == (g // groups) * A + ag))
    for g, gives in givers:
        @pl.when(gives)
        def _():
            filt_copy(g).start()

    @pl.when(keeps)
    def _():
        filt_in[...] = filt[...]

    def halo_copy(da, db):
        if db == 0:
            row = 0 if da < 0 else points - lon_cols
            source, target = xb.at[pl.ds(row, lon_cols)], edge_in.at[1 if da < 0 else 0]
            kind = 0
        elif da == 0:
            slot = 3 if db < 0 else 2
            source, target = edge_out.at[0 if db < 0 else 1], edge_in.at[slot]
            kind = 0
        else:
            index = (0 if da < 0 else 2) + (0 if db < 0 else 1)
            source, target = corner_out.at[index], corner_in.at[3 - index]
            kind = 1
        return pltpu.make_async_remote_copy(
            src_ref=source, dst_ref=target, send_sem=halo_send.at[kind], recv_sem=halo_recv.at[kind],
            device_id=at(da, db), device_id_type=MESH,
        )

    def left_already(blocks, sem):
        pltpu.make_async_copy(blocks, blocks, sem).wait()

    @pl.when(worker)
    def _():
        left_already(src.at[pl.ds(0, workers - 1)], send1)

    @pl.when(jnp.logical_not(worker))
    def _():
        left_already(src, send1)

    @pl.when(b == 0)
    def _():
        pl.semaphore_wait(wrap, 1 + rims)

    for da, db in neighbours:
        @pl.when(inside(da))
        def _():
            halo_copy(da, db).start()

    def index_of(ai, bi):
        return bi * A + ai

    def arrived(zone, start, count):
        blocks = mid.at[pl.ds(start, count)]
        pltpu.make_async_copy(blocks, blocks, recv1.at[zone]).wait()

    def widths(c):
        return pl.ds(starts[c], starts[c + 1] - starts[c])

    def folded(bs):
        tiles = [[] for _ in CLASSES]
        for bi in bs:
            parts = []
            for ai in range(A2):
                f00, f10, f01, f11 = [
                    mid[index_of(i, j)].astype(f32)
                    for i, j in [(ai, bi), (A - 1 - ai, bi), (ai, B - 1 - bi), (A - 1 - ai, B - 1 - bi)]
                ]
                s0, d0, s1, d1 = f00 + f10, f00 - f10, f01 + f11, f01 - f11
                w = quad[ai : ai + 1, :]
                parts.append([(s0 + s1) * w, (d0 + d1) * w, (s0 - s1) * w, (d0 - d1) * w])
            for ai in range(0, A2, 2):
                for c in range(4):
                    u, v = parts[ai][c], parts[ai + 1][c]
                    upper = jnp.where(left, u, pltpu.roll(v, half, 1))
                    lower = jnp.where(left, pltpu.roll(u, half, 1), v)
                    tiles[c].append(jnp.concatenate(joined(upper, lower), 0).astype(bf16))
        return [jnp.concatenate(t, 1) for t in tiles]

    inner = tuple(reversed(range(B2 // 2, B2)))
    outer = tuple(reversed(range(B2 // 2)))
    rows_of = lambda bs: pl.ds((B2 - 1 - bs[0]) * A2 * half, len(bs) * A2 * half)

    def second_copy(o):
        return pltpu.make_async_remote_copy(
            src_ref=out.at[o], dst_ref=dst.at[mine], send_sem=send2, recv_sem=recv2,
            device_id=(lax.rem(o, A), lax.div(o, A)), device_id_type=MESH,
        )

    @pl.when(worker)
    def _():
        for i in (2, 3, 4):
            fetch[i].wait()

        @pl.when(jnp.logical_not(keeps))
        def _():
            pltpu.make_async_copy(filt, filt_in, filt_recv).wait()

        held = filt_in.shape[1]
        r = lax.broadcasted_iota(jnp.int32, (own, held), 0)
        c = lax.broadcasted_iota(jnp.int32, (own, held), 1)
        pick = jnp.where(c == r + lax.rem(mine, groups) * own, 1.0, 0.0)
        rows = lax.dot_general(pick, filt_in[...], NT, precision=highest, preferred_element_type=f32)
        gain = jnp.dot(rows, select[...], precision=highest, preferred_element_type=f32)

        arrived(1, A * B4, devices - 2 * A * B4)
        acc = [
            jnp.dot(t, table[rows_of(inner), widths(i)], preferred_element_type=f32)
            for i, t in enumerate(folded(inner))
        ]
        arrived(0, 0, A * B4)
        arrived(2, devices - A * B4, A * B4)
        for i, t in enumerate(folded(outer)):
            acc[i] = acc[i] + jnp.dot(t, table[rows_of(outer), widths(i)], preferred_element_type=f32)
        coef = [(acc[i] * gain[:, starts[i] : starts[i + 1]]).astype(bf16) for i in range(4)]

        for bs in (outer, inner):
            grid = [
                lax.dot_general(coef[i], table[rows_of(bs), widths(i)], NT, preferred_element_type=f32)
                for i in range(4)
            ]
            for n, bi in enumerate(bs):
                for ai in range(0, A2, 2):
                    at_lane = (n * A2 + ai) * half
                    pp, mp, pm, mm = [g[:, at_lane : at_lane + 2 * half] for g in grid]
                    e0, e1, o0, o1 = pp + mp, pp - mp, pm + mm, pm - mm
                    for i, j, value in [(0, 0, e0 + o0), (1, 0, e1 + o1), (0, 1, e0 - o0), (1, 1, e1 - o1)]:
                        upper, lower = halves(value)
                        bj = B - 1 - bi if j else bi
                        a0, a1 = (A - 1 - ai, A - 2 - ai) if i else (ai, ai + 1)
                        out[index_of(a0, bj)] = jnp.where(left, upper, pltpu.roll(lower, half, 1)).astype(bf16)
                        out[index_of(a1, bj)] = jnp.where(left, pltpu.roll(upper, half, 1), lower).astype(bf16)

            def near_send(step, carry):
                o = lax.rem(step, B4) * A + lax.div(step, B4)

                @pl.when(o != me)
                def _():
                    second_copy(o).start()

                return carry

            def second_send(o, carry):
                @pl.when(o != me)
                def _():
                    second_copy(o).start()

                return carry

            def far_send(step, carry):
                return second_send(A * (B - B4) - 1 - step, carry)

            @pl.when(b < quarter)
            def _():
                if bs == outer:
                    lax.fori_loop(A * (B - B4), devices, second_send, 0)
                else:
                    lax.fori_loop(0, A * (B - B4), far_send, 0)

            @pl.when(b >= quarter)
            def _():
                if bs == outer:
                    lax.fori_loop(0, B4, near_send, 0)
                else:
                    lax.fori_loop(B4, A * B4, near_send, 0)
                    lax.fori_loop(A * B4, devices, second_send, 0)

        pltpu.make_async_copy(out.at[me], dst.at[mine], recv2).start()

    @pl.when(a == 0)
    def _():
        edge_in[0] = jnp.zeros(edge_in.shape[1:], bf16)
        corner_in[0] = jnp.zeros(corner_in.shape[1:], bf16)
        corner_in[1] = jnp.zeros(corner_in.shape[1:], bf16)

    @pl.when(a == A - 1)
    def _():
        edge_in[1] = jnp.zeros(edge_in.shape[1:], bf16)
        corner_in[2] = jnp.zeros(corner_in.shape[1:], bf16)
        corner_in[3] = jnp.zeros(corner_in.shape[1:], bf16)

    pole = rims == 1

    def halo_wait(sems):
        for edges, corners, case in [(3, 2, pole), (4, 4, jnp.logical_not(pole))]:
            @pl.when(case)
            def _():
                for kind, blocks in enumerate([edge_in.at[pl.ds(0, edges)], corner_in.at[pl.ds(0, corners)]]):
                    pltpu.make_async_copy(blocks, blocks, sems.at[kind]).wait()

    halo_wait(halo_recv)

    fetch[5].wait()
    weight = taps[...]
    grid_rows = [edge_in[0].astype(f32)]
    grid_rows += [xf[pl.ds(lon_cols * r, lon_cols), :] for r in range(lat_rows)]
    grid_rows += [edge_in[1].astype(f32)]

    def corner(i):
        piece = corner_in[i].astype(f32)
        return jnp.concatenate([piece[c : c + 1] for c in range(chunks)], 1)

    west, east = edge_in[2].astype(f32), edge_in[3].astype(f32)
    west = [corner(0)] + [west[r : r + 1] for r in range(lat_rows)] + [corner(2)]
    east = [corner(1)] + [east[r : r + 1] for r in range(lat_rows)] + [corner(3)]
    sub = lax.broadcasted_iota(jnp.int32, (lon_cols, channels), 0)
    shifted = []
    for r in range(lat_rows + 2):
        here = grid_rows[r]
        before = jnp.where(sub == 0, west[r], pltpu.roll(here, 1, 0))
        after = jnp.where(sub == lon_cols - 1, east[r], pltpu.roll(here, lon_cols - 1, 0))
        shifted.append((before, here, after))
    for r in range(lat_rows):
        mix = sum(
            weight[3 * i + j : 3 * i + j + 1] * shifted[r + i][j] for i in range(3) for j in range(3)
        )
        mix = mix.astype(bf16).astype(f32)
        total[pl.ds(lon_cols * r, lon_cols), :] = grid_rows[r + 1] + mix

    for i in (6, 7, 8):
        fetch[i].wait()

    pltpu.make_async_copy(dst, dst, recv2).wait()
    parts = []
    for g in range(workers):
        piece = dst[g].astype(f32)
        parts += joined(piece, pltpu.roll(piece, half, 1))
    spectral = jnp.concatenate(parts, 0).astype(bf16)
    spectral = lax.dot_general(place_left, spectral, NT, preferred_element_type=f32)
    summed = (total[...] + spectral).astype(bf16).astype(f32)
    scale = lax.rsqrt(jnp.mean(summed * summed, axis=1, keepdims=True) + epsilon_norm)
    scaled = (summed * norm[...][None, :]).astype(bf16)
    hidden = jnp.dot(scaled, win[...], preferred_element_type=f32) * scale
    hidden = (0.5 * hidden * (1.0 + lax.erf(hidden * math.sqrt(0.5)))).astype(bf16)
    result = summed + jnp.dot(hidden, wout[...], preferred_element_type=f32)
    res[...] = result.astype(bf16)

    @pl.when(worker)
    def _():
        left_already(out.at[pl.ds(0, devices - 1)], send2)

    for g, gives in givers:
        @pl.when(gives)
        def _():
            filt_copy(g).wait_send()

    halo_wait(halo_send)

    @pl.when(jnp.logical_not(worker))
    def _():
        for i in (2, 3, 4):
            fetch[i].wait()


def sphere_block(lat_devices, lon_devices, latent_field, spectral_filter, conv_weight, norm_gain, weight_in, weight_out):
    channels, lat_rows, lon_cols = latent_field.shape
    points = lat_rows * lon_cols
    workers = len(worker_places(lat_devices, lon_devices))
    own = channels // workers
    table, select, quad, starts = folded_tables(lat_devices, lon_devices, lat_rows, lon_cols)
    table = jnp.asarray(table.astype(jnp.bfloat16))
    args = [
        jnp.transpose(latent_field, (1, 2, 0)).reshape(points, channels),
        spectral_filter.T,
        conv_weight,
        norm_gain,
        weight_in,
        weight_out,
        table,
        jnp.asarray(select),
        jnp.asarray(quad),
    ]
    order = range(len(args))
    copies = [pltpu.VMEM(args[i].shape, args[i].dtype) for i in order]
    devices = lat_devices * lon_devices
    bf16, f32, dma = jnp.bfloat16, jnp.float32, pltpu.SemaphoreType.DMA
    scratch = [
        pltpu.VMEM((points, channels), f32),
        pltpu.VMEM((workers, own // 2, 128), bf16),
        pltpu.VMEM((devices, own // 2, 128), bf16),
        pltpu.VMEM((devices, own // 2, 128), bf16),
        pltpu.VMEM((workers, own // 2, 128), bf16),
        pltpu.VMEM(args[1].shape, f32),
        pltpu.VMEM((2, lat_rows, channels), bf16),
        pltpu.VMEM((4, 8, 128), bf16),
        pltpu.VMEM((4, lat_rows, channels), bf16),
        pltpu.VMEM((4, 8, 128), bf16),
        pltpu.VMEM((points, channels), f32),
        dma((len(args),)), dma, dma((3,)), dma, dma, dma((2,)), dma((2,)), dma((workers // lon_devices,)), dma,
        pltpu.SemaphoreType.REGULAR,
    ]
    result = pl.pallas_call(
        functools.partial(block_kernel, lat_devices, lon_devices, lat_rows, lon_cols, starts),
        out_shape=pltpu.VMEM((points, channels), bf16),
        in_specs=[pl.BlockSpec(memory_space=pl.ANY)] * len(args),
        out_specs=pl.BlockSpec(memory_space=pltpu.VMEM),
        scratch_shapes=copies + scratch,
        compiler_params=pltpu.CompilerParams(collective_id=0, has_side_effects=True),
        name="sphere_block",
    )(*args)
    return jnp.transpose(result.reshape(lat_rows, lon_cols, channels), (2, 0, 1))


def fits_block(lat_devices, lon_devices, latent_field):
    channels, lat_rows, lon_cols = latent_field.shape
    workers = len(worker_places(lat_devices, lon_devices))
    return (
        lat_devices % 4 == 0
        and lon_devices % 4 == 0
        and lat_rows == 8
        and lon_cols == 8
        and channels % (8 * workers) == 0
        and channels // workers % 2 == 0
        and channels % 128 == 0
        and channels <= 1024
    )


def block_or_banded(lat_devices, lon_devices, *arguments):
    if fits_block(lat_devices, lon_devices, arguments[0]):
        return sphere_block(lat_devices, lon_devices, *arguments)
    return on_device(*arguments)


def solution(mesh):
    return jax.shard_map(
        functools.partial(block_or_banded, mesh.shape["lat"], mesh.shape["lon"]),
        mesh=mesh,
        in_specs=(P(None, "lat", "lon"), P("lon", None), P(), P(), P(), P()),
        out_specs=P(None, "lat", "lon"),
        check_vma=False,
    )
```

```python
import functools
import math

import jax
import jax.numpy as jnp
import numpy as np
from jax import lax
from jax.experimental import pallas as pl
from jax.experimental.pallas import tpu as pltpu
from jax.sharding import PartitionSpec as P

highest = lax.Precision.HIGHEST
epsilon_norm = 1e-06


def with_halo(cells, sides, width):
    for axis, dim in sides:
        count = lax.axis_size(axis)
        ends = count - 1
        head = lax.slice_in_dim(cells, 0, width, axis=dim)
        tail = lax.slice_in_dim(cells, cells.shape[dim] - width, cells.shape[dim], axis=dim)
        cells = jnp.concatenate(
            [
                lax.ppermute(tail, axis, [(i, (i + 1) % count) for i in range(ends)]),
                cells,
                lax.ppermute(head, axis, [((i + 1) % count, i) for i in range(ends)]),
            ],
            axis=dim,
        )
    return cells


def quadrature(lat_count):
    colatitude = (jnp.arange(lat_count, dtype=jnp.float32) + 0.5) * (math.pi / lat_count)
    return jnp.sin(colatitude) * (math.pi / lat_count)


def fourier_tables(lon_count, mode_count):
    wave_index = (
        jnp.arange(mode_count, dtype=jnp.int32)[:, None]
        * jnp.arange(lon_count, dtype=jnp.int32)[None, :]
    )
    phase_angle = (wave_index % lon_count).astype(jnp.float32) * (2.0 * math.pi / lon_count)
    cosine = jnp.cos(phase_angle)
    sine_table = jnp.sin(phase_angle)
    angle_step = 2.0 * math.pi / lon_count
    forward = jnp.concatenate([angle_step * cosine, -angle_step * sine_table], axis=0)
    weight = jnp.where(jnp.arange(mode_count, dtype=jnp.int32) == 0, 1.0, 2.0).astype(jnp.float32)[
        :, None
    ]
    inverse = jnp.concatenate([weight * cosine, -weight * sine_table], axis=0)
    return (forward, inverse)


def legendre_rows(order_ids, lat_count):
    colatitude = (jnp.arange(lat_count, dtype=jnp.float32) + 0.5) * (math.pi / lat_count)
    cosine = jnp.cos(colatitude)
    sine_col = jnp.sin(colatitude)
    order_f = order_ids.astype(jnp.float32)
    factor_index = jnp.arange(1, lat_count, dtype=jnp.float32)
    ratio_log = jnp.log((2.0 * factor_index - 1.0) / (2.0 * factor_index))
    included = (factor_index[None, :] <= order_f[:, None]).astype(jnp.float32)
    log_factor = jnp.sum(included * ratio_log[None, :], axis=1)
    start_log = 0.5 * jnp.log((2.0 * order_f + 1.0) / (4.0 * math.pi)) + 0.5 * log_factor
    start_log = start_log[:, None] + order_f[:, None] * jnp.log(sine_col)[None, :]
    blank_rows = jnp.zeros((order_ids.shape[0], lat_count), jnp.float32)
    order_col = order_f[:, None]

    def advance(state_carry, degree):
        before, current, scale_log = state_carry
        degree_f = degree.astype(jnp.float32)
        alpha_term = jnp.sqrt(
            (4.0 * degree_f * degree_f - 1.0)
            / jnp.maximum(degree_f * degree_f - order_col * order_col, 1.0)
        )
        beta_term = jnp.sqrt(
            jnp.maximum((degree_f - 1.0) ** 2 - order_col * order_col, 0.0)
            / jnp.maximum(4.0 * (degree_f - 1.0) ** 2 - 1.0, 1.0)
        )
        stepped = alpha_term * (cosine[None, :] * current - beta_term * before)
        at_start = order_ids[:, None] == degree
        past_start = order_ids[:, None] < degree
        fresh_value = jnp.where(at_start, 1.0, jnp.where(past_start, stepped, 0.0))
        fresh_log = jnp.where(at_start, start_log, scale_log)
        entry_value = fresh_value * jnp.exp(fresh_log)
        rescale = jnp.where(
            past_start | at_start, jnp.maximum(jnp.abs(fresh_value), jnp.abs(current)), 1.0
        )
        return (
            (current / rescale, fresh_value / rescale, fresh_log + jnp.log(rescale)),
            entry_value,
        )

    degrees = jnp.arange(lat_count, dtype=jnp.int32)
    unused, legendre = lax.scan(advance, (blank_rows, blank_rows, blank_rows), degrees)
    return legendre


def filter_modes(banded, legendre, filter_block, quad_weights):
    coefficients = jnp.einsum(
        "lmj,pmcj->pmcl", legendre, banded * quad_weights[None, None, None, :], precision=highest
    )
    coefficients = coefficients * filter_block[None, None, :, :]
    return jnp.einsum("lmj,pmcl->pmcj", legendre, coefficients, precision=highest)


def wrap_columns(extended):
    return jnp.concatenate([extended[:, :, -1:], extended, extended[:, :, :1]], axis=2)


def depthwise_core(extended, kernel, lat_rows, lon_cols):
    accumulated = jnp.zeros((extended.shape[0], lat_rows, lon_cols), jnp.float32)
    for row_shift in range(3):
        for col_shift in range(3):
            piece = extended[
                :, row_shift : row_shift + lat_rows, col_shift : col_shift + lon_cols
            ].astype(jnp.float32)
            accumulated = accumulated + kernel[3 * row_shift + col_shift][:, None, None] * piece
    return accumulated.astype(jnp.bfloat16)


def channel_mlp(summed_low, norm_gain, weight_in, weight_out):
    summed = summed_low.astype(jnp.float32)
    scale_inv = lax.rsqrt(jnp.mean(summed * summed, axis=0, keepdims=True) + epsilon_norm)
    normed = (summed * scale_inv * norm_gain[:, None]).astype(jnp.bfloat16)
    hidden = lax.dot_general(
        weight_in, normed, (((0,), (0,)), ((), ())), preferred_element_type=jnp.float32
    )
    hidden = jax.nn.gelu(hidden, approximate=False).astype(jnp.bfloat16)
    result = summed + lax.dot_general(
        weight_out, hidden, (((0,), (0,)), ((), ())), preferred_element_type=jnp.float32
    )
    return result.astype(jnp.bfloat16)


def add_three(first, second, third):
    total = first.astype(jnp.float32) + second.astype(jnp.float32) + third.astype(jnp.float32)
    return total.astype(jnp.bfloat16)


def on_device(latent_field, spectral_filter, conv_weight, norm_gain, weight_in, weight_out):
    channels, lat_rows, lon_cols = latent_field.shape
    sector_count = lax.axis_size("lon")
    lat_count = lat_rows * lax.axis_size("lat")
    lon_count = lon_cols * sector_count
    chan_block = channels // sector_count
    spread = lax.all_to_all(latent_field, "lon", split_axis=0, concat_axis=2, tiled=True)
    forward, inverse = fourier_tables(lon_count, lat_count)
    flattened = spread.astype(jnp.float32).reshape(chan_block * lat_rows, lon_count)
    spectrum = lax.dot_general(forward, flattened, (((1,), (1,)), ((), ())), precision=highest)
    spectrum = spectrum.reshape(2, lat_count, chan_block, lat_rows)
    banded = lax.all_to_all(spectrum, "lat", split_axis=1, concat_axis=3, tiled=True)
    order_ids = lax.axis_index("lat") * lat_rows + jnp.arange(lat_rows, dtype=jnp.int32)
    legendre = legendre_rows(order_ids, lat_count)
    synthesized = filter_modes(banded, legendre, spectral_filter, quadrature(lat_count))
    regathered = lax.all_to_all(synthesized, "lat", split_axis=3, concat_axis=1, tiled=True)
    regridded = lax.dot_general(
        regathered.reshape(2 * lat_count, chan_block * lat_rows),
        inverse,
        (((0,), (0,)), ((), ())),
        precision=highest,
    )
    spectral = regridded.reshape(chan_block, lat_rows, lon_count).astype(jnp.bfloat16)
    own_kernel = lax.dynamic_slice_in_dim(
        conv_weight, lax.axis_index("lon") * chan_block, chan_block, 1
    )
    rimmed = with_halo(spread, (("lat", 1),), 1)
    sector_mix = depthwise_core(wrap_columns(rimmed), own_kernel, lat_rows, lon_count)
    sector_sum = add_three(spread, spectral, sector_mix)
    summed = lax.all_to_all(sector_sum, "lon", split_axis=2, concat_axis=0, tiled=True)
    summed = summed.reshape(channels, lat_rows * lon_cols)
    result = channel_mlp(summed, norm_gain, weight_in, weight_out)
    return result.reshape(channels, lat_rows, lon_cols)


CLASSES = ((0, 0), (1, 0), (0, 1), (1, 1))


def folded_tables(lat_devices, lon_devices, lat_rows, lon_cols):
    lat_count, lon_count = lat_devices * lat_rows, lon_devices * lon_cols
    theta = (np.arange(lat_count // 2) + 0.5) * (math.pi / lat_count)
    x, s = np.cos(theta), np.sin(theta)
    phi = 2.0 * math.pi * (np.arange(lon_count // 2) + 0.5) / lon_count
    row, column = [], []
    for b in reversed(range(lon_devices // 2)):
        for a in range(lat_devices // 2):
            row.append(np.repeat(a * lat_rows + np.arange(lat_rows), lon_cols))
            column.append(np.tile(b * lon_cols + np.arange(lon_cols), lat_rows))
    row, column = np.concatenate(row), np.concatenate(column)
    columns = {key: [] for key in CLASSES}
    degrees = {key: [] for key in CLASSES}
    weights = {key: [] for key in CLASSES}
    for m in range(lat_count):
        k = np.arange(1, m + 1)
        log_start = 0.5 * (
            np.log((2 * m + 1) / (4 * math.pi)) + np.sum(np.log((2 * k - 1) / (2 * k)))
        )
        before, current = np.zeros(lat_count // 2), np.exp(log_start + m * np.log(s))
        for l in range(m, lat_count):
            if l > m:
                a = math.sqrt((4.0 * l * l - 1) / (l * l - m * m))
                b = math.sqrt(((l - 1.0) ** 2 - m * m) / (4.0 * (l - 1) ** 2 - 1))
                before, current = current, a * (x * current - b * before)
            for phase, wave in enumerate([np.cos(m * phi), -np.sin(m * phi)][: 1 if m == 0 else 2]):
                key = ((l + m) % 2, phase)
                columns[key].append(current[row] * wave[column])
                degrees[key].append(l)
                weights[key].append((1.0 if m == 0 else 2.0) * 2.0 * math.pi / lon_count)
    tables, selects, starts = [], [], [0]
    for key in CLASSES:
        width = -(-len(columns[key]) // 128) * 128
        fill = width - len(columns[key])
        tables.append(np.pad(np.stack(columns[key], 1), ((0, 0), (0, fill))))
        select = np.arange(lat_count)[:, None] == np.array(degrees[key])[None, :]
        selects.append(np.pad(select * np.array(weights[key])[None, :], ((0, 0), (0, fill))))
        starts.append(starts[-1] + width)
    quad = s * (math.pi / lat_count)
    quad = np.repeat(quad.reshape(lat_devices // 2, lat_rows), lon_cols, axis=1)
    return (
        np.concatenate(tables, 1),
        np.concatenate(selects, 1).astype(np.float32),
        np.tile(quad, (1, 2)).astype(np.float32),
        tuple(starts),
    )


MESH = pl.DeviceIdType.MESH


def worker_places(lat_devices, lon_devices):
    quarter = lon_devices // 4
    second = [(a, b) for b in range(quarter, 2 * quarter) for a in range(lat_devices)]
    third = [(a, b) for b in range(2 * quarter, 3 * quarter) for a in range(lat_devices - 1)]
    return [(0, b) for b in range(quarter)] + second + third


NT = (((1,), (1,)), ((), ()))


def block_kernel(
    lat_devices, lon_devices, lat_rows, lon_cols, starts,
    x_hbm, filter_hbm, taps_hbm, norm_hbm, win_hbm, wout_hbm, table_hbm, select_hbm, quad_hbm,
    res,
    xb, filt, taps, norm, win, wout, table, select, quad,
    xf, src, mid, out, dst, filt_in, edge_out, corner_out, edge_in, corner_in, total,
    local_sem, send1, recv1, send2, recv2, halo_send, halo_recv, filt_send, filt_recv, wrap,
):
    A, B = lat_devices, lon_devices
    A2, B2 = A // 2, B // 2
    places = worker_places(A, B)
    workers, devices = len(places), A * B
    groups = workers // B
    points, channels = xb.shape
    own = channels // workers
    rows = own // 2
    whole = rows // 8 * 8
    half = points
    a, b = lax.axis_index("lat"), lax.axis_index("lon")
    me = b * A + a
    quarter = B // 4

    def works(a, b):
        z = lax.div(b, quarter)
        return jnp.logical_or(
            z == 1, jnp.logical_or(jnp.logical_and(z == 2, a < A - 1), jnp.logical_and(z == 0, a == 0))
        )

    worker = works(a, b)
    mine = jnp.where(
        b < quarter,
        b,
        quarter
        + jnp.where(b < 2 * quarter, (b - quarter) * A + a, quarter * A + (b - 2 * quarter) * (A - 1) + a),
    )
    mine = jnp.where(worker, mine, -1)
    f32, bf16 = jnp.float32, jnp.bfloat16

    fetch = [
        pltpu.make_async_copy(s, d, local_sem.at[i])
        for i, (s, d) in enumerate(
            [(x_hbm, xb), (filter_hbm, filt), (quad_hbm, quad), (table_hbm, table), (select_hbm, select),
             (taps_hbm, taps), (norm_hbm, norm), (win_hbm, win), (wout_hbm, wout)]
        )
    ]
    fetch[0].start()
    barrier = pltpu.get_barrier_semaphore()
    neighbours = [(da, db) for da in (-1, 0, 1) for db in (-1, 0, 1) if (da, db) != (0, 0)]

    def inside(da):
        return jnp.logical_and(a + da >= 0, a + da < A)

    def at(da, db):
        return (a + da, lax.rem(b + db + B, B))

    @pl.when(worker)
    def _():
        def greet(peer, carry):
            @pl.when(peer != me)
            def _():
                pl.semaphore_signal(
                    barrier, inc=1, device_id=(lax.rem(peer, A), lax.div(peer, A)), device_id_type=MESH
                )

            return carry

        lax.fori_loop(0, devices, greet, 0)

    @pl.when(jnp.logical_not(worker))
    def _():
        for da, db in neighbours:
            @pl.when(jnp.logical_and(inside(da), b < B - 1) if db > 0 else inside(da))
            def _():
                pl.semaphore_signal(barrier, inc=1, device_id=at(da, db), device_id_type=MESH)

    for copy in fetch[1:]:
        copy.start()

    turn_lat, turn_lon = a >= A2, b >= B2
    p_row = lax.broadcasted_iota(jnp.int32, (points, 2 * half), 0)
    p_col = lax.broadcasted_iota(jnp.int32, (points, 2 * half), 1)

    def turned(index):
        jl, kl = lax.div(index, lon_cols), lax.rem(index, lon_cols)
        jl = jnp.where(turn_lat, lat_rows - 1 - jl, jl)
        kl = jnp.where(turn_lon, lon_cols - 1 - kl, kl)
        return jl * lon_cols + kl

    place = jnp.where(p_row == turned(lax.rem(p_col, half)), 1.0, 0.0)
    place_both = place.astype(bf16)
    place_left = jnp.where(p_col < half, place, 0.0).astype(bf16)
    left = lax.broadcasted_iota(jnp.int32, (rows, 2 * half), 1) < half

    def halves(value):
        if rows == whole:
            return value[:rows], value[rows:]
        rest = value[2 * whole :]
        return (
            jnp.concatenate([value[:whole], rest[: rows - whole]], 0),
            jnp.concatenate([value[whole : 2 * whole], rest[rows - whole :]], 0),
        )

    def joined(upper, lower):
        pieces = [upper[:whole], lower[:whole]]
        if rows > whole:
            pieces += [upper[whole:], lower[whole:]]
        return pieces

    fetch[0].wait()
    xf[...] = xb[...].astype(f32)
    xt = jnp.transpose(xf[...], (1, 0)).astype(bf16)
    xt = jnp.dot(xt, place_both, preferred_element_type=f32)
    for g in range(workers):
        upper, lower = halves(xt[own * g : own * (g + 1)])
        src[g] = jnp.where(left, upper, lower).astype(bf16)

    west, east = [
        jnp.concatenate([xf[k + lon_cols * r : k + lon_cols * r + 1] for r in range(lat_rows)], 0)
        for k in (0, lon_cols - 1)
    ]
    edge_out[0] = west.astype(bf16)
    edge_out[1] = east.astype(bf16)
    chunks = channels // 128
    for i, (r, side) in enumerate([(0, west), (0, east), (lat_rows - 1, west), (lat_rows - 1, east)]):
        parts = [side[r : r + 1, 128 * c : 128 * (c + 1)] for c in range(chunks)]
        parts.append(jnp.zeros((8 - chunks, 128), f32))
        corner_out[i] = jnp.concatenate(parts, 0).astype(bf16)

    rims = jnp.where(a > 0, 1, 0) + jnp.where(a < A - 1, 1, 0)
    greetings = jnp.where(worker, workers - 1, workers)
    for da, db in neighbours:
        other = at(da, db)
        known = jnp.logical_and(inside(da), jnp.logical_not(works(*other)))
        if db < 0:
            known = jnp.logical_and(known, b > 0)
        greetings = greetings + jnp.where(known, 1, 0)
    pl.semaphore_wait(barrier, greetings)

    @pl.when(b == B - 1)
    def _():
        for da in (-1, 0, 1):
            @pl.when(inside(da))
            def _():
                pl.semaphore_signal(wrap, inc=1, device_id=(a + da, 0), device_id_type=MESH)

    B4 = B2 // 2
    zone = jnp.where(b < B4, 0, jnp.where(b < B - B4, 1, 2))

    def first_copy(g):
        return pltpu.make_async_remote_copy(
            src_ref=src.at[g], dst_ref=mid.at[me], send_sem=send1, recv_sem=recv1.at[zone],
            device_id=places[g], device_id_type=MESH,
        )

    @pl.when(worker)
    def _():
        pltpu.make_async_copy(src.at[mine], mid.at[me], recv1.at[zone]).start()

    for order, case in [(reversed(range(workers)), b < B2), (range(workers), b >= B2)]:
        for g in order:
            @pl.when(jnp.logical_and(mine != g, case))
            def _():
                first_copy(g).start()

    fetch[1].wait()
    def filt_copy(g):
        return pltpu.make_async_remote_copy(
            src_ref=filt, dst_ref=filt_in, send_sem=filt_send.at[g % groups], recv_sem=filt_recv,
            device_id=places[g], device_id_type=MESH,
        )

    givers, keeps = [], False
    for g, (ag, bg) in enumerate(places):
        if bg == g // groups:
            keeps = jnp.logical_or(keeps, mine == g)
        else:
            givers.append((g, me == (g // groups) * A + ag))
    for g, gives in givers:
        @pl.when(gives)
        def _():
            filt_copy(g).start()

    @pl.when(keeps)
    def _():
        filt_in[...] = filt[...]

    def halo_copy(da, db):
        if db == 0:
            row = 0 if da < 0 else points - lon_cols
            source, target = xb.at[pl.ds(row, lon_cols)], edge_in.at[1 if da < 0 else 0]
            kind = 0
        elif da == 0:
            slot = 3 if db < 0 else 2
            source, target = edge_out.at[0 if db < 0 else 1], edge_in.at[slot]
            kind = 0
        else:
            index = (0 if da < 0 else 2) + (0 if db < 0 else 1)
            source, target = corner_out.at[index], corner_in.at[3 - index]
            kind = 1
        return pltpu.make_async_remote_copy(
            src_ref=source, dst_ref=target, send_sem=halo_send.at[kind], recv_sem=halo_recv.at[kind],
            device_id=at(da, db), device_id_type=MESH,
        )

    def left_already(blocks, sem):
        pltpu.make_async_copy(blocks, blocks, sem).wait()

    @pl.when(jnp.logical_not(worker))
    def _():
        left_already(src, send1)

    @pl.when(b == 0)
    def _():
        pl.semaphore_wait(wrap, 1 + rims)

    for da, db in neighbours:
        @pl.when(inside(da))
        def _():
            halo_copy(da, db).start()

    def index_of(ai, bi):
        return bi * A + ai

    def arrived(zone, start, count):
        blocks = mid.at[pl.ds(start, count)]
        pltpu.make_async_copy(blocks, blocks, recv1.at[zone]).wait()

    def widths(c):
        return pl.ds(starts[c], starts[c + 1] - starts[c])

    def folded(bs):
        tiles = [[] for _ in CLASSES]
        for bi in bs:
            parts = []
            for ai in range(A2):
                f00, f10, f01, f11 = [
                    mid[index_of(i, j)].astype(f32)
                    for i, j in [(ai, bi), (A - 1 - ai, bi), (ai, B - 1 - bi), (A - 1 - ai, B - 1 - bi)]
                ]
                s0, d0, s1, d1 = f00 + f10, f00 - f10, f01 + f11, f01 - f11
                w = quad[ai : ai + 1, :]
                parts.append([(s0 + s1) * w, (d0 + d1) * w, (s0 - s1) * w, (d0 - d1) * w])
            for ai in range(0, A2, 2):
                for c in range(4):
                    u, v = parts[ai][c], parts[ai + 1][c]
                    upper = jnp.where(left, u, pltpu.roll(v, half, 1))
                    lower = jnp.where(left, pltpu.roll(u, half, 1), v)
                    tiles[c].append(jnp.concatenate(joined(upper, lower), 0).astype(bf16))
        return [jnp.concatenate(t, 1) for t in tiles]

    inner = tuple(reversed(range(B2 // 2, B2)))
    outer = tuple(reversed(range(B2 // 2)))
    rows_of = lambda bs: pl.ds((B2 - 1 - bs[0]) * A2 * half, len(bs) * A2 * half)

    def second_copy(o):
        return pltpu.make_async_remote_copy(
            src_ref=out.at[o], dst_ref=dst.at[mine], send_sem=send2, recv_sem=recv2,
            device_id=(lax.rem(o, A), lax.div(o, A)), device_id_type=MESH,
        )

    @pl.when(worker)
    def _():
        for i in (2, 3, 4):
            fetch[i].wait()

        @pl.when(jnp.logical_not(keeps))
        def _():
            pltpu.make_async_copy(filt, filt_in, filt_recv).wait()

        held = filt_in.shape[1]
        r = lax.broadcasted_iota(jnp.int32, (own, held), 0)
        c = lax.broadcasted_iota(jnp.int32, (own, held), 1)
        pick = jnp.where(c == r + lax.rem(mine, groups) * own, 1.0, 0.0)
        rows = lax.dot_general(pick, filt_in[...], NT, precision=highest, preferred_element_type=f32)
        gain = jnp.dot(rows, select[...], precision=highest, preferred_element_type=f32)

        arrived(1, A * B4, devices - 2 * A * B4)
        acc = [
            jnp.dot(t, table[rows_of(inner), widths(i)], preferred_element_type=f32)
            for i, t in enumerate(folded(inner))
        ]
        arrived(0, 0, A * B4)
        arrived(2, devices - A * B4, A * B4)
        for i, t in enumerate(folded(outer)):
            acc[i] = acc[i] + jnp.dot(t, table[rows_of(outer), widths(i)], preferred_element_type=f32)
        coef = [(acc[i] * gain[:, starts[i] : starts[i + 1]]).astype(bf16) for i in range(4)]

        for bs in (outer, inner):
            grid = [
                lax.dot_general(coef[i], table[rows_of(bs), widths(i)], NT, preferred_element_type=f32)
                for i in range(4)
            ]
            for n, bi in enumerate(bs):
                for ai in range(0, A2, 2):
                    at_lane = (n * A2 + ai) * half
                    pp, mp, pm, mm = [g[:, at_lane : at_lane + 2 * half] for g in grid]
                    e0, e1, o0, o1 = pp + mp, pp - mp, pm + mm, pm - mm
                    for i, j, value in [(0, 0, e0 + o0), (1, 0, e1 + o1), (0, 1, e0 - o0), (1, 1, e1 - o1)]:
                        upper, lower = halves(value)
                        bj = B - 1 - bi if j else bi
                        a0, a1 = (A - 1 - ai, A - 2 - ai) if i else (ai, ai + 1)
                        out[index_of(a0, bj)] = jnp.where(left, upper, pltpu.roll(lower, half, 1)).astype(bf16)
                        out[index_of(a1, bj)] = jnp.where(left, pltpu.roll(upper, half, 1), lower).astype(bf16)

            def near_send(step, carry):
                o = lax.rem(step, B4) * A + lax.div(step, B4)

                @pl.when(o != me)
                def _():
                    second_copy(o).start()

                return carry

            def second_send(o, carry):
                @pl.when(o != me)
                def _():
                    second_copy(o).start()

                return carry

            def far_send(step, carry):
                return second_send(A * (B - B4) - 1 - step, carry)

            @pl.when(b < quarter)
            def _():
                if bs == outer:
                    lax.fori_loop(A * (B - B4), devices, second_send, 0)
                else:
                    lax.fori_loop(0, A * (B - B4), far_send, 0)

            @pl.when(b >= quarter)
            def _():
                if bs == outer:
                    lax.fori_loop(0, B4, near_send, 0)
                else:
                    lax.fori_loop(B4, A * B4, near_send, 0)
                    lax.fori_loop(A * B4, devices, second_send, 0)

        pltpu.make_async_copy(out.at[me], dst.at[mine], recv2).start()

    @pl.when(a == 0)
    def _():
        edge_in[0] = jnp.zeros(edge_in.shape[1:], bf16)
        corner_in[0] = jnp.zeros(corner_in.shape[1:], bf16)
        corner_in[1] = jnp.zeros(corner_in.shape[1:], bf16)

    @pl.when(a == A - 1)
    def _():
        edge_in[1] = jnp.zeros(edge_in.shape[1:], bf16)
        corner_in[2] = jnp.zeros(corner_in.shape[1:], bf16)
        corner_in[3] = jnp.zeros(corner_in.shape[1:], bf16)

    pole = rims == 1

    def halo_wait(sems):
        for edges, corners, case in [(3, 2, pole), (4, 4, jnp.logical_not(pole))]:
            @pl.when(case)
            def _():
                for kind, blocks in enumerate([edge_in.at[pl.ds(0, edges)], corner_in.at[pl.ds(0, corners)]]):
                    pltpu.make_async_copy(blocks, blocks, sems.at[kind]).wait()

    halo_wait(halo_recv)

    fetch[5].wait()
    weight = taps[...]
    grid_rows = [edge_in[0].astype(f32)]
    grid_rows += [xf[pl.ds(lon_cols * r, lon_cols), :] for r in range(lat_rows)]
    grid_rows += [edge_in[1].astype(f32)]

    def corner(i):
        piece = corner_in[i].astype(f32)
        return jnp.concatenate([piece[c : c + 1] for c in range(chunks)], 1)

    west, east = edge_in[2].astype(f32), edge_in[3].astype(f32)
    west = [corner(0)] + [west[r : r + 1] for r in range(lat_rows)] + [corner(2)]
    east = [corner(1)] + [east[r : r + 1] for r in range(lat_rows)] + [corner(3)]
    sub = lax.broadcasted_iota(jnp.int32, (lon_cols, channels), 0)
    shifted = []
    for r in range(lat_rows + 2):
        here = grid_rows[r]
        before = jnp.where(sub == 0, west[r], pltpu.roll(here, 1, 0))
        after = jnp.where(sub == lon_cols - 1, east[r], pltpu.roll(here, lon_cols - 1, 0))
        shifted.append((before, here, after))
    for r in range(lat_rows):
        mix = sum(
            weight[3 * i + j : 3 * i + j + 1] * shifted[r + i][j] for i in range(3) for j in range(3)
        )
        mix = mix.astype(bf16).astype(f32)
        total[pl.ds(lon_cols * r, lon_cols), :] = grid_rows[r + 1] + mix

    for i in (6, 7, 8):
        fetch[i].wait()

    pltpu.make_async_copy(dst, dst, recv2).wait()
    parts = []
    for g in range(workers):
        piece = dst[g].astype(f32)
        parts += joined(piece, pltpu.roll(piece, half, 1))
    spectral = jnp.concatenate(parts, 0).astype(bf16)
    spectral = lax.dot_general(place_left, spectral, NT, preferred_element_type=f32)
    summed = (total[...] + spectral).astype(bf16).astype(f32)
    scale = lax.rsqrt(jnp.mean(summed * summed, axis=1, keepdims=True) + epsilon_norm)
    scaled = (summed * norm[...][None, :]).astype(bf16)
    hidden = jnp.dot(scaled, win[...], preferred_element_type=f32) * scale
    hidden = (0.5 * hidden * (1.0 + lax.erf(hidden * math.sqrt(0.5)))).astype(bf16)
    result = summed + jnp.dot(hidden, wout[...], preferred_element_type=f32)
    res[...] = result.astype(bf16)

    @pl.when(worker)
    def _():
        left_already(out.at[pl.ds(0, devices - 1)], send2)
        left_already(src.at[pl.ds(0, workers - 1)], send1)

    for g, gives in givers:
        @pl.when(gives)
        def _():
            filt_copy(g).wait_send()

    halo_wait(halo_send)

    @pl.when(jnp.logical_not(worker))
    def _():
        for i in (2, 3, 4):
            fetch[i].wait()


def sphere_block(lat_devices, lon_devices, latent_field, spectral_filter, conv_weight, norm_gain, weight_in, weight_out):
    channels, lat_rows, lon_cols = latent_field.shape
    points = lat_rows * lon_cols
    workers = len(worker_places(lat_devices, lon_devices))
    own = channels // workers
    table, select, quad, starts = folded_tables(lat_devices, lon_devices, lat_rows, lon_cols)
    table = jnp.asarray(table.astype(jnp.bfloat16))
    args = [
        jnp.transpose(latent_field, (1, 2, 0)).reshape(points, channels),
        spectral_filter.T,
        conv_weight,
        norm_gain,
        weight_in,
        weight_out,
        table,
        jnp.asarray(select),
        jnp.asarray(quad),
    ]
    order = range(len(args))
    copies = [pltpu.VMEM(args[i].shape, args[i].dtype) for i in order]
    devices = lat_devices * lon_devices
    bf16, f32, dma = jnp.bfloat16, jnp.float32, pltpu.SemaphoreType.DMA
    scratch = [
        pltpu.VMEM((points, channels), f32),
        pltpu.VMEM((workers, own // 2, 128), bf16),
        pltpu.VMEM((devices, own // 2, 128), bf16),
        pltpu.VMEM((devices, own // 2, 128), bf16),
        pltpu.VMEM((workers, own // 2, 128), bf16),
        pltpu.VMEM(args[1].shape, f32),
        pltpu.VMEM((2, lat_rows, channels), bf16),
        pltpu.VMEM((4, 8, 128), bf16),
        pltpu.VMEM((4, lat_rows, channels), bf16),
        pltpu.VMEM((4, 8, 128), bf16),
        pltpu.VMEM((points, channels), f32),
        dma((len(args),)), dma, dma((3,)), dma, dma, dma((2,)), dma((2,)), dma((workers // lon_devices,)), dma,
        pltpu.SemaphoreType.REGULAR,
    ]
    result = pl.pallas_call(
        functools.partial(block_kernel, lat_devices, lon_devices, lat_rows, lon_cols, starts),
        out_shape=pltpu.VMEM((points, channels), bf16),
        in_specs=[pl.BlockSpec(memory_space=pl.ANY)] * len(args),
        out_specs=pl.BlockSpec(memory_space=pltpu.VMEM),
        scratch_shapes=copies + scratch,
        compiler_params=pltpu.CompilerParams(collective_id=0, has_side_effects=True),
        name="sphere_block",
    )(*args)
    return jnp.transpose(result.reshape(lat_rows, lon_cols, channels), (2, 0, 1))


def fits_block(lat_devices, lon_devices, latent_field):
    channels, lat_rows, lon_cols = latent_field.shape
    workers = len(worker_places(lat_devices, lon_devices))
    return (
        lat_devices % 4 == 0
        and lon_devices % 4 == 0
        and lat_rows == 8
        and lon_cols == 8
        and channels % (8 * workers) == 0
        and channels // workers % 2 == 0
        and channels % 128 == 0
        and channels <= 1024
    )


def block_or_banded(lat_devices, lon_devices, *arguments):
    if fits_block(lat_devices, lon_devices, arguments[0]):
        return sphere_block(lat_devices, lon_devices, *arguments)
    return on_device(*arguments)


def solution(mesh):
    return jax.shard_map(
        functools.partial(block_or_banded, mesh.shape["lat"], mesh.shape["lon"]),
        mesh=mesh,
        in_specs=(P(None, "lat", "lon"), P("lon", None), P(), P(), P(), P()),
        out_specs=P(None, "lat", "lon"),
        check_vma=False,
    )
```
